16 devices in a mesh: dp: 4 (over z, y), dap: 4 (over x, core).
Axes of the slice: x: 2, y: 2, z: 2, core: 2. Of those that a mesh axis runs over, the one named last changes fastest.
Arguments:
- single_rep: bfloat16 [4, 128, 384], P('dp', 'dap')
- pair_rep: bfloat16 [4, 128, 128, 128], P('dp', 'dap')
- token_mask: int32 [4, 128], P('dp')
- d_single_out: bfloat16 [4, 128, 384], P('dp', 'dap')
- d_pair_out: bfloat16 [4, 128, 128, 128], P('dp', 'dap')
- mul_out_in: bfloat16 [128, 512], replicated
- mul_out_gate: bfloat16 [128, 128], replicated
- mul_out_proj: bfloat16 [128, 128], replicated
- mul_in_in: bfloat16 [128, 512], replicated
- mul_in_gate: bfloat16 [128, 128], replicated
- mul_in_proj: bfloat16 [128, 128], replicated
- att_st_qkvg: bfloat16 [128, 512], replicated
- att_st_bias: bfloat16 [128, 4], replicated
- att_st_proj: bfloat16 [128, 128], replicated
- att_en_qkvg: bfloat16 [128, 512], replicated
- att_en_bias: bfloat16 [128, 4], replicated
- att_en_proj: bfloat16 [128, 128], replicated
- pair_up: bfloat16 [128, 1024], replicated
- pair_down: bfloat16 [512, 128], replicated
- sing_qkvg: bfloat16 [384, 1536], replicated
- sing_qbias: bfloat16 [384], replicated
- sing_pbias: bfloat16 [128, 16], replicated
- sing_proj: bfloat16 [384, 384], replicated
- sing_up: bfloat16 [384, 3072], replicated
- sing_down: bfloat16 [1536, 384], replicated
Outputs:
- output 1: bfloat16 [4, 128, 384], P('dp', 'dap')
- output 2: bfloat16 [4, 128, 128, 128], P('dp', 'dap')
- output 3: bfloat16 [4, 128, 384], P('dp', 'dap')
- output 4: bfloat16 [4, 128, 128, 128], P('dp', 'dap')
- output 5: float32 [3067264], P('dp')
All inputs are finite; a program needn't handle non-finite values.
Results may differ from the reference program's by a relative error of at most 0.02.
Values are sent between devices in bfloat16 or wider.
A program may use at most 1 GiB of HBM per device.

```python
import jax
import jax.numpy as jnp
from jax import lax

BATCH = 4
TOKENS = 128
C_S = 384
C_Z = 128
HEADS_S = 16
HEAD_S = 24
TRI_HEADS = 4
TRI_HEAD = 32
C_MUL = 128

NORM_EPS = 1e-5
MASK_PENALTY = 1.0e9


def weight_shapes():
    tri_width = TRI_HEADS * TRI_HEAD
    single_width = HEADS_S * HEAD_S
    return [
        ('mul_out_in', (C_Z, 4 * C_MUL), C_Z),
        ('mul_out_gate', (C_Z, C_Z), C_Z),
        ('mul_out_proj', (C_MUL, C_Z), C_MUL),
        ('mul_in_in', (C_Z, 4 * C_MUL), C_Z),
        ('mul_in_gate', (C_Z, C_Z), C_Z),
        ('mul_in_proj', (C_MUL, C_Z), C_MUL),
        ('att_st_qkvg', (C_Z, 4 * tri_width), C_Z),
        ('att_st_bias', (C_Z, TRI_HEADS), C_Z),
        ('att_st_proj', (tri_width, C_Z), tri_width),
        ('att_en_qkvg', (C_Z, 4 * tri_width), C_Z),
        ('att_en_bias', (C_Z, TRI_HEADS), C_Z),
        ('att_en_proj', (tri_width, C_Z), tri_width),
        ('pair_up', (C_Z, 8 * C_Z), C_Z),
        ('pair_down', (4 * C_Z, C_Z), 4 * C_Z),
        ('sing_qkvg', (C_S, 4 * single_width), C_S),
        ('sing_qbias', (single_width,), 1),
        ('sing_pbias', (C_Z, HEADS_S), C_Z),
        ('sing_proj', (single_width, C_S), single_width),
        ('sing_up', (C_S, 8 * C_S), C_S),
        ('sing_down', (4 * C_S, C_S), 4 * C_S),
    ]


def setup_inputs(seed: int = 0) -> dict:
    base_key = jax.random.key(seed)
    key_list = jax.random.split(base_key, 32)
    lengths = jax.random.randint(key_list[0], (BATCH,), TOKENS // 4, TOKENS + 1)
    full_pick = jax.random.randint(key_list[1], (), 0, BATCH)
    lengths = jnp.where(jnp.arange(BATCH) == full_pick, TOKENS, lengths)
    inputs = {}
    inputs['single_rep'] = jax.random.normal(key_list[2], (BATCH, TOKENS, C_S), jnp.float32).astype(jnp.bfloat16)
    inputs['pair_rep'] = jax.random.normal(key_list[3], (BATCH, TOKENS, TOKENS, C_Z), jnp.float32).astype(jnp.bfloat16)
    inputs['token_mask'] = (jnp.arange(TOKENS)[None, :] < lengths[:, None]).astype(jnp.int32)
    inputs['d_single_out'] = jax.random.normal(key_list[4], (BATCH, TOKENS, C_S), jnp.float32).astype(jnp.bfloat16)
    inputs['d_pair_out'] = jax.random.normal(key_list[5], (BATCH, TOKENS, TOKENS, C_Z), jnp.float32).astype(jnp.bfloat16)
    for w_index, (w_name, w_shape, fan_in) in enumerate(weight_shapes()):
        w_draw = jax.random.normal(key_list[6 + w_index], w_shape, jnp.float32)
        inputs[w_name] = (w_draw * fan_in ** -0.5).astype(jnp.bfloat16)
    return inputs


def layer_norm(x_in):
    x_f32 = x_in.astype(jnp.float32)
    centered = x_f32 - jnp.mean(x_f32, axis=-1, keepdims=True)
    row_var = jnp.mean(centered * centered, axis=-1, keepdims=True)
    return centered * lax.rsqrt(row_var + NORM_EPS)


def tri_mul(z_one, w_in, w_gate, w_out, mix_form):
    normed = layer_norm(z_one).astype(jnp.bfloat16)
    proj_all = jnp.dot(normed, w_in, preferred_element_type=jnp.float32)
    left_proj = (jax.nn.sigmoid(proj_all[..., C_MUL:2 * C_MUL]) * proj_all[..., :C_MUL]).astype(jnp.bfloat16)
    right_proj = (jax.nn.sigmoid(proj_all[..., 3 * C_MUL:]) * proj_all[..., 2 * C_MUL:3 * C_MUL]).astype(jnp.bfloat16)
    gate_vals = jax.nn.sigmoid(jnp.dot(normed, w_gate, preferred_element_type=jnp.float32))
    mixed_sum = jnp.einsum(mix_form, left_proj.astype(jnp.float32), right_proj.astype(jnp.float32))
    mixed_norm = layer_norm(mixed_sum).astype(jnp.bfloat16)
    update = gate_vals * jnp.dot(mixed_norm, w_out, preferred_element_type=jnp.float32)
    return (z_one.astype(jnp.float32) + update).astype(jnp.bfloat16)


def tri_att(z_one, mask_bias, w_qkvg, w_tb, w_o):
    normed = layer_norm(z_one).astype(jnp.bfloat16)
    proj_all = jnp.dot(normed, w_qkvg, preferred_element_type=jnp.float32)
    tri_width = TRI_HEADS * TRI_HEAD
    head_shape = (TOKENS, TOKENS, TRI_HEADS, TRI_HEAD)
    q_all = proj_all[..., :tri_width].astype(jnp.bfloat16).reshape(head_shape)
    k_all = proj_all[..., tri_width:2 * tri_width].astype(jnp.bfloat16).reshape(head_shape)
    v_all = proj_all[..., 2 * tri_width:3 * tri_width].astype(jnp.bfloat16).reshape(head_shape)
    gate_vals = jax.nn.sigmoid(proj_all[..., 3 * tri_width:])
    bias_hjk = jnp.transpose(jnp.dot(normed, w_tb, preferred_element_type=jnp.float32).astype(jnp.bfloat16), (2, 0, 1)).astype(jnp.float32)
    att_scale = TRI_HEAD ** -0.5

    def one_row(row_item):
        q_row, k_row, v_row = row_item
        logits = jnp.einsum('jhd,khd->hjk', q_row.astype(jnp.float32), k_row.astype(jnp.float32)) * att_scale + bias_hjk + mask_bias
        prob_mat = jax.nn.softmax(logits, axis=-1).astype(jnp.bfloat16)
        return jnp.einsum('hjk,khd->jhd', prob_mat.astype(jnp.float32), v_row.astype(jnp.float32))

    attended = lax.map(one_row, (q_all, k_all, v_all))
    gated = (gate_vals * attended.reshape(TOKENS, TOKENS, tri_width)).astype(jnp.bfloat16)
    return (z_one.astype(jnp.float32) + jnp.dot(gated, w_o, preferred_element_type=jnp.float32)).astype(jnp.bfloat16)


def transition(x_rows, w_up, w_down):
    normed = layer_norm(x_rows).astype(jnp.bfloat16)
    hidden = jnp.dot(normed, w_up, preferred_element_type=jnp.float32)
    inner_dim = w_down.shape[0]
    acted = (jax.nn.silu(hidden[..., :inner_dim]) * hidden[..., inner_dim:]).astype(jnp.bfloat16)
    return (x_rows.astype(jnp.float32) + jnp.dot(acted, w_down, preferred_element_type=jnp.float32)).astype(jnp.bfloat16)


def single_att(s_one, z_one, mask_bias, w_qkvg, q_bias, w_pb, w_o):
    normed = layer_norm(s_one).astype(jnp.bfloat16)
    proj_all = jnp.dot(normed, w_qkvg, preferred_element_type=jnp.float32)
    single_width = HEADS_S * HEAD_S
    head_shape = (TOKENS, HEADS_S, HEAD_S)
    q_all = (proj_all[:, :single_width] + q_bias.astype(jnp.float32)).astype(jnp.bfloat16).reshape(head_shape)
    k_all = proj_all[:, single_width:2 * single_width].astype(jnp.bfloat16).reshape(head_shape)
    v_all = proj_all[:, 2 * single_width:3 * single_width].astype(jnp.bfloat16).reshape(head_shape)
    gate_vals = jax.nn.sigmoid(proj_all[:, 3 * single_width:])
    pair_norm = layer_norm(z_one).astype(jnp.bfloat16)
    bias_all = jnp.dot(pair_norm, w_pb, preferred_element_type=jnp.float32).astype(jnp.bfloat16)
    logits = jnp.einsum('ihd,jhd->hij', q_all.astype(jnp.float32), k_all.astype(jnp.float32)) * HEAD_S ** -0.5
    logits = logits + jnp.transpose(bias_all, (2, 0, 1)).astype(jnp.float32) + mask_bias
    prob_mat = jax.nn.softmax(logits, axis=-1).astype(jnp.bfloat16)
    attended = jnp.einsum('hij,jhd->ihd', prob_mat.astype(jnp.float32), v_all.astype(jnp.float32))
    gated = (gate_vals * attended.reshape(TOKENS, single_width)).astype(jnp.bfloat16)
    return (s_one.astype(jnp.float32) + jnp.dot(gated, w_o, preferred_element_type=jnp.float32)).astype(jnp.bfloat16)


def block_forward(s_one, z_one, mask_one, params):
    w_list = [p_item.astype(jnp.bfloat16) for p_item in params]
    mask_bias = (mask_one.astype(jnp.float32) - 1.0) * MASK_PENALTY
    z_val = tri_mul(z_one, w_list[0], w_list[1], w_list[2], 'ikc,jkc->ijc')
    z_val = tri_mul(z_val, w_list[3], w_list[4], w_list[5], 'kic,kjc->ijc')
    z_val = tri_att(z_val, mask_bias, w_list[6], w_list[7], w_list[8])
    z_val = jnp.transpose(tri_att(jnp.transpose(z_val, (1, 0, 2)), mask_bias, w_list[9], w_list[10], w_list[11]), (1, 0, 2))
    z_val = transition(z_val, w_list[12], w_list[13])
    s_val = single_att(s_one, z_val, mask_bias, w_list[14], w_list[15], w_list[16], w_list[17])
    s_val = transition(s_val, w_list[18], w_list[19])
    return s_val, z_val


def reference(single_rep, pair_rep, token_mask, d_single_out, d_pair_out, mul_out_in, mul_out_gate, mul_out_proj, mul_in_in, mul_in_gate, mul_in_proj, att_st_qkvg, att_st_bias, att_st_proj, att_en_qkvg, att_en_bias, att_en_proj, pair_up, pair_down, sing_qkvg, sing_qbias, sing_pbias, sing_proj, sing_up, sing_down):
    weights = (mul_out_in, mul_out_gate, mul_out_proj, mul_in_in, mul_in_gate, mul_in_proj, att_st_qkvg, att_st_bias, att_st_proj, att_en_qkvg, att_en_bias, att_en_proj, pair_up, pair_down, sing_qkvg, sing_qbias, sing_pbias, sing_proj, sing_up, sing_down)
    params = tuple(w_item.astype(jnp.float32) for w_item in weights)

    def scan_step(grad_acc, scan_item):
        s_one, z_one, mask_one, gs_one, gz_one = scan_item

        def forward_one(s_val, z_val, p_val):
            return block_forward(s_val, z_val, mask_one, p_val)

        outs_one, pull_back = jax.vjp(forward_one, s_one, z_one, params)
        ds_one, dz_one, grad_one = pull_back((gs_one, gz_one))
        new_acc = tuple(acc_item + grad_item for acc_item, grad_item in zip(grad_acc, grad_one))
        return new_acc, (outs_one[0], outs_one[1], ds_one, dz_one)

    init_acc = tuple(jnp.zeros_like(p_item) for p_item in params)
    grad_sums, stacked = lax.scan(scan_step, init_acc, (single_rep, pair_rep, token_mask, d_single_out, d_pair_out))
    grad_flat = jnp.concatenate([g_item.reshape(-1) for g_item in grad_sums])
    return stacked[0], stacked[1], stacked[2], stacked[3], grad_flat
```

```python
import functools
import jax
import jax.numpy as jnp
from jax import lax
from jax.experimental import pallas as pl
from jax.experimental.pallas import tpu as pltpu
from jax.sharding import PartitionSpec as P

BATCH_AXIS = 'dp'
GROUP_AXIS = 'dap'
NORM_EPS = 1e-5
MASK_PENALTY = 1.0e9


def gather_rows(x_in):
    return lax.all_gather(x_in, GROUP_AXIS, axis=0, tiled=True)


F32 = jnp.float32
NOMINAL_BYTES = 4 << 20
GIGA = 1 << 30
BF16 = jnp.bfloat16
ROWS = 32
COLS = 128
CH = 128
HALF = 2 * CH
N_POS = ROWS * COLS
TRI_HEADS = 4
GRP = 4
OFFSETS = (1, 2, 3)
MESH_ID = pl.DeviceIdType.MESH
FOUR = 4
N_DEV = 16
WIDE = FOUR * COLS
TRI_DIM = 32
TRI_SCALE = TRI_DIM ** -0.5
STEP_ROWS = 4
CHUNK = STEP_ROWS * COLS


def dot_nn(a, b):
    return lax.dot_general(a, b, (((1,), (0,)), ((), ())), preferred_element_type=F32)


def dot_nt(a, b):
    return lax.dot_general(a, b, (((1,), (1,)), ((), ())), preferred_element_type=F32)


def dot_tn(a, b):
    return lax.dot_general(a, b, (((0,), (0,)), ((), ())), preferred_element_type=F32)


def cat0(xs):
    return jnp.concatenate(xs, axis=0)


def cat1(xs):
    return jnp.concatenate(xs, axis=1)


def loop(count, step, unroll=1):
    def body(i, carry):
        step(i)
        return carry

    lax.fori_loop(0, count, body, 0, unroll=unroll)


def col_mean(x):
    return jnp.mean(x, axis=0, keepdims=True)


def col_sum(x):
    return jnp.sum(x, axis=0, keepdims=True)


def row_mean(x):
    return jnp.mean(x, axis=-1, keepdims=True)


def softmax_cols(x):
    e = jnp.exp(x - jnp.max(x, axis=0, keepdims=True))
    return e * (1.0 / col_sum(e))


def col_norm(x):
    c = x - col_mean(x)
    r = lax.rsqrt(col_mean(c * c) + NORM_EPS)
    return c * r, r


def swap_all(x, split, join):
    return lax.all_to_all(x, GROUP_AXIS, split, join, tiled=True)


def norm_parts(x):
    c = x - row_mean(x)
    r = lax.rsqrt(row_mean(c * c) + NORM_EPS)
    return c * r, r


def norm_back(dn, nhat, r):
    return r * (dn - row_mean(dn) - nhat * row_mean(dn * nhat))


def chunk_ds(t, size=CHUNK):
    return pl.ds(pl.multiple_of(t * size, size), size)


def call(kernel, out_shape, scratch=(), flops=0, name=None, comm=None):
    n_out = len(out_shape)
    vm = pl.BlockSpec(memory_space=pltpu.VMEM)

    def run(*args):
        return pl.pallas_call(
            kernel, out_shape=tuple(out_shape), in_specs=[vm] * len(args), out_specs=tuple([vm] * n_out),
            scratch_shapes=list(scratch), name=name,
            compiler_params=pltpu.CompilerParams(collective_id=comm, has_side_effects=comm is not None),
            cost_estimate=pl.CostEstimate(flops=flops, bytes_accessed=NOMINAL_BYTES, transcendentals=0),
        )(*args)

    def run_one(*args):
        return run(*args)[0]

    return run if n_out > 1 else run_one


def sds(shape, dtype):
    return jax.ShapeDtypeStruct(shape, dtype)


def greet(me):
    sem = pltpu.get_barrier_semaphore()
    for off in OFFSETS:
        pl.semaphore_signal(sem, inc=1, device_id={GROUP_AXIS: lax.rem(me + off, GRP)}, device_id_type=MESH_ID)


def await_group():
    pl.semaphore_wait(pltpu.get_barrier_semaphore(), len(OFFSETS))


class Exchange:
    def __init__(self, me, src_at, dst_at, send_sem, recv_sem):
        self.copies = []
        for i, off in enumerate(OFFSETS):
            dest = lax.rem(me + off, GRP)
            self.copies.append(pltpu.make_async_remote_copy(
                src_ref=src_at(dest), dst_ref=dst_at(me), send_sem=send_sem.at[i], recv_sem=recv_sem.at[i],
                device_id={GROUP_AXIS: dest}, device_id_type=MESH_ID))
        for c in self.copies:
            c.start()

    def arrive(self):
        for c in self.copies:
            c.wait_recv()

    def leave(self):
        for c in self.copies:
            c.wait_send()


def own_rows(p, size=ROWS):
    return pl.ds(pl.multiple_of(p * size, size), size)


class Turn:
    def __init__(self, me, scr_ref, stage_ref, out_ref, send, recv):
        self.me, self.scr, self.stage, self.out, self.send, self.recv = me, scr_ref, stage_ref, out_ref, send, recv
        self.sent = []

    def half(self, n):
        lo = n * HALF_ROWS

        def cast(j):
            rows = self.scr[pl.ds(pl.multiple_of(j * ROWS + lo, HALF_ROWS), HALF_ROWS), :]
            self.stage[j // ROWS, lax.rem(j, ROWS), lo:lo + HALF_ROWS, :] = rows.astype(BF16)

        loop(COLS, cast, FOUR)
        part = (slice(None), slice(lo, lo + HALF_ROWS))
        self.sent.append(Exchange(self.me, lambda p: self.stage.at[(p, *part)], lambda m: self.out.at[(m, *part)], self.send.at[n], self.recv.at[n]))

    def finish(self):
        self.out[self.me] = self.stage[self.me]
        for ex in self.sent:
            ex.arrive()
            ex.leave()


TURNED = (GRP, ROWS, ROWS, CH)
HALF_ROWS = ROWS // 2


def turn_scratch():
    sems = pltpu.SemaphoreType.DMA((2, len(OFFSETS)))
    return [pltpu.VMEM((N_POS, CH), F32), pltpu.VMEM(TURNED, BF16), sems, sems]


def peer_sems():
    sems = pltpu.SemaphoreType.DMA((len(OFFSETS),))
    return [sems, sems]


ATT_STEP = 4
PACK = 8
BWD_STEP = 4


def fill_bias(bias_ref, mask_ref, bm_ref):
    mask = mask_ref[...]
    for h in range(TRI_HEADS):
        cols = slice(h * COLS, (h + 1) * COLS)
        bm_ref[:, cols] = bias_ref[:, cols].astype(F32).T + mask


def head_rows(x, h):
    return x[h * TRI_DIM:(h + 1) * TRI_DIM]


def spread_heads(xt):
    zero = jnp.zeros((TRI_DIM, COLS), xt.dtype)
    return cat1([
        cat0([head_rows(xt, h) if g == h else zero for g in range(TRI_HEADS)])
        for h in range(TRI_HEADS)])


def probs_of(k, q_wide, bm_ref):
    x = dot_nn(k, q_wide) * TRI_SCALE + bm_ref[...]
    return softmax_cols(x)


def heads_nn(xt, wide):
    return cat0([dot_nn(head_rows(xt, h), wide[:, h * COLS:(h + 1) * COLS]) for h in range(TRI_HEADS)])


def att_fwd_kernel(ending, z_ref, wbt_ref, mask_ref, wt_ref, wo_ref, o_ref, bias_ref, bm_ref, own_ref, send, recv, *rest):
    me = lax.axis_index(GROUP_AXIS)
    greet(me)
    turn = None if ending else Turn(me, rest[0], rest[1], o_ref, *rest[2:])

    def bias_step(t):
        nhat, _ = norm_parts(cat0([load_row(z_ref, t * PACK + r, ending) for r in range(PACK)]).astype(F32))
        nb = nhat.astype(BF16)
        b = [dot_nt(wbt_ref[...], nb[r * COLS:(r + 1) * COLS]) for r in range(PACK)]
        for h in range(TRI_HEADS):
            own_ref[chunk_ds(t, PACK), h * COLS:(h + 1) * COLS] = cat0([x[h:h + 1, :] for x in b])

    loop(ROWS // PACK, bias_step)
    bias_ref[own_rows(me), :] = own_ref[...].astype(BF16)
    await_group()
    ex = Exchange(me, lambda p: bias_ref.at[own_rows(me), :], lambda m: bias_ref.at[own_rows(m), :], send, recv)
    ex.arrive()
    fill_bias(bias_ref, mask_ref, bm_ref)

    def step(t):
        z = cat0([load_row(z_ref, t * ATT_STEP + r, ending) for r in range(ATT_STEP)]).astype(F32)
        nhat, _ = norm_parts(z)
        nb = nhat.astype(BF16)
        qt_all = dot_nt(wt_ref[:CH, :], nb)
        k_all = dot_nt(nb, wt_ref[CH:HALF, :]).astype(BF16)
        vg_all = dot_nt(wt_ref[HALF:, :], nb)
        gate = jax.nn.sigmoid(vg_all[CH:])
        outs = []
        for r in range(ATT_STEP):
            cols = slice(r * COLS, (r + 1) * COLS)
            q_wide = spread_heads(qt_all[:, cols]).astype(BF16)
            probs = probs_of(k_all[cols], q_wide, bm_ref).astype(BF16)
            outs.append(heads_nn(vg_all[:CH, cols].astype(BF16), probs))
        gated = (gate * cat1(outs)).astype(BF16)
        out = z + dot_tn(gated, wo_ref[...])
        for r in range(ATT_STEP):
            rows = slice(r * COLS, (r + 1) * COLS)
            if turn is None:
                o_ref[chunk_ds(t * ATT_STEP + r, COLS), :] = out[rows].astype(BF16)
            else:
                put_strided(turn.scr, t * ATT_STEP + r, out[rows])

    halves(ROWS // ATT_STEP, step, turn)
    ex.leave()


def halves(count, step, turn):
    if turn is None:
        loop(count, step)
        return
    loop(count // 2, step)
    turn.half(0)
    loop(count // 2, lambda t: step(t + count // 2))
    turn.half(1)
    turn.finish()


def att_fwd(z, w_b, mask_col, wt, w_o, ending):
    scr = [pltpu.VMEM((COLS, TRI_HEADS * COLS), F32), pltpu.VMEM((ROWS, TRI_HEADS * COLS), F32)] + peer_sems()
    out = sds((N_POS, CH) if ending else TURNED, BF16)
    return call(functools.partial(att_fwd_kernel, ending), [out, sds((COLS, TRI_HEADS * COLS), BF16)],
                scr if ending else scr + turn_scratch(), flops=3 * GIGA, name='att_fwd', comm=4 if ending else 3,
                )(z, w_b.T, mask_col, wt, w_o)


def att_bwd_kernel(z_blocked, dz_blocked, z_ref, dz_ref, bias_ref, mask_ref, wt_ref, wo_ref, dzo_ref, dwr_ref, dwo_ref, db_ref, bm_ref, acc_ref, dwqg_ref, dwkv_ref):
    fill_bias(bias_ref, mask_ref, bm_ref)
    acc_ref[...] = jnp.zeros_like(acc_ref)
    dwqg_ref[...] = jnp.zeros_like(dwqg_ref)
    dwkv_ref[...] = jnp.zeros_like(dwkv_ref)
    dwo_ref[...] = jnp.zeros_like(dwo_ref)

    def step(t):
        nhat, r_std = norm_parts(cat0([load_row(z_ref, t * BWD_STEP + r, z_blocked) for r in range(BWD_STEP)]).astype(F32))
        nb = nhat.astype(BF16)
        pt_all = dot_nt(wt_ref[...], nb)
        kv_all = dot_nt(nb, wt_ref[CH:3 * CH, :]).astype(BF16)
        gate = jax.nn.sigmoid(pt_all[3 * CH:])
        dz = cat0([load_row(dz_ref, t * BWD_STEP + r, dz_blocked) for r in range(BWD_STEP)])
        d_gated = dot_nt(wo_ref[...], dz)
        d_att = d_gated * gate
        outs, dqs, dkvs = [], [], []
        for r in range(BWD_STEP):
            cols = slice(r * COLS, (r + 1) * COLS)
            q_wide = spread_heads(pt_all[:CH, cols]).astype(BF16)
            do_wide = spread_heads(d_att[:, cols]).astype(BF16)
            p = probs_of(kv_all[cols, :CH], q_wide, bm_ref)
            pb = p.astype(BF16)
            outs.append(heads_nn(pt_all[2 * CH:3 * CH, cols].astype(BF16), pb))
            dp = dot_nn(kv_all[cols, CH:], do_wide)
            ds = p * (dp - col_sum(dp * p))
            acc_ref[...] += ds
            dsb = (ds * TRI_SCALE).astype(BF16)
            dqs.append(heads_nn(pt_all[CH:2 * CH, cols].astype(BF16), dsb))
            dkvs.append(cat1([dot_nt(dsb, q_wide), dot_nt(pb, do_wide)]).astype(BF16))
        o = cat1(outs)
        gated = (gate * o).astype(BF16)
        dgl = d_gated * o * gate * (1.0 - gate)
        dqg = cat0([cat1(dqs), dgl]).astype(BF16)
        dkv = cat0(dkvs)
        dwo_ref[...] += dot_nn(gated, dz)
        dwqg_ref[...] += dot_nn(dqg, nb)
        dwkv_ref[...] += dot_tn(nb, dkv)
        dn = dot_nn(dkv, wt_ref[CH:3 * CH, :]) + dot_tn(dqg[:CH], wt_ref[:CH, :]) + dot_tn(dqg[CH:], wt_ref[3 * CH:, :])
        dzo_ref[chunk_ds(t, BWD_STEP * COLS), :] = (dz.astype(F32) + norm_back(dn, nhat, r_std)).astype(BF16)

    loop(ROWS // BWD_STEP, step)
    for h in range(TRI_HEADS):
        cols = slice(h * COLS, (h + 1) * COLS)
        db_ref[:, cols] = acc_ref[:, cols].T
    for m in range(2):
        dwr_ref[pl.ds(3 * m, CH, stride=4), :] = dwqg_ref[m * CH:(m + 1) * CH, :].T
        dwr_ref[pl.ds(1 + m, CH, stride=4), :] = dwkv_ref[:, m * CH:(m + 1) * CH]


def att_bwd(z, dz, bias_all, mask_col, wt, w_o, z_blocked, dz_blocked):
    return call(functools.partial(att_bwd_kernel, z_blocked, dz_blocked),
                [sds((N_POS, CH), BF16), sds((4 * CH, CH), F32), sds((CH, CH), F32), sds((COLS, TRI_HEADS * COLS), F32)],
                [pltpu.VMEM((COLS, TRI_HEADS * COLS), F32), pltpu.VMEM((COLS, TRI_HEADS * COLS), F32),
                 pltpu.VMEM((2 * CH, CH), F32), pltpu.VMEM((CH, 2 * CH), F32)],
                flops=8 * GIGA, name='att_bwd')(z, dz, bias_all, mask_col, wt, w_o)


def bias_bwd_kernel(ending, z_ref, dz_ref, db_ref, wbt_ref, dzo_ref, dwt_ref, parts_ref, send, recv, *rest):
    me = lax.axis_index(GROUP_AXIS)
    greet(me)
    turn = Turn(me, rest[0], rest[1], dzo_ref, *rest[2:]) if ending else None
    dwt_ref[...] = jnp.zeros_like(dwt_ref)
    wbt = wbt_ref[...]
    await_group()
    ex = Exchange(me, lambda p: db_ref.at[own_rows(p), :], lambda m: parts_ref.at[m], send, recv)
    parts_ref[me] = db_ref[own_rows(me), :]
    ex.arrive()

    def step(t):
        block = sum(parts_ref[g, chunk_ds(t, PACK), :] for g in range(GRP))
        nhat, r_std = norm_parts(cat0([load_row(z_ref, t * PACK + r, ending) for r in range(PACK)]).astype(F32))
        nb = nhat.astype(BF16)
        dwt = jnp.zeros((TRI_HEADS, CH), F32)
        dns = []
        for r in range(PACK):
            db = cat0([block[r:r + 1, h * COLS:(h + 1) * COLS] for h in range(TRI_HEADS)]).astype(BF16)
            dwt += dot_nn(db, nb[r * COLS:(r + 1) * COLS])
            dns.append(dot_tn(db, wbt))
        out = dz_ref[chunk_ds(t, PACK * COLS), :].astype(F32) + norm_back(cat0(dns), nhat, r_std)
        if turn is None:
            dzo_ref[chunk_ds(t, PACK * COLS), :] = out.astype(BF16)
        else:
            for r in range(PACK):
                put_strided(turn.scr, t * PACK + r, out[r * COLS:(r + 1) * COLS])
        dwt_ref[...] += dwt

    halves(ROWS // PACK, step, turn)
    ex.leave()


def bias_bwd(z, dz, db, w_b, ending):
    scr = [pltpu.VMEM((GRP, ROWS, TRI_HEADS * COLS), F32)] + peer_sems()
    out = sds(TURNED if ending else (N_POS, CH), BF16)
    return call(functools.partial(bias_bwd_kernel, ending), [out, sds((TRI_HEADS, CH), F32)],
                scr + turn_scratch() if ending else scr, flops=GIGA, name='bias_bwd', comm=6 if ending else 5,
                )(z, dz, db, w_b.T)


SING_HEADS = 16


def trans_fwd_kernel(z_ref, wu_ref, wd_ref, wpt_ref, o_ref, b_ref, scr_ref):
    def step(t):
        z = z_ref[chunk_ds(t), :].astype(F32)
        nhat, _ = norm_parts(z)
        hid = dot_nn(nhat.astype(BF16), wu_ref[...])
        h1, h2 = hid[:, :4 * CH], hid[:, 4 * CH:]
        act = (jax.nn.sigmoid(h1) * h1 * h2).astype(BF16)
        out = (z + dot_nn(act, wd_ref[...])).astype(BF16)
        o_ref[chunk_ds(t), :] = out
        n5, _ = norm_parts(out.astype(F32))
        n5 = n5.astype(BF16)
        for r in range(STEP_ROWS):
            scr_ref[pl.ds(t * STEP_ROWS + r, SING_HEADS, stride=ROWS), :] = dot_nt(wpt_ref[...], n5[r * COLS:(r + 1) * COLS])

    loop(ROWS // STEP_ROWS, step)
    b_ref[...] = scr_ref[...].astype(BF16)


def trans_fwd(z, w_up, w_down, w_pb):
    return call(trans_fwd_kernel, [sds((N_POS, CH), BF16), sds((SING_HEADS * ROWS, COLS), BF16)],
                [pltpu.VMEM((SING_HEADS * ROWS, COLS), F32)],
                flops=2 * GIGA, name='trans_fwd')(z, w_up, w_down, w_pb.T)


def trans_bwd_kernel(z_ref, z5_ref, dz_ref, db_ref, wu_ref, wd_ref, wpt_ref, dzo_ref, dwr_ref, dwd_ref, dwpt_ref, dwu_ref, scr_ref):
    dwu_ref[...] = jnp.zeros_like(dwu_ref)
    dwd_ref[...] = jnp.zeros_like(dwd_ref)
    dwpt_ref[...] = jnp.zeros_like(dwpt_ref)
    scr_ref[...] = db_ref[...].astype(F32)

    def step(t):
        n5, r5 = norm_parts(z5_ref[chunk_ds(t), :].astype(F32))
        n5b = n5.astype(BF16)
        dn5 = []
        for r in range(STEP_ROWS):
            db = scr_ref[pl.ds(t * STEP_ROWS + r, SING_HEADS, stride=ROWS), :].astype(BF16)
            dwpt_ref[...] += dot_nn(db, n5b[r * COLS:(r + 1) * COLS])
            dn5.append(dot_tn(db, wpt_ref[...]))
        dz = dz_ref[chunk_ds(t), :].astype(F32) + norm_back(cat0(dn5), n5, r5)
        dzb = dz.astype(BF16)
        nhat, r_std = norm_parts(z_ref[chunk_ds(t), :].astype(F32))
        nb = nhat.astype(BF16)
        hid = dot_nn(nb, wu_ref[...])
        h1, h2 = hid[:, :4 * CH], hid[:, 4 * CH:]
        sg = jax.nn.sigmoid(h1)
        a1 = h1 * sg
        d_act = dot_nt(dzb, wd_ref[...])
        dwd_ref[...] += dot_tn((a1 * h2).astype(BF16), dzb)
        dhid = cat1([d_act * h2 * (sg + a1 * (1.0 - sg)), d_act * a1]).astype(BF16)
        dwu_ref[...] += dot_tn(nb, dhid)
        dn = dot_nt(dhid, wu_ref[...])
        dzo_ref[chunk_ds(t), :] = (dz + norm_back(dn, nhat, r_std)).astype(BF16)

    loop(ROWS // STEP_ROWS, step)
    store_rows(dwr_ref, dwu_ref[...], 8)


def trans_bwd(z, z5, dz, db, w_up, w_down, w_pb):
    return call(trans_bwd_kernel,
                [sds((N_POS, CH), BF16), sds((8 * CH, CH), F32), sds((4 * CH, CH), F32), sds((SING_HEADS, CH), F32)],
                [pltpu.VMEM((CH, 8 * CH), F32), pltpu.VMEM((SING_HEADS * ROWS, COLS), F32)],
                flops=6 * GIGA, name='trans_bwd')(z, z5, dz, db, w_up, w_down, w_pb.T)


def load_row(ref, i, blocked):
    if not blocked:
        return ref[chunk_ds(i, COLS), :]
    return cat0([ref[pl.ds(pl.multiple_of(s * ROWS * ROWS + i * ROWS, ROWS), ROWS), :] for s in range(GRP)])


def load_rows(ref, t, blocked):
    if not blocked:
        return ref[chunk_ds(t), :]
    return cat0([load_row(ref, t * STEP_ROWS + r, True) for r in range(STEP_ROWS)])


def put_strided(scr_ref, i, value):
    scr_ref[pl.ds(i, COLS, stride=ROWS), :] = value


def get_strided(scr_ref, i):
    return scr_ref[pl.ds(i, COLS, stride=ROWS), :]


def get_four(scr_ref, t):
    return cat1([get_strided(scr_ref, t * FOUR + r) for r in range(FOUR)])


def cast_out(scr_ref, o_ref):
    def step(t):
        o_ref[chunk_ds(t, 256), :] = scr_ref[chunk_ds(t, 256), :].astype(BF16)

    loop(N_POS // 256, step)


def group_rows(ref, c):
    return cat0([ref[s, chunk_ds(c, ROWS), :] for s in range(GRP)])


def make_proj(n_out, blocked):
    def kernel(z_ref, wt_ref, *rest):
        outs, scrs = rest[:n_out], rest[n_out:]

        def step(t):
            z = cat0([load_row(z_ref, t * FOUR + r, blocked) for r in range(FOUR)]).astype(F32)
            nhat, _ = norm_parts(z)
            pt = dot_nt(wt_ref[...], nhat.astype(BF16))
            for m in range(n_out):
                val = jax.nn.sigmoid(pt[(2 * m + 1) * CH:(2 * m + 2) * CH]) * pt[2 * m * CH:(2 * m + 1) * CH]
                for r in range(FOUR):
                    put_strided(scrs[m], t * FOUR + r, val[:, r * COLS:(r + 1) * COLS])

        loop(ROWS // FOUR, step)
        for m in range(n_out):
            cast_out(scrs[m], outs[m])

    return kernel


def mul_proj(z, wt, blocked=False):
    n_out = wt.shape[0] // (2 * CH)
    return call(make_proj(n_out, blocked), [sds((N_POS, CH), BF16)] * n_out, [pltpu.VMEM((N_POS, CH), F32)] * n_out,
                flops=GIGA, name='mul_proj')(z, wt)


def start_turn(rest):
    me = lax.axis_index(GROUP_AXIS)
    greet(me)
    out_ref, scr_ref, stage_ref, send, recv = rest
    return Turn(me, scr_ref, stage_ref, out_ref, send, recv)


def make_mix(outgoing):
    def kernel(left_ref, right_ref, z_ref, wg_ref, wo_ref, x_ref, o_ref, *rest):
        turn = start_turn(rest) if outgoing else None

        def mix(c):
            a = left_ref[chunk_ds(c, ROWS), :]
            b = group_rows(right_ref, c)
            x_ref[chunk_ds(c, ROWS), :] = dot_nt(a, b) if outgoing else dot_nn(a, b)

        loop(CH, mix, 8)

        def step(t):
            x = get_four(x_ref, t)
            xb = col_norm(x)[0].astype(BF16)
            z = z_ref[chunk_ds(t, WIDE), :].astype(F32)
            nhat, _ = norm_parts(z)
            gate = jax.nn.sigmoid(dot_nn(nhat.astype(BF16), wg_ref[...]))
            out = z + gate * dot_tn(xb, wo_ref[...])
            if outgoing:
                for r in range(FOUR):
                    put_strided(turn.scr, t * FOUR + r, out[r * COLS:(r + 1) * COLS])
            o_ref[chunk_ds(t, WIDE), :] = out.astype(BF16)

        if outgoing:
            await_group()
        halves(ROWS // FOUR, step, turn)

    return kernel


def mul_mix(left, right_all, z, w_gate, w_out, outgoing):
    outs = [sds((N_POS, COLS), F32), sds((N_POS, CH), BF16)]
    scr = []
    if outgoing:
        outs.append(sds(TURNED, BF16))
        scr = turn_scratch()
    return call(make_mix(outgoing), outs, scr, flops=3 * GIGA, name='mul_mix', comm=7 if outgoing else None)(left, right_all, z, w_gate, w_out)


def make_post_bwd(outgoing):
    def kernel(dz_ref, x_ref, z_ref, wg_ref, wo_ref, dx_ref, dgl_ref, dwo_ref, *rest):
        scr_ref, rest = rest[-1], rest[:-1]
        turn = start_turn(rest) if outgoing else None
        dwo_ref[...] = jnp.zeros_like(dwo_ref)

        def step(t):
            x = get_four(x_ref, t)
            xhat, r = col_norm(x)
            xb = xhat.astype(BF16)
            nhat, _ = norm_parts(z_ref[chunk_ds(t, WIDE), :].astype(F32))
            gate = jax.nn.sigmoid(dot_nn(nhat.astype(BF16), wg_ref[...]))
            du = dz_ref[chunk_ds(t, WIDE), :].astype(F32)
            dy = (gate * du).astype(BF16)
            dgl_ref[chunk_ds(t, WIDE), :] = (dot_tn(xb, wo_ref[...]) * du * gate * (1.0 - gate)).astype(BF16)
            dwo_ref[...] += dot_nn(xb, dy)
            dn = dot_nt(wo_ref[...], dy)
            dx = r * (dn - col_mean(dn) - xhat * col_mean(dn * xhat))
            for r in range(FOUR):
                part = dx[:, r * COLS:(r + 1) * COLS]
                put_strided(scr_ref, t * FOUR + r, part)
                if outgoing:
                    put_strided(turn.scr, t * FOUR + r, part.T)

        if outgoing:
            await_group()
        halves(ROWS // FOUR, step, turn)
        cast_out(scr_ref, dx_ref)

    return kernel


def mul_post_bwd(dz, x, z, w_gate, w_out, outgoing):
    outs = [sds((N_POS, COLS), BF16), sds((N_POS, CH), BF16), sds((CH, CH), F32)]
    scr = [pltpu.VMEM((N_POS, CH), F32)]
    if outgoing:
        outs.append(sds(TURNED, BF16))
        scr = turn_scratch() + scr
    return call(make_post_bwd(outgoing), outs, scr, flops=3 * GIGA, name='mul_post_bwd', comm=8 if outgoing else None)(dz, x, z, w_gate, w_out)


def make_pre_bwd(outgoing):
    def kernel(*refs):
        if outgoing:
            dx_ref, dxr_ref, left_ref, right_ref, z_ref, wt_ref, wg_ref, dgl_ref, dz_ref, dzo_ref, dwr_ref, dwg_ref, da_ref, db_ref, dwt_ref, scr_ref = refs

            def turn(j):
                put_strided(scr_ref, j, load_row(dxr_ref, j, True).astype(F32).T)

            loop(ROWS, turn, 2)

            def mix(c):
                da_ref[chunk_ds(c, ROWS), :] = dot_nn(dx_ref[chunk_ds(c, ROWS), :], group_rows(right_ref, c))
                db_ref[chunk_ds(c, ROWS), :] = dot_nn(scr_ref[chunk_ds(c, ROWS), :].astype(BF16), group_rows(left_ref, c))
        else:
            dx_ref, left_ref, right_ref, z_ref, wt_ref, wg_ref, dgl_ref, dz_ref, dzo_ref, dwr_ref, dwg_ref, da_ref, db_ref, dwt_ref = refs

            def mix(c):
                dx = group_rows(dx_ref, c)
                da_ref[chunk_ds(c, ROWS), :] = dot_nt(right_ref[chunk_ds(c, ROWS), :], dx)
                db_ref[chunk_ds(c, ROWS), :] = dot_nn(left_ref[chunk_ds(c, ROWS), :], dx)

        loop(CH, mix, 8)
        dwt_ref[...] = jnp.zeros_like(dwt_ref)
        dwg_ref[...] = jnp.zeros_like(dwg_ref)

        def step(t):
            nhat, r_std = norm_parts(z_ref[chunk_ds(t, WIDE), :].astype(F32))
            nb = nhat.astype(BF16)
            pt = dot_nt(wt_ref[...], nb)
            parts = []
            for m, d_ref in enumerate((da_ref, db_ref)):
                d = get_four(d_ref, t)
                val = pt[2 * m * CH:(2 * m + 1) * CH]
                sg = jax.nn.sigmoid(pt[(2 * m + 1) * CH:(2 * m + 2) * CH])
                dv = d * sg
                parts += [dv, dv * val * (1.0 - sg)]
            dpt = cat0(parts).astype(BF16)
            dgl = dgl_ref[chunk_ds(t, WIDE), :]
            dwt_ref[...] += dot_nn(dpt, nb)
            dwg_ref[...] += dot_tn(nb, dgl)
            dn = dot_tn(dpt, wt_ref[...]) + dot_nt(dgl, wg_ref[...])
            dzo_ref[chunk_ds(t, WIDE), :] = (dz_ref[chunk_ds(t, WIDE), :].astype(F32) + norm_back(dn, nhat, r_std)).astype(BF16)

        loop(ROWS // FOUR, step)
        for t in range(FOUR):
            dwr_ref[pl.ds(t, CH, stride=4), :] = dwt_ref[t * CH:(t + 1) * CH, :].T

    return kernel


def mul_pre_bwd(dx, left, right, z, wt, w_gate, dgl, dz, dx_turned=None):
    outgoing = dx_turned is not None
    args = [dx] + ([dx_turned] if outgoing else []) + [left, right, z, wt, w_gate, dgl, dz]
    scr = [pltpu.VMEM((N_POS, CH), F32)] * 2 + [pltpu.VMEM((4 * CH, CH), F32)]
    if outgoing:
        scr.append(pltpu.VMEM((N_POS, CH), F32))
    return call(make_pre_bwd(outgoing), [sds((N_POS, CH), BF16), sds((4 * CH, CH), F32), sds((CH, CH), F32)], scr,
                flops=6 * GIGA, name='mul_pre_bwd')(*args)


def gather_blocks(x):
    return lax.all_gather(x, GROUP_AXIS, axis=0)


def swap_rows(x_in):
    x_t = swap_all(x_in, 1, 0)
    return jnp.swapaxes(x_t, 0, 1).reshape(N_POS, CH)


def att_backward(z, dz, bias_all, mask_col, w_qkvg, w_tb, w_o, ending):
    dz_part, g_qkvg, g_out, db = att_bwd(z, dz, bias_all, mask_col, w_qkvg.T, w_o, ending, not ending)
    dz_new, g_bt = bias_bwd(z, dz_part, db, w_tb, ending)
    return dz_new.reshape(N_POS, CH), [g_qkvg, g_bt, g_out]


C_S = 384
SING_DIM = 24
SING_SCALE = SING_DIM ** -0.5
GRP_HEADS = SING_HEADS // GRP
GRP_W = GRP_HEADS * SING_DIM
TOKENS = 128


def store_rows(out_ref, value, tiles):
    n = value.shape[0]
    if tiles == 1:
        out_ref[...] = value
        return
    for t in range(tiles):
        out_ref[pl.ds(t, n, stride=tiles), :] = value[:, t * 128:(t + 1) * 128]


def sing_pre_kernel(s_ref, w_ref, qb_ref, qkv_ref, gate_ref):
    nhat, _ = norm_parts(s_ref[...].astype(F32))
    nb = nhat.astype(BF16)
    p_all = dot_nn(nb, w_ref[...])
    qkv_ref[:, :C_S] = (p_all[:, :C_S] + qb_ref[...].astype(F32)).astype(BF16)
    qkv_ref[:, C_S:] = p_all[:, C_S:3 * C_S].astype(BF16)
    gate_ref[...] = jax.nn.sigmoid(p_all[:, 3 * C_S:])


def sing_pre(s, w_qkvg, q_bias):
    return call(sing_pre_kernel, [sds((ROWS, 3 * C_S), BF16), sds((ROWS, C_S), F32)],
                flops=GIGA, name='sing_pre')(s, w_qkvg, q_bias[None, :])


def sing_stack(x):
    lane = lax.broadcasted_iota(jnp.int32, (TOKENS, GRP_W), 1) // SING_DIM
    x = x.astype(F32)
    return cat0([jnp.where(lane == h, x, 0.0) for h in range(GRP_HEADS)]).astype(BF16)


def sing_merge(parts):
    lane = lax.broadcasted_iota(jnp.int32, (TOKENS, GRP_W), 1) // SING_DIM
    out = jnp.where(lane == 0, parts[0], 0.0)
    for h in range(1, GRP_HEADS):
        out = jnp.where(lane == h, parts[h], out)
    return out


P_GATED, P_DMID, P_X2, P_DH, P_ACT, P_DOUT = 0, 384, 768, 1152, 4224, 5760
P_NS, P_DQ = 6144, 6528


P_ALL = 8064


def sing_fused_kernel(bias_ref, q_ref, k_ref, v_ref, gate_ref, s_ref, m_ref, wo_ref, wu_ref, wd_ref, wq_ref, ds_ref,
                      so_ref, dsi_ref, pk_ref, dbt_ref, qb_ref,
                      b_all, o_out, o_in, do_out, do_in, dq_out, dq_in, db_out, send, recv):
    me = lax.axis_index(GROUP_AXIS)
    greet(me)
    await_group()

    def block(ref):
        return lambda p: ref.at[p]

    def rows_block(ref):
        return lambda p: ref.at[pl.ds(pl.multiple_of(p * TOKENS, TOKENS), TOKENS), :]

    def start(i, src_at, dst_at):
        return Exchange(me, src_at, dst_at, send.at[i], recv.at[i])

    def lanes_of(x):
        return [x[:, g * GRP_W:(g + 1) * GRP_W] for g in range(GRP)]

    def rows_of(x):
        return [x[g * ROWS:(g + 1) * ROWS] for g in range(GRP)]

    stage = 0
    ex_bias = start(stage, rows_block(bias_ref), block(b_all))
    b_all[me] = bias_ref[pl.ds(pl.multiple_of(me * TOKENS, TOKENS), TOKENS), :]
    q, ks, vs = q_ref[...], sing_stack(k_ref[...]), sing_stack(v_ref[...])
    logits = dot_nt(ks, q) * SING_SCALE
    mask = m_ref[...]
    ex_bias.arrive()
    probs = []
    for h in range(GRP_HEADS):
        b = cat0([b_all[g, h * ROWS:(h + 1) * ROWS, :] for g in range(GRP)]).astype(F32)
        probs.append(softmax_cols(logits[h * TOKENS:(h + 1) * TOKENS] + b + mask))
    pb = [p.astype(BF16) for p in probs]
    for g, x in enumerate(rows_of(dot_tn(cat0(pb), vs))):
        o_out[g] = x
    stage += 1
    ex_o = start(stage, block(o_out), block(o_in))
    o_in[me] = o_out[me]
    gate, s = gate_ref[...], s_ref[...].astype(F32)
    ds = ds_ref[...]
    d_act = dot_nt(ds, wd_ref[...])
    n_s, r_s = norm_parts(s)
    ex_o.arrive()
    att = cat1([o_in[g] for g in range(GRP)])
    gated = (gate * att).astype(BF16)
    s_mid = (s + dot_nn(gated, wo_ref[...])).astype(BF16).astype(F32)
    nhat, r_std = norm_parts(s_mid)
    nb = nhat.astype(BF16)
    hid = dot_nn(nb, wu_ref[...])
    h1, h2 = hid[:, :4 * C_S], hid[:, 4 * C_S:]
    sg = jax.nn.sigmoid(h1)
    a1 = h1 * sg
    dhid = cat1([d_act * h2 * (sg + a1 * (1.0 - sg)), d_act * a1]).astype(BF16)
    dsm = ds.astype(F32) + norm_back(dot_nt(dhid, wu_ref[...]), nhat, r_std)
    dsmb = dsm.astype(BF16)
    d_gated = dot_nt(dsmb, wo_ref[...])
    for g, x in enumerate(lanes_of((d_gated * gate).astype(BF16))):
        do_out[g] = x
    stage += 1
    ex_do = start(stage, block(do_out), block(do_in))
    do_in[me] = do_out[me]
    act = (a1 * h2).astype(BF16)
    so_ref[...] = (s_mid + dot_nn(act, wd_ref[...])).astype(BF16)
    dgl = (d_gated * att * gate * (1.0 - gate)).astype(BF16)
    for at, x in ((P_GATED, gated), (P_DMID, dsmb), (P_X2, nb), (P_DH, dhid), (P_ACT, act), (P_DOUT, ds), (P_NS, n_s.astype(BF16))):
        pk_ref[:, at:at + x.shape[1]] = x
    ex_do.arrive()
    do = cat0([do_in[g] for g in range(GRP)])
    dp = dot_nt(vs, do)
    dsb, dk, dv = [], [], []
    for h in range(GRP_HEADS):
        d = dp[h * TOKENS:(h + 1) * TOKENS]
        dlog = probs[h] * (d - col_sum(probs[h] * d))
        for g, x in enumerate(rows_of(dlog.astype(BF16))):
            db_out[g, h * ROWS:(h + 1) * ROWS, :] = x
        dsb.append((dlog * SING_SCALE).astype(BF16))
    stage += 1
    ex_db = start(stage, block(db_out), rows_block(dbt_ref))
    rows_block(dbt_ref)(me)[...] = db_out[me]
    for h in range(GRP_HEADS):
        dk.append(dot_nn(dsb[h], q))
        dv.append(dot_nn(pb[h], do))
    for t, x in enumerate((dot_tn(cat0(dsb), ks), sing_merge(dk), sing_merge(dv))):
        for g, y in enumerate(rows_of(x.astype(BF16))):
            dq_out[g, t] = y
    stage += 1
    ex_dq = start(stage, block(dq_out), block(dq_in))
    dq_in[me] = dq_out[me]
    ex_dq.arrive()
    dp_all = cat1([dq_in[g, t] for t in range(3) for g in range(GRP)] + [dgl])
    pk_ref[:, P_DQ:] = dp_all
    dsi_ref[...] = (dsm + norm_back(dot_nt(dp_all, wq_ref[...]), n_s, r_s)).astype(BF16)
    qb = col_sum(dp_all[:, :C_S].astype(F32))
    qb_ref[...] = cat0([qb[:, t * CH:(t + 1) * CH] for t in range(3)])
    ex_db.arrive()
    for ex in (ex_bias, ex_o, ex_do, ex_db, ex_dq):
        ex.leave()


def sing_fused(*args):
    vm = pl.BlockSpec(memory_space=pltpu.VMEM)
    dma = pltpu.SemaphoreType.DMA
    piece = (GRP, ROWS, GRP_W)
    triple = (GRP, 3, ROWS, GRP_W)
    outs = (sds((ROWS, C_S), BF16), sds((ROWS, C_S), BF16), sds((ROWS, P_ALL), BF16), sds((GRP * TOKENS, TOKENS), BF16), sds((3, CH), F32))
    sems = dma((5, len(OFFSETS)))
    return pl.pallas_call(
        sing_fused_kernel, out_shape=outs, in_specs=[vm] * len(args), out_specs=(vm,) * len(outs),
        scratch_shapes=[pltpu.VMEM((GRP, TOKENS, TOKENS), BF16), pltpu.VMEM(piece, F32), pltpu.VMEM(piece, F32),
                        pltpu.VMEM(piece, BF16), pltpu.VMEM(piece, BF16), pltpu.VMEM(triple, BF16), pltpu.VMEM(triple, BF16),
                        pltpu.VMEM((GRP, TOKENS, TOKENS), BF16), sems, sems],
        compiler_params=pltpu.CompilerParams(collective_id=2, has_side_effects=True), name='sing_fused',
        cost_estimate=pl.CostEstimate(flops=2 * GIGA, bytes_accessed=NOMINAL_BYTES, transcendentals=0),
    )(*args)


QKVG, PROJ, UP, DOWN = (4360, 12, 3), (8987, 3, 1), (10139, 24, 6), (19355, 3, 3)
KEPT = (((QKVG, 0, 136),), ((QKVG, 128, 384), (PROJ, 0, 384), (UP, 0, 80)), ((UP, 72, 328),), ((UP, 320, 384), (DOWN, 0, 384)))
W_ROWS = 1632


def kept_blocks(d):
    at = 0
    for weight, lo, hi in KEPT[d]:
        for t in range(weight[-1]):
            yield weight, lo, hi, t, at
            at += hi - lo


def sing_wgrad_kernel(m_ref, o_ref):
    k = lax.axis_index(GROUP_AXIS)

    def lanes(base, tiles, idx):
        width = tiles * CH
        return m_ref[:, pl.ds(pl.multiple_of(base + idx * width, CH), width)]

    def whole(base):
        return m_ref[:, base:base + C_S]

    grads = {
        QKVG: dot_tn(whole(P_NS), lanes(P_DQ, QKVG[-1], k)),
        PROJ: dot_tn(whole(P_GATED), lanes(P_DMID, 1, jnp.minimum(k, 2))),
        UP: dot_tn(whole(P_X2), lanes(P_DH, UP[-1], k)),
        DOWN: dot_tn(lanes(P_ACT, DOWN[-1], k), whole(P_DOUT)),
    }
    for d in range(GRP):
        end = 0
        for weight, lo, hi, t, at in kept_blocks(d):
            end = at + hi - lo
            o_ref[d, at:end, :] = grads[weight][lo:hi, t * CH:(t + 1) * CH]
        if end < W_ROWS:
            o_ref[d, end:, :] = jnp.zeros((W_ROWS - end, CH), F32)


def sing_wgrad(packed_all):
    return call(sing_wgrad_kernel, [sds((4, W_ROWS, 128), F32)], flops=GIGA, name='sing_wgrad')(packed_all)


PART = 766816
OUT_ROWS = 5992
SHIFT_ROWS = 56
SMALL_AT = ((0, 2048, 4, 24), (0, 2692, 4, 32), (1, 2978, 3, 0), (1, 2981, 16, 8))
LATE_ROWS = 1536
PIECE = LATE_ROWS // 16
LATE_SIZES = (512, 128, 128, 512, 128, 128)
EARLY_SIZES = (512, 128, 512, 128, 1024, 512)
EARLY_AT = (1536, 2052, 2180, 2696, 2824, 3848)


def finish_kernel(*refs):
    late_refs, (g_ref, p_ref, small_ref, o_ref, w_ref, x_ref, buf_ref, sum_ref, copy_sem, send1, recv1, send2, recv2) = refs[:6], refs[6:]
    d, k = lax.axis_index(BATCH_AXIS), lax.axis_index(GROUP_AXIS)
    me = 4 * d + k
    row, fills = 0, []
    for i, ref in enumerate(late_refs):
        fills.append(pltpu.make_async_copy(ref, x_ref.at[pl.ds(row, LATE_SIZES[i]), :], copy_sem.at[i]))
        row += LATE_SIZES[i]
    for c in fills:
        c.start()
    barrier = pltpu.get_barrier_semaphore()

    def device(p):
        return {BATCH_AXIS: p // 4, GROUP_AXIS: lax.rem(p, 4)}

    def piece(p):
        return pl.ds(pl.multiple_of(p * PIECE, PIECE), PIECE)

    for off in range(1, N_DEV):
        pl.semaphore_signal(barrier, inc=1, device_id=device(lax.rem(me + off, N_DEV)), device_id_type=MESH_ID)
    for c in fills:
        c.wait()
    pl.semaphore_wait(barrier, 15)
    first = []
    for off in range(1, N_DEV):
        p = lax.rem(me + off, N_DEV)
        c = pltpu.make_async_remote_copy(
            src_ref=x_ref.at[piece(p), :], dst_ref=buf_ref.at[off - 1], send_sem=send1.at[off - 1], recv_sem=recv1.at[off - 1],
            device_id=device(p), device_id_type=MESH_ID)
        c.start()
        first.append(c)

    def lay_out(part):
        begin = part * PART // 128
        lanes_off = part * PART % 128
        for weight, lo, hi, t, at in kept_blocks(part):
            base, tiles, own = weight
            for k in range(GRP):
                if weight == DOWN:
                    first_row = base + own * CH * k * tiles + t - begin
                else:
                    first_row = base + own * k + t - begin
                    if own * k + t >= tiles:
                        continue
                r0 = max(lo, -(first_row // tiles))
                r1 = min(hi, (OUT_ROWS - first_row) // tiles + 1)
                src = at + r0 - lo
                w_ref[pl.ds(first_row + r0 * tiles, r1 - r0, stride=tiles), :] = g_ref[k, src:src + r1 - r0, :]
        if part:
            lane = lax.broadcasted_iota(jnp.int32, (SHIFT_ROWS, CH), 1)
            for i in range(OUT_ROWS // SHIFT_ROWS):
                rows = slice(i * SHIFT_ROWS, (i + 1) * SHIFT_ROWS)
                a = pltpu.roll(w_ref[rows, :], CH - lanes_off, 1)
                b = pltpu.roll(w_ref[rows.start + 1:rows.stop + 1, :], CH - lanes_off, 1)
                o_ref[rows, :] = jnp.where(lane < CH - lanes_off, a, b)
        else:
            o_ref[LATE_ROWS:, :] = w_ref[LATE_ROWS:OUT_ROWS, :]

    for part in range(GRP):
        @pl.when(d == part)
        def _():
            if part == 0:
                src = 0
                for n, at in zip(EARLY_SIZES, EARLY_AT):
                    w_ref[at:at + n, :] = p_ref[src:src + n, :]
                    src += n
            for own, at, n, src in SMALL_AT:
                if own == part:
                    w_ref[at:at + n, :] = small_ref[src:src + n, :]
            lay_out(part)

    for c in first:
        c.wait_recv()
    total = x_ref[piece(me), :]
    for i in range(15):
        total += buf_ref[i]
    sum_ref[...] = total

    def second(k, src):
        return pltpu.make_async_remote_copy(
            src_ref=sum_ref, dst_ref=o_ref.at[piece(src), :], send_sem=send2.at[k], recv_sem=recv2.at[src],
            device_id={BATCH_AXIS: 0, GROUP_AXIS: k}, device_id_type=MESH_ID)

    for k in range(FOUR):
        @pl.when(me != k)
        def _():
            second(k, me).start()

    @pl.when(d == 0)
    def _():
        o_ref[piece(me), :] = total

    for k in range(FOUR):
        @pl.when(me != k)
        def _():
            second(k, me).wait_send()

    @pl.when(d == 0)
    def _():
        for off in range(1, N_DEV):
            second(0, lax.rem(me + off, N_DEV)).wait_recv()

    for c in first:
        c.wait_send()


def finish(late, g_all, early, small):
    vm = pl.BlockSpec(memory_space=pltpu.VMEM)
    dma = pltpu.SemaphoreType.DMA
    return pl.pallas_call(
        finish_kernel, out_shape=sds((OUT_ROWS, 128), F32), in_specs=[vm] * 9, out_specs=vm,
        scratch_shapes=[pltpu.VMEM((6016, 128), F32), pltpu.VMEM((LATE_ROWS, 128), F32), pltpu.VMEM((15, PIECE, 128), F32),
                        pltpu.VMEM((PIECE, 128), F32), dma((6,)), dma((15,)), dma((15,)), dma((4,)), dma((16,))],
        compiler_params=pltpu.CompilerParams(collective_id=1, has_side_effects=True), name='finish',
        cost_estimate=pl.CostEstimate(flops=GIGA, bytes_accessed=NOMINAL_BYTES, transcendentals=0),
    )(*late, g_all, early, small)


def flat_cols(x):
    return x.T.reshape(x.shape)


def to_heads(x, n):
    x = x.reshape(ROWS, n, GRP, GRP_W)
    x = swap_all(jnp.transpose(x, (2, 1, 0, 3)), 0, 0)
    x = jnp.transpose(x, (1, 0, 2, 3)).reshape(n, TOKENS, GRP_W)
    return [x[t] for t in range(n)]


def device_step(single_blk, pair_blk, mask_blk, d_single_blk, d_pair_blk, *weights):
    (w1_in, w1_gate, w1_out, w2_in, w2_gate, w2_out, st_qkvg, st_bias, st_proj, en_qkvg,
     en_bias, en_proj, p_up, p_down, s_qkvg, s_qbias, s_pbias, s_proj, s_up, s_down) = weights
    s_rows = single_blk[0]
    z_zero = pair_blk[0].reshape(N_POS, CH)
    mask_bias = (mask_blk[0].astype(jnp.float32) - 1.0) * MASK_PENALTY
    mask_col = mask_bias[:, None]
    wt_out, wt_in = w1_in.T, w2_in.T
    right_out = mul_proj(z_zero, wt_out[HALF:])
    right_out_all = gather_blocks(right_out)
    left_out = mul_proj(z_zero, wt_out[:HALF])
    x_out, z_one, z_one_turned = mul_mix(left_out, right_out_all, z_zero, w1_gate, w1_out, True)
    right_in = mul_proj(z_one, wt_in[HALF:])
    right_in_all = gather_blocks(right_in)
    zt_one = z_one_turned.reshape(N_POS, CH)
    left_in = mul_proj(z_one, wt_in[:HALF])
    left_in_t = mul_proj(zt_one, wt_in[:HALF], True)
    x_in, z_two = mul_mix(left_in_t, right_in_all, z_one, w2_gate, w2_out, False)
    left_out, z_two = lax.optimization_barrier((left_out, z_two))
    left_out_all = gather_blocks(left_out)
    z_three_turned, bias_st = att_fwd(z_two, st_bias, mask_col, st_qkvg.T, st_proj, False)
    zt_three = z_three_turned.reshape(N_POS, CH)
    d_pair, zt_three = lax.optimization_barrier((d_pair_blk[0], zt_three))
    dzt_out = swap_rows(d_pair)
    zt_four, bias_en = att_fwd(zt_three, en_bias, mask_col, en_qkvg.T, en_proj, True)
    s_qkv, s_gate = sing_pre(s_rows, s_qkvg, s_qbias)
    qkv_heads = to_heads(s_qkv, 3)
    zt_four, left_out_all, dzt_out, qkv_heads = lax.optimization_barrier((zt_four, left_out_all, dzt_out, qkv_heads))
    zt_five, bias_t = trans_fwd(zt_four, p_up, p_down, s_pbias)
    s_out, ds_in, packed, d_bias_t, g_qb = sing_fused(
        bias_t, *qkv_heads, s_gate, s_rows, mask_col, s_proj, s_up, s_down, s_qkvg, d_single_blk[0])
    packed, zt_five, d_bias_t, dzt_out = lax.optimization_barrier((packed, zt_five, d_bias_t, dzt_out))
    packed_all = gather_rows(packed)
    z_five = swap_rows(zt_five.reshape(ROWS, COLS, CH))
    dzt_four, g_pup, g_pdown, g_pbt = trans_bwd(zt_four, zt_five, dzt_out, d_bias_t, p_up, p_down, s_pbias)
    windows = sing_wgrad(packed_all)
    dzt_four, windows = lax.optimization_barrier((dzt_four, windows))
    piece = lax.psum_scatter(windows.reshape(4 * W_ROWS, 128), BATCH_AXIS, scatter_dimension=0, tiled=True)
    dz_three, end_grads = att_backward(zt_three, dzt_four, bias_en, mask_col, en_qkvg, en_bias, en_proj, True)
    dz_three, piece = lax.optimization_barrier((dz_three, piece))
    pieces = gather_rows(piece)
    dz_two, start_grads = att_backward(z_two, dz_three, bias_st, mask_col, st_qkvg, st_bias, st_proj, False)
    dz_two, pieces, z_five = lax.optimization_barrier((dz_two, pieces, z_five))
    dx_in, dgl_in, g_in_out = mul_post_bwd(dz_two, x_in, z_one, w2_gate, w2_out, False)
    dx_all = gather_blocks(dx_in)
    five = jnp.zeros((5, 128), F32)
    early = cat0([start_grads[0], start_grads[2], end_grads[0], end_grads[2], g_pup, g_pdown, g_qb, five, g_pbt,
                             start_grads[1], five[:4], end_grads[1], five[:4]])
    dx_all, early = lax.optimization_barrier((dx_all, early))
    early = lax.psum(early, (BATCH_AXIS, GROUP_AXIS))
    tail = early[sum(EARLY_SIZES):]
    small = cat0([tail[:8], flat_cols(tail[8:24]), flat_cols(tail[24:28]), five[:4], flat_cols(tail[32:36]), five[:4]])
    dz_one, g_in_in, g_in_gate = mul_pre_bwd(dx_all, left_in, right_in, z_one, wt_in, w2_gate, dgl_in, dz_two)
    dx_out, dgl_out, g_out_out, dx_turned = mul_post_bwd(dz_one, x_out, z_zero, w1_gate, w1_out, True)
    dz_zero, g_out_in, g_out_gate = mul_pre_bwd(dx_out, left_out_all, right_out_all, z_zero, wt_out, w1_gate, dgl_out, dz_one, dx_turned.reshape(N_POS, CH))
    late = (g_out_in, g_out_gate, g_out_out, g_in_in, g_in_gate, g_in_out)
    grad_flat = finish(late, pieces.reshape(4, W_ROWS, 128), early, small).reshape(-1)[:PART]
    z_five = z_five.reshape(ROWS, COLS, CH)
    dz_zero = dz_zero.reshape(ROWS, COLS, CH)
    return s_out[None], z_five[None], ds_in[None], dz_zero[None], grad_flat


def solution(mesh):
    spec_single = P(BATCH_AXIS, GROUP_AXIS, None)
    spec_pair = P(BATCH_AXIS, GROUP_AXIS, None, None)
    spec_mask = P(BATCH_AXIS, None)

    def block_fn(single_rep, pair_rep, token_mask, d_single_out, d_pair_out, *weights):
        in_specs = (spec_single, spec_pair, spec_mask, spec_single, spec_pair) + tuple(P() for w_item in weights)
        out_specs = (spec_single, spec_pair, spec_single, spec_pair, P(BATCH_AXIS))
        mapped = jax.shard_map(device_step, mesh=mesh, in_specs=in_specs, out_specs=out_specs, check_vma=False)
        return mapped(single_rep, pair_rep, token_mask, d_single_out, d_pair_out, *weights)

    return block_fn
```

```python
import functools
import jax
import jax.numpy as jnp
from jax import lax
from jax.experimental import pallas as pl
from jax.experimental.pallas import tpu as pltpu
from jax.sharding import PartitionSpec as P

BATCH_AXIS = 'dp'
GROUP_AXIS = 'dap'
NORM_EPS = 1e-5
MASK_PENALTY = 1.0e9


def gather_rows(x_in):
    return lax.all_gather(x_in, GROUP_AXIS, axis=0, tiled=True)


F32 = jnp.float32
NOMINAL_BYTES = 4 << 20
GIGA = 1 << 30
BF16 = jnp.bfloat16
ROWS = 32
COLS = 128
CH = 128
HALF = 2 * CH
N_POS = ROWS * COLS
TRI_HEADS = 4
GRP = 4
OFFSETS = (1, 2, 3)
MESH_ID = pl.DeviceIdType.MESH
FOUR = 4
N_DEV = 16
WIDE = FOUR * COLS
TRI_DIM = 32
TRI_SCALE = TRI_DIM ** -0.5
STEP_ROWS = 4
CHUNK = STEP_ROWS * COLS


def dot_nn(a, b):
    return lax.dot_general(a, b, (((1,), (0,)), ((), ())), preferred_element_type=F32)


def dot_nt(a, b):
    return lax.dot_general(a, b, (((1,), (1,)), ((), ())), preferred_element_type=F32)


def dot_tn(a, b):
    return lax.dot_general(a, b, (((0,), (0,)), ((), ())), preferred_element_type=F32)


def cat0(xs):
    return jnp.concatenate(xs, axis=0)


def cat1(xs):
    return jnp.concatenate(xs, axis=1)


def loop(count, step, unroll=1):
    def body(i, carry):
        step(i)
        return carry

    lax.fori_loop(0, count, body, 0, unroll=unroll)


def col_mean(x):
    return jnp.mean(x, axis=0, keepdims=True)


def col_sum(x):
    return jnp.sum(x, axis=0, keepdims=True)


def row_mean(x):
    return jnp.mean(x, axis=-1, keepdims=True)


def softmax_cols(x):
    e = jnp.exp(x - jnp.max(x, axis=0, keepdims=True))
    return e * (1.0 / col_sum(e))


def col_norm(x):
    c = x - col_mean(x)
    r = lax.rsqrt(col_mean(c * c) + NORM_EPS)
    return c * r, r


def swap_all(x, split, join):
    return lax.all_to_all(x, GROUP_AXIS, split, join, tiled=True)


def norm_parts(x):
    c = x - row_mean(x)
    r = lax.rsqrt(row_mean(c * c) + NORM_EPS)
    return c * r, r


def norm_back(dn, nhat, r):
    return r * (dn - row_mean(dn) - nhat * row_mean(dn * nhat))


def chunk_ds(t, size=CHUNK):
    return pl.ds(pl.multiple_of(t * size, size), size)


def call(kernel, out_shape, scratch=(), flops=0, name=None, comm=None):
    n_out = len(out_shape)
    vm = pl.BlockSpec(memory_space=pltpu.VMEM)

    def run(*args):
        return pl.pallas_call(
            kernel, out_shape=tuple(out_shape), in_specs=[vm] * len(args), out_specs=tuple([vm] * n_out),
            scratch_shapes=list(scratch), name=name,
            compiler_params=pltpu.CompilerParams(collective_id=comm, has_side_effects=comm is not None),
            cost_estimate=pl.CostEstimate(flops=flops, bytes_accessed=NOMINAL_BYTES, transcendentals=0),
        )(*args)

    def run_one(*args):
        return run(*args)[0]

    return run if n_out > 1 else run_one


def sds(shape, dtype):
    return jax.ShapeDtypeStruct(shape, dtype)


def greet(me):
    sem = pltpu.get_barrier_semaphore()
    for off in OFFSETS:
        pl.semaphore_signal(sem, inc=1, device_id={GROUP_AXIS: lax.rem(me + off, GRP)}, device_id_type=MESH_ID)


def await_group():
    pl.semaphore_wait(pltpu.get_barrier_semaphore(), len(OFFSETS))


class Exchange:
    def __init__(self, me, src_at, dst_at, send_sem, recv_sem):
        self.copies = []
        for i, off in enumerate(OFFSETS):
            dest = lax.rem(me + off, GRP)
            self.copies.append(pltpu.make_async_remote_copy(
                src_ref=src_at(dest), dst_ref=dst_at(me), send_sem=send_sem.at[i], recv_sem=recv_sem.at[i],
                device_id={GROUP_AXIS: dest}, device_id_type=MESH_ID))
        for c in self.copies:
            c.start()

    def arrive(self):
        for c in self.copies:
            c.wait_recv()

    def leave(self):
        for c in self.copies:
            c.wait_send()


PACK = 8
CHUNKS = 4
CHUNK_ROWS = N_POS // CHUNKS


class Gather:
    def __init__(self, me, own_ref, all_ref, send, recv):
        self.all, self.send, self.recv = all_ref, send, recv
        self.partner, self.across = me + 1 - 2 * lax.rem(me, 2), lax.rem(me + 2, GRP)
        self.far = [self.copy(own_ref.at[self.rows(c), :], me, self.across, 0, c) for c in range(CHUNKS)]
        self.near = [self.copy(own_ref.at[self.rows(c), :], me, self.partner, 1, c) for c in range(CHUNKS)]
        self.passed = []
        for c in self.far + self.near:
            c.start()
        all_ref[me] = own_ref[...]

    def rows(self, c):
        return pl.ds(c * CHUNK_ROWS, CHUNK_ROWS)

    def copy(self, src, slot, dest, kind, c):
        return pltpu.make_async_remote_copy(
            src_ref=src, dst_ref=self.all.at[slot, self.rows(c), :], send_sem=self.send.at[kind, c], recv_sem=self.recv.at[kind, c],
            device_id={GROUP_AXIS: dest}, device_id_type=MESH_ID)

    def each(self, work):
        for c in range(CHUNKS + 1):
            if c < CHUNKS:
                self.far[c].wait_recv()
                self.passed.append(self.copy(self.all.at[self.across, self.rows(c), :], self.across, self.partner, 2, c))
                self.passed[c].start()
            if c:
                self.near[c - 1].wait_recv()
                self.passed[c - 1].wait_recv()
                loop(CH // CHUNKS, lambda k: work(k + (c - 1) * (CH // CHUNKS)), PACK)

    def pass_on(self):
        for c in range(CHUNKS):
            self.far[c].wait_recv()
            self.passed.append(self.copy(self.all.at[self.across, self.rows(c), :], self.across, self.partner, 2, c))
            self.passed[c].start()

    def arrive(self):
        for c in self.near + self.passed:
            c.wait_recv()

    def leave(self):
        for c in self.far + self.near + self.passed:
            c.wait_send()


def gather_sems():
    sems = pltpu.SemaphoreType.DMA((3, CHUNKS))
    return [sems, sems]


def own_rows(p, size=ROWS):
    return pl.ds(pl.multiple_of(p * size, size), size)


class Turn:
    def __init__(self, me, scr_ref, stage_ref, out_ref, send, recv):
        self.me, self.scr, self.stage, self.out, self.send, self.recv = me, scr_ref, stage_ref, out_ref, send, recv
        self.sent = []

    def half(self, n):
        lo = n * HALF_ROWS

        def cast(j):
            rows = self.scr[pl.ds(pl.multiple_of(j * ROWS + lo, HALF_ROWS), HALF_ROWS), :]
            self.stage[j // ROWS, lax.rem(j, ROWS), lo:lo + HALF_ROWS, :] = rows.astype(BF16)

        loop(COLS, cast, FOUR)
        part = (slice(None), slice(lo, lo + HALF_ROWS))
        self.sent.append(Exchange(self.me, lambda p: self.stage.at[(p, *part)], lambda m: self.out.at[(m, *part)], self.send.at[n], self.recv.at[n]))

    def finish(self):
        self.out[self.me] = self.stage[self.me]
        for ex in self.sent:
            ex.arrive()
            ex.leave()


TURNED = (GRP, ROWS, ROWS, CH)
HALF_ROWS = ROWS // 2


def turn_scratch():
    sems = pltpu.SemaphoreType.DMA((2, len(OFFSETS)))
    return [pltpu.VMEM((N_POS, CH), F32), pltpu.VMEM(TURNED, BF16), sems, sems]


def peer_sems():
    sems = pltpu.SemaphoreType.DMA((len(OFFSETS),))
    return [sems, sems]


ATT_STEP = 4
BWD_STEP = 4


def fill_bias(bias_ref, mask_ref, bm_ref):
    mask = mask_ref[...]
    for h in range(TRI_HEADS):
        cols = slice(h * COLS, (h + 1) * COLS)
        bm_ref[:, cols] = bias_ref[:, cols].astype(F32).T + mask


def head_rows(x, h):
    return x[h * TRI_DIM:(h + 1) * TRI_DIM]


def spread_heads(xt):
    zero = jnp.zeros((TRI_DIM, COLS), xt.dtype)
    return cat1([
        cat0([head_rows(xt, h) if g == h else zero for g in range(TRI_HEADS)])
        for h in range(TRI_HEADS)])


def probs_of(k, q_wide, bm_ref):
    x = dot_nn(k, q_wide) * TRI_SCALE + bm_ref[...]
    return softmax_cols(x)


def heads_nn(xt, wide):
    return cat0([dot_nn(head_rows(xt, h), wide[:, h * COLS:(h + 1) * COLS]) for h in range(TRI_HEADS)])


def att_fwd_kernel(ending, z_ref, wbt_ref, mask_ref, w_ref, wo_ref, *rest):
    *rest, wt_ref = rest
    wt_ref[...] = w_ref[...].T
    if ending:
        dp_ref, o_ref, bias_ref, dpt_ref, bm_ref, own_ref, send, recv, dp_send, dp_recv = rest
    else:
        o_ref, bias_ref, bm_ref, own_ref, send, recv, *rest = rest
    me = lax.axis_index(GROUP_AXIS)
    greet(me)
    turn = None if ending else Turn(me, rest[0], rest[1], o_ref, *rest[2:])

    def bias_step(t):
        nhat, _ = norm_parts(cat0([load_row(z_ref, t * PACK + r, ending) for r in range(PACK)]).astype(F32))
        nb = nhat.astype(BF16)
        b = [dot_nt(wbt_ref[...], nb[r * COLS:(r + 1) * COLS]) for r in range(PACK)]
        for h in range(TRI_HEADS):
            own_ref[chunk_ds(t, PACK), h * COLS:(h + 1) * COLS] = cat0([x[h:h + 1, :] for x in b])

    loop(ROWS // PACK, bias_step)
    bias_ref[own_rows(me), :] = own_ref[...].astype(BF16)
    await_group()
    ex = Exchange(me, lambda p: bias_ref.at[own_rows(me), :], lambda m: bias_ref.at[own_rows(m), :], send, recv)
    ex.arrive()
    if ending:
        ex_dp = Exchange(me, lambda p: dp_ref.at[:, own_rows(p), :], lambda m: dpt_ref.at[m], dp_send, dp_recv)
        dpt_ref[me] = dp_ref[:, own_rows(me), :]
    fill_bias(bias_ref, mask_ref, bm_ref)

    def step(t):
        z = cat0([load_row(z_ref, t * ATT_STEP + r, ending) for r in range(ATT_STEP)]).astype(F32)
        nhat, _ = norm_parts(z)
        nb = nhat.astype(BF16)
        qt_all = dot_nt(wt_ref[:CH, :], nb)
        k_all = dot_nt(nb, wt_ref[CH:HALF, :]).astype(BF16)
        vg_all = dot_nt(wt_ref[HALF:, :], nb)
        gate = jax.nn.sigmoid(vg_all[CH:])
        outs = []
        for r in range(ATT_STEP):
            cols = slice(r * COLS, (r + 1) * COLS)
            q_wide = spread_heads(qt_all[:, cols]).astype(BF16)
            probs = probs_of(k_all[cols], q_wide, bm_ref).astype(BF16)
            outs.append(heads_nn(vg_all[:CH, cols].astype(BF16), probs))
        gated = (gate * cat1(outs)).astype(BF16)
        out = z + dot_tn(gated, wo_ref[...])
        for r in range(ATT_STEP):
            rows = slice(r * COLS, (r + 1) * COLS)
            if turn is None:
                o_ref[chunk_ds(t * ATT_STEP + r, COLS), :] = out[rows].astype(BF16)
            else:
                put_strided(turn.scr, t * ATT_STEP + r, out[rows])

    halves(ROWS // ATT_STEP, step, turn)
    ex.leave()
    if ending:
        ex_dp.arrive()
        ex_dp.leave()


def halves(count, step, turn, filler=None):
    if turn is None:
        loop(count, step)
        return
    loop(count // 2, step)
    turn.half(0)
    loop(count // 2, lambda t: step(t + count // 2))
    turn.half(1)
    if filler:
        filler()
    turn.finish()


def att_fwd(z, w_b, mask_col, wt, w_o, d_pair=None):
    ending = d_pair is not None
    scr = [pltpu.VMEM((COLS, TRI_HEADS * COLS), F32), pltpu.VMEM((ROWS, TRI_HEADS * COLS), F32)] + peer_sems()
    outs = [sds((N_POS, CH) if ending else TURNED, BF16), sds((COLS, TRI_HEADS * COLS), BF16)]
    args = [z, w_b.T, mask_col, wt, w_o]
    if ending:
        outs.append(sds(TURNED, BF16))
        args.append(d_pair)
    return call(functools.partial(att_fwd_kernel, ending), outs, scr + (peer_sems() if ending else turn_scratch()) + [pltpu.VMEM((4 * CH, CH), BF16)],
                flops=3 * GIGA, name='att_fwd', comm=4 if ending else 3)(*args)


def att_bwd_kernel(ending, z_ref, dz_ref, bias_ref, mask_ref, w_ref, wo_ref, *rest):
    *rest, wt_ref = rest
    wt_ref[...] = w_ref[...].T
    z_blocked, dz_blocked = ending, not ending
    if ending:
        own_ref, all_ref, *rest = rest
        *rest, send, recv = rest
        me = lax.axis_index(GROUP_AXIS)
        greet(me)
        await_group()
        gather = Gather(me, own_ref, all_ref, send, recv)
    dzo_ref, dwr_ref, dwo_ref, db_ref, bm_ref, acc_ref, dwqg_ref, dwkv_ref = rest
    fill_bias(bias_ref, mask_ref, bm_ref)
    acc_ref[...] = jnp.zeros_like(acc_ref)
    dwqg_ref[...] = jnp.zeros_like(dwqg_ref)
    dwkv_ref[...] = jnp.zeros_like(dwkv_ref)
    dwo_ref[...] = jnp.zeros_like(dwo_ref)

    def step(t):
        nhat, r_std = norm_parts(cat0([load_row(z_ref, t * BWD_STEP + r, z_blocked) for r in range(BWD_STEP)]).astype(F32))
        nb = nhat.astype(BF16)
        pt_all = dot_nt(wt_ref[...], nb)
        kv_all = dot_nt(nb, wt_ref[CH:3 * CH, :]).astype(BF16)
        gate = jax.nn.sigmoid(pt_all[3 * CH:])
        dz = cat0([load_row(dz_ref, t * BWD_STEP + r, dz_blocked) for r in range(BWD_STEP)])
        d_gated = dot_nt(wo_ref[...], dz)
        d_att = d_gated * gate
        outs, dqs, dkvs = [], [], []
        for r in range(BWD_STEP):
            cols = slice(r * COLS, (r + 1) * COLS)
            q_wide = spread_heads(pt_all[:CH, cols]).astype(BF16)
            do_wide = spread_heads(d_att[:, cols]).astype(BF16)
            p = probs_of(kv_all[cols, :CH], q_wide, bm_ref)
            pb = p.astype(BF16)
            outs.append(heads_nn(pt_all[2 * CH:3 * CH, cols].astype(BF16), pb))
            dp = dot_nn(kv_all[cols, CH:], do_wide)
            ds = p * (dp - col_sum(dp * p))
            acc_ref[...] += ds
            dsb = (ds * TRI_SCALE).astype(BF16)
            dqs.append(heads_nn(pt_all[CH:2 * CH, cols].astype(BF16), dsb))
            dkvs.append(cat1([dot_nt(dsb, q_wide), dot_nt(pb, do_wide)]).astype(BF16))
        o = cat1(outs)
        gated = (gate * o).astype(BF16)
        dgl = d_gated * o * gate * (1.0 - gate)
        dqg = cat0([cat1(dqs), dgl]).astype(BF16)
        dkv = cat0(dkvs)
        dwo_ref[...] += dot_nn(gated, dz)
        dwqg_ref[...] += dot_nn(dqg, nb)
        dwkv_ref[...] += dot_tn(nb, dkv)
        dn = dot_nn(dkv, wt_ref[CH:3 * CH, :]) + dot_tn(dqg[:CH], wt_ref[:CH, :]) + dot_tn(dqg[CH:], wt_ref[3 * CH:, :])
        dzo_ref[chunk_ds(t, BWD_STEP * COLS), :] = (dz.astype(F32) + norm_back(dn, nhat, r_std)).astype(BF16)

    loop(ROWS // BWD_STEP, step)
    if ending:
        gather.pass_on()
    for h in range(TRI_HEADS):
        cols = slice(h * COLS, (h + 1) * COLS)
        db_ref[:, cols] = acc_ref[:, cols].T
    for m in range(2):
        dwr_ref[pl.ds(3 * m, CH, stride=4), :] = dwqg_ref[m * CH:(m + 1) * CH, :].T
        dwr_ref[pl.ds(1 + m, CH, stride=4), :] = dwkv_ref[:, m * CH:(m + 1) * CH]
    if ending:
        gather.arrive()
        gather.leave()


def att_bwd(z, dz, bias_all, mask_col, wt, w_o, left=None):
    ending = left is not None
    outs = [sds((N_POS, CH), BF16), sds((4 * CH, CH), F32), sds((CH, CH), F32), sds((COLS, TRI_HEADS * COLS), F32)]
    wide = pltpu.VMEM((COLS, TRI_HEADS * COLS), F32)
    scr = [wide, wide, pltpu.VMEM((HALF, CH), F32), pltpu.VMEM((CH, HALF), F32)]
    args = [z, dz, bias_all, mask_col, wt, w_o]
    if ending:
        outs = [sds((GRP, N_POS, CH), BF16)] + outs
        scr = scr + gather_sems()
        args.append(left)
    scr.append(pltpu.VMEM((4 * CH, CH), BF16))
    return call(functools.partial(att_bwd_kernel, ending), outs, scr, flops=8 * GIGA, name='att_bwd', comm=9 if ending else None)(*args)


def bias_bwd_kernel(ending, z_ref, dz_ref, db_ref, wbt_ref, dzo_ref, dwt_ref, parts_ref, send, recv, *rest):
    me = lax.axis_index(GROUP_AXIS)
    greet(me)
    turn = Turn(me, rest[0], rest[1], dzo_ref, *rest[2:]) if ending else None
    dwt_ref[...] = jnp.zeros_like(dwt_ref)
    wbt = wbt_ref[...]
    await_group()
    ex = Exchange(me, lambda p: db_ref.at[own_rows(p), :], lambda m: parts_ref.at[m], send, recv)
    parts_ref[me] = db_ref[own_rows(me), :]
    ex.arrive()

    def step(t):
        block = sum(parts_ref[g, chunk_ds(t, PACK), :] for g in range(GRP))
        nhat, r_std = norm_parts(cat0([load_row(z_ref, t * PACK + r, ending) for r in range(PACK)]).astype(F32))
        nb = nhat.astype(BF16)
        dwt = jnp.zeros((TRI_HEADS, CH), F32)
        dns = []
        for r in range(PACK):
            db = cat0([block[r:r + 1, h * COLS:(h + 1) * COLS] for h in range(TRI_HEADS)]).astype(BF16)
            dwt += dot_nn(db, nb[r * COLS:(r + 1) * COLS])
            dns.append(dot_tn(db, wbt))
        out = dz_ref[chunk_ds(t, PACK * COLS), :].astype(F32) + norm_back(cat0(dns), nhat, r_std)
        if turn is None:
            dzo_ref[chunk_ds(t, PACK * COLS), :] = out.astype(BF16)
        else:
            for r in range(PACK):
                put_strided(turn.scr, t * PACK + r, out[r * COLS:(r + 1) * COLS])
        dwt_ref[...] += dwt

    halves(ROWS // PACK, step, turn)
    ex.leave()


def bias_bwd(z, dz, db, w_b, ending):
    scr = [pltpu.VMEM((GRP, ROWS, TRI_HEADS * COLS), F32)] + peer_sems()
    out = sds(TURNED if ending else (N_POS, CH), BF16)
    return call(functools.partial(bias_bwd_kernel, ending), [out, sds((TRI_HEADS, CH), F32)],
                scr + turn_scratch() if ending else scr, flops=GIGA, name='bias_bwd', comm=6 if ending else 5,
                )(z, dz, db, w_b.T)


SING_HEADS = 16


def trans_fwd_kernel(z_ref, wu_ref, wd_ref, wpt_ref, o_ref, b_ref, turned_ref, scr_ref, turn_ref):
    def step(t):
        z = z_ref[chunk_ds(t), :].astype(F32)
        nhat, _ = norm_parts(z)
        hid = dot_nn(nhat.astype(BF16), wu_ref[...])
        h1, h2 = hid[:, :4 * CH], hid[:, 4 * CH:]
        act = (jax.nn.sigmoid(h1) * h1 * h2).astype(BF16)
        out = (z + dot_nn(act, wd_ref[...])).astype(BF16)
        o_ref[chunk_ds(t), :] = out
        for r in range(STEP_ROWS):
            put_strided(turn_ref, t * STEP_ROWS + r, out[r * COLS:(r + 1) * COLS].astype(F32))
        n5, _ = norm_parts(out.astype(F32))
        n5 = n5.astype(BF16)
        for r in range(STEP_ROWS):
            scr_ref[pl.ds(t * STEP_ROWS + r, SING_HEADS, stride=ROWS), :] = dot_nt(wpt_ref[...], n5[r * COLS:(r + 1) * COLS])

    loop(ROWS // STEP_ROWS, step)
    b_ref[...] = scr_ref[...].astype(BF16)
    cast_out(turn_ref, turned_ref)


def trans_fwd(z, w_up, w_down, w_pb):
    return call(trans_fwd_kernel, [sds((N_POS, CH), BF16), sds((SING_HEADS * ROWS, COLS), BF16), sds((N_POS, CH), BF16)],
                [pltpu.VMEM((SING_HEADS * ROWS, COLS), F32), pltpu.VMEM((N_POS, CH), F32)],
                flops=2 * GIGA, name='trans_fwd')(z, w_up, w_down, w_pb.T)


def trans_bwd_kernel(z_ref, z5_ref, dz_ref, db_ref, wu_ref, wd_ref, wpt_ref,
                     dzo_ref, dwr_ref, dwd_ref, dwpt_ref, dwu_ref, scr_ref, dzs_ref):

    def convert(t):
        dzs_ref[chunk_ds(t, WIDE), :] = dz_ref[chunk_ds(t, WIDE), :].astype(F32)

    loop(N_POS // WIDE, convert)

    def dz_row(j):
        return cat0([dzs_ref[pl.ds(g * ROWS * ROWS + j, ROWS, stride=ROWS), :] for g in range(GRP)])

    dwu_ref[...] = jnp.zeros_like(dwu_ref)
    dwd_ref[...] = jnp.zeros_like(dwd_ref)
    dwpt_ref[...] = jnp.zeros_like(dwpt_ref)
    scr_ref[...] = db_ref[...].astype(F32)

    def step(t):
        n5, r5 = norm_parts(z5_ref[chunk_ds(t), :].astype(F32))
        n5b = n5.astype(BF16)
        dn5 = []
        for r in range(STEP_ROWS):
            db = scr_ref[pl.ds(t * STEP_ROWS + r, SING_HEADS, stride=ROWS), :].astype(BF16)
            dwpt_ref[...] += dot_nn(db, n5b[r * COLS:(r + 1) * COLS])
            dn5.append(dot_tn(db, wpt_ref[...]))
        dz = cat0([dz_row(t * STEP_ROWS + r) for r in range(STEP_ROWS)]) + norm_back(cat0(dn5), n5, r5)
        dzb = dz.astype(BF16)
        nhat, r_std = norm_parts(z_ref[chunk_ds(t), :].astype(F32))
        nb = nhat.astype(BF16)
        hid = dot_nn(nb, wu_ref[...])
        h1, h2 = hid[:, :4 * CH], hid[:, 4 * CH:]
        sg = jax.nn.sigmoid(h1)
        a1 = h1 * sg
        d_act = dot_nt(dzb, wd_ref[...])
        dwd_ref[...] += dot_tn((a1 * h2).astype(BF16), dzb)
        dhid = cat1([d_act * h2 * (sg + a1 * (1.0 - sg)), d_act * a1]).astype(BF16)
        dwu_ref[...] += dot_tn(nb, dhid)
        dn = dot_nt(dhid, wu_ref[...])
        dzo_ref[chunk_ds(t), :] = (dz + norm_back(dn, nhat, r_std)).astype(BF16)

    loop(ROWS // STEP_ROWS, step)
    store_rows(dwr_ref, dwu_ref[...], PACK)


def trans_bwd(z, z5, dz, db, w_up, w_down, w_pb):
    outs = [sds((N_POS, CH), BF16), sds((8 * CH, CH), F32), sds((4 * CH, CH), F32), sds((SING_HEADS, CH), F32)]
    scr = [pltpu.VMEM((CH, 8 * CH), F32), pltpu.VMEM((SING_HEADS * ROWS, COLS), F32), pltpu.VMEM((N_POS, CH), F32)]
    return call(trans_bwd_kernel, outs, scr, flops=6 * GIGA, name='trans_bwd')(z, z5, dz, db, w_up, w_down, w_pb.T)


def load_row(ref, i, blocked):
    if not blocked:
        return ref[chunk_ds(i, COLS), :]
    return cat0([ref[pl.ds(pl.multiple_of(s * ROWS * ROWS + i * ROWS, ROWS), ROWS), :] for s in range(GRP)])


def load_rows(ref, t, blocked):
    if not blocked:
        return ref[chunk_ds(t), :]
    return cat0([load_row(ref, t * STEP_ROWS + r, True) for r in range(STEP_ROWS)])


def put_strided(scr_ref, i, value):
    scr_ref[pl.ds(i, COLS, stride=ROWS), :] = value


def get_strided(scr_ref, i):
    return scr_ref[pl.ds(i, COLS, stride=ROWS), :]


def get_four(scr_ref, t):
    return cat1([get_strided(scr_ref, t * FOUR + r) for r in range(FOUR)])


def cast_out(scr_ref, o_ref):
    def step(t):
        o_ref[chunk_ds(t, 256), :] = scr_ref[chunk_ds(t, 256), :].astype(BF16)

    loop(N_POS // 256, step)


def group_rows(ref, c):
    return cat0([ref[s, chunk_ds(c, ROWS), :] for s in range(GRP)])


def project(z_ref, wt_ref, scr_ref, out_ref, blocked):
    def step(t):
        z = cat0([load_row(z_ref, t * FOUR + r, blocked) for r in range(FOUR)]).astype(F32)
        nhat, _ = norm_parts(z)
        pt = dot_nt(wt_ref[...], nhat.astype(BF16))
        val = jax.nn.sigmoid(pt[CH:]) * pt[:CH]
        for r in range(FOUR):
            put_strided(scr_ref, t * FOUR + r, val[:, r * COLS:(r + 1) * COLS])

    loop(ROWS // FOUR, step)
    cast_out(scr_ref, out_ref)


def proj_kernel(z_ref, w_ref, o_ref, scr_ref, wt_ref):
    wt_ref[...] = w_ref[:, HALF:].T
    project(z_ref, wt_ref, scr_ref, o_ref, False)


def mul_proj(z, w):
    return call(proj_kernel, [sds((N_POS, CH), BF16)], [pltpu.VMEM((N_POS, CH), F32), pltpu.VMEM((HALF, CH), BF16)],
                flops=GIGA, name='mul_proj')(z, w)


def sing_heads(me, s_ref, w_ref, qb_ref, gate_ref, out_ref, in_ref, send, recv):
    nhat, _ = norm_parts(s_ref[...].astype(F32))
    p_all = dot_nn(nhat.astype(BF16), w_ref[...])
    gate_ref[...] = jax.nn.sigmoid(p_all[:, 3 * C_S:])
    qkv = cat1([p_all[:, :C_S] + qb_ref[...].astype(F32), p_all[:, C_S:3 * C_S]]).astype(BF16)
    for t in range(3):
        for g in range(GRP):
            at = t * C_S + g * GRP_W
            out_ref[g, t] = qkv[:, at:at + GRP_W]
    in_ref[me] = out_ref[me]
    return Exchange(me, lambda p: out_ref.at[p], lambda m: in_ref.at[m], send, recv)


def make_mix(outgoing):
    def kernel(*refs):
        turn = None
        me = lax.axis_index(GROUP_AXIS)
        greet(me)
        if outgoing:
            (zl_ref, wl_ref, own_ref, z_ref, wg_ref, wo_ref, wn_ref, x_ref, o_ref, right_ref, left_ref, turned_ref, next_ref,
             scr_ref, stage_ref, send, recv, g_send, g_recv, wt_ref) = refs
            turn = Turn(me, scr_ref, stage_ref, turned_ref, send, recv)
        else:
            (zl_ref, wl_ref, own_ref, z_ref, wg_ref, wo_ref, s_ref, wq_ref, qb_ref, x_ref, o_ref, right_ref, left_ref, gate_ref, heads_ref,
             heads_out, send, recv, g_send, g_recv, wt_ref) = refs
        await_group()
        gather = Gather(me, own_ref, right_ref, g_send, g_recv)
        ex = None if outgoing else sing_heads(me, s_ref, wq_ref, qb_ref, gate_ref, heads_out, heads_ref, send, recv)
        wt_ref[...] = wl_ref[:, :HALF].T
        project(zl_ref, wt_ref, x_ref, left_ref, not outgoing)

        def mix(c):
            a = left_ref[chunk_ds(c, ROWS), :]
            b = group_rows(right_ref, c)
            x_ref[chunk_ds(c, ROWS), :] = dot_nt(a, b) if outgoing else dot_nn(a, b)

        gather.each(mix)

        def step(t):
            x = get_four(x_ref, t)
            xb = col_norm(x)[0].astype(BF16)
            z = z_ref[chunk_ds(t, WIDE), :].astype(F32)
            nhat, _ = norm_parts(z)
            gate = jax.nn.sigmoid(dot_nn(nhat.astype(BF16), wg_ref[...]))
            out = z + gate * dot_tn(xb, wo_ref[...])
            if outgoing:
                for r in range(FOUR):
                    put_strided(turn.scr, t * FOUR + r, out[r * COLS:(r + 1) * COLS])
            o_ref[chunk_ds(t, WIDE), :] = out.astype(BF16)

        def following():
            wt_ref[...] = wn_ref[:, HALF:].T
            project(o_ref, wt_ref, scr_ref, next_ref, False)

        halves(ROWS // FOUR, step, turn, following)
        gather.leave()
        if ex is not None:
            ex.arrive()
            ex.leave()

    return kernel


def mul_mix(z_left, wt_left, right, z, w_gate, w_out, wt_next=None, single=None):
    outgoing = single is None
    flat = sds((N_POS, CH), BF16)
    outs = [sds((N_POS, COLS), F32), flat, sds((GRP, N_POS, CH), BF16), flat]
    scr = gather_sems() + [pltpu.VMEM((HALF, CH), BF16)]
    if outgoing:
        outs += [sds(TURNED, BF16), flat]
        scr = turn_scratch() + scr
    else:
        heads = (GRP, 3, ROWS, GRP_W)
        outs += [sds((ROWS, C_S), F32), sds(heads, BF16)]
        scr = [pltpu.VMEM(heads, BF16)] + peer_sems() + scr
    return call(make_mix(outgoing), outs, scr, flops=3 * GIGA, name='mul_mix', comm=7 if outgoing else 10)(z_left, wt_left, right, z, w_gate, w_out, *(single or (wt_next,)))


def make_post_bwd(outgoing):
    def kernel(dz_ref, x_ref, z_ref, wg_ref, wo_ref, dx_ref, dgl_ref, dwo_ref, *rest):
        scr_ref, rest = rest[-1], rest[:-1]
        turn = None
        if outgoing:
            me = lax.axis_index(GROUP_AXIS)
            greet(me)
            turned_ref, turn_scr, stage_ref, send, recv = rest
            turn = Turn(me, turn_scr, stage_ref, turned_ref, send, recv)
        dwo_ref[...] = jnp.zeros_like(dwo_ref)

        def step(t):
            x = get_four(x_ref, t)
            xhat, r = col_norm(x)
            xb = xhat.astype(BF16)
            nhat, _ = norm_parts(z_ref[chunk_ds(t, WIDE), :].astype(F32))
            gate = jax.nn.sigmoid(dot_nn(nhat.astype(BF16), wg_ref[...]))
            du = dz_ref[chunk_ds(t, WIDE), :].astype(F32)
            dy = (gate * du).astype(BF16)
            dgl_ref[chunk_ds(t, WIDE), :] = (dot_tn(xb, wo_ref[...]) * du * gate * (1.0 - gate)).astype(BF16)
            dwo_ref[...] += dot_nn(xb, dy)
            dn = dot_nt(wo_ref[...], dy)
            dx = r * (dn - col_mean(dn) - xhat * col_mean(dn * xhat))
            for r in range(FOUR):
                part = dx[:, r * COLS:(r + 1) * COLS]
                put_strided(scr_ref, t * FOUR + r, part)
                if outgoing:
                    put_strided(turn.scr, t * FOUR + r, part.T)

        if outgoing:
            await_group()
        halves(ROWS // FOUR, step, turn)
        cast_out(scr_ref, dx_ref)

    return kernel


def mul_post_bwd(dz, x, z, w_gate, w_out, outgoing):
    outs = [sds((N_POS, COLS), BF16), sds((N_POS, CH), BF16), sds((CH, CH), F32)]
    scr = [pltpu.VMEM((N_POS, CH), F32)]
    if outgoing:
        outs.append(sds(TURNED, BF16))
        scr = turn_scratch() + scr
    return call(make_post_bwd(outgoing), outs, scr, flops=3 * GIGA, name='mul_post_bwd', comm=8 if outgoing else None)(dz, x, z, w_gate, w_out)


def make_pre_bwd(outgoing):
    def kernel(*refs):
        *refs, wt_ref = refs
        if outgoing:
            (dx_ref, dxr_ref, left_ref, right_ref, z_ref, w_ref, wg_ref, dgl_ref, dz_ref, turned_ref, dzo_ref, dwr_ref, dwg_ref, zrow_ref,
             da_ref, db_ref, dwt_ref, scr_ref, send, recv) = refs
            me = lax.axis_index(GROUP_AXIS)
            greet(me)
            await_group()
            ex = Exchange(me, lambda p: turned_ref.at[p], lambda m: zrow_ref.at[:, own_rows(m), :], send, recv)
            zrow_ref[:, own_rows(me), :] = turned_ref[me]
            wt_ref[...] = w_ref[...].T

            def turn(j):
                put_strided(scr_ref, j, load_row(dxr_ref, j, True).astype(F32).T)

            loop(ROWS, turn, 2)

            def mix(c):
                da_ref[chunk_ds(c, ROWS), :] = dot_nn(dx_ref[chunk_ds(c, ROWS), :], group_rows(right_ref, c))
                db_ref[chunk_ds(c, ROWS), :] = dot_nn(scr_ref[chunk_ds(c, ROWS), :].astype(BF16), group_rows(left_ref, c))
        else:
            (own_ref, right_ref, z_ref, w_ref, wg_ref, dgl_ref, dz_ref, dzo_ref, dwr_ref, dwg_ref, da_ref, db_ref, dwt_ref,
             dx_ref, left_ref, pt_ref, send, recv) = refs
            me = lax.axis_index(GROUP_AXIS)
            greet(me)
            await_group()
            gather = Gather(me, own_ref, dx_ref, send, recv)
            wt_ref[...] = w_ref[...].T

            def prepare(t):
                nb = norm_parts(z_ref[chunk_ds(t, WIDE), :].astype(F32))[0].astype(BF16)
                pt = dot_nt(wt_ref[...], nb)
                pt_ref[t] = pt
                val = jax.nn.sigmoid(pt[CH:HALF]) * pt[:CH]
                for r in range(FOUR):
                    put_strided(da_ref, t * FOUR + r, val[:, r * COLS:(r + 1) * COLS])

            loop(ROWS // FOUR, prepare)
            cast_out(da_ref, left_ref)

            def mix(c):
                dx = group_rows(dx_ref, c)
                da_ref[chunk_ds(c, ROWS), :] = dot_nt(right_ref[chunk_ds(c, ROWS), :], dx)
                db_ref[chunk_ds(c, ROWS), :] = dot_nn(left_ref[chunk_ds(c, ROWS), :], dx)

        if outgoing:
            loop(CH, mix, PACK)
        else:
            gather.each(mix)
        dwt_ref[...] = jnp.zeros_like(dwt_ref)
        dwg_ref[...] = jnp.zeros_like(dwg_ref)

        def step(t):
            nhat, r_std = norm_parts(z_ref[chunk_ds(t, WIDE), :].astype(F32))
            nb = nhat.astype(BF16)
            pt = dot_nt(wt_ref[...], nb) if outgoing else pt_ref[t]
            parts = []
            for m, d_ref in enumerate((da_ref, db_ref)):
                d = get_four(d_ref, t)
                val = pt[2 * m * CH:(2 * m + 1) * CH]
                sg = jax.nn.sigmoid(pt[(2 * m + 1) * CH:(2 * m + 2) * CH])
                dv = d * sg
                parts += [dv, dv * val * (1.0 - sg)]
            dpt = cat0(parts).astype(BF16)
            dgl = dgl_ref[chunk_ds(t, WIDE), :]
            dwt_ref[...] += dot_nn(dpt, nb)
            dwg_ref[...] += dot_tn(nb, dgl)
            dn = dot_tn(dpt, wt_ref[...]) + dot_nt(dgl, wg_ref[...])
            dzo_ref[chunk_ds(t, WIDE), :] = (dz_ref[chunk_ds(t, WIDE), :].astype(F32) + norm_back(dn, nhat, r_std)).astype(BF16)

        loop(ROWS // FOUR, step)
        for t in range(FOUR):
            dwr_ref[pl.ds(t, CH, stride=FOUR), :] = dwt_ref[t * CH:(t + 1) * CH, :].T
        if outgoing:
            ex.arrive()
            ex.leave()
        else:
            gather.leave()

    return kernel


def mul_pre_bwd(dx, left, right, z, wt, w_gate, dgl, dz, dx_turned=None, z_turned=None):
    outgoing = dx_turned is not None
    args = [dx] + ([dx_turned, left] if outgoing else []) + [right, z, wt, w_gate, dgl, dz] + ([z_turned] if outgoing else [])
    outs = [sds((N_POS, CH), BF16), sds((4 * CH, CH), F32), sds((CH, CH), F32)]
    block = pltpu.VMEM((N_POS, CH), F32)
    scr = [block, block, pltpu.VMEM((4 * CH, CH), F32)]
    if outgoing:
        outs.append(sds((ROWS, COLS, CH), BF16))
        scr += [block] + peer_sems()
    else:
        scr += [pltpu.VMEM((GRP, N_POS, CH), BF16), pltpu.VMEM((N_POS, CH), BF16), pltpu.VMEM((ROWS // FOUR, 4 * CH, WIDE), F32)] + gather_sems()
    return call(make_pre_bwd(outgoing), outs, scr + [pltpu.VMEM((4 * CH, CH), BF16)],
                flops=6 * GIGA, name='mul_pre_bwd', comm=12 if outgoing else 11)(*args)


def att_backward(z, dz, bias_all, mask_col, w_qkvg, w_tb, w_o, left=None):
    *left_all, dz_part, g_qkvg, g_out, db = att_bwd(z, dz, bias_all, mask_col, w_qkvg, w_o, left)
    dz_new, g_bt = bias_bwd(z, dz_part, db, w_tb, left is not None)
    return dz_new.reshape(N_POS, CH), [g_qkvg, g_bt, g_out], left_all


C_S = 384
SING_DIM = 24
SING_SCALE = SING_DIM ** -0.5
GRP_HEADS = SING_HEADS // GRP
GRP_W = GRP_HEADS * SING_DIM
TOKENS = 128


def store_rows(out_ref, value, tiles):
    n = value.shape[0]
    if tiles == 1:
        out_ref[...] = value
        return
    for t in range(tiles):
        out_ref[pl.ds(t, n, stride=tiles), :] = value[:, t * 128:(t + 1) * 128]


def sing_stack(x):
    lane = lax.broadcasted_iota(jnp.int32, (TOKENS, GRP_W), 1) // SING_DIM
    x = x.astype(F32)
    return cat0([jnp.where(lane == h, x, 0.0) for h in range(GRP_HEADS)]).astype(BF16)


def sing_merge(parts):
    lane = lax.broadcasted_iota(jnp.int32, (TOKENS, GRP_W), 1) // SING_DIM
    out = jnp.where(lane == 0, parts[0], 0.0)
    for h in range(1, GRP_HEADS):
        out = jnp.where(lane == h, parts[h], out)
    return out


P_GATED, P_DMID, P_X2, P_DH, P_ACT, P_DOUT = 0, 384, 768, 1152, 4224, 5760
P_NS, P_DQ = 6144, 6528


P_ALL = 8064


def sing_fused_kernel(bias_ref, heads_ref, gate_ref, s_ref, m_ref, wo_ref, wu_ref, wd_ref, wq_ref, ds_ref,
                      so_ref, dsi_ref, pk_ref, dbt_ref, qb_ref,
                      b_all, o_out, o_in, do_out, do_in, dq_out, dq_in, db_out, send, recv):
    me = lax.axis_index(GROUP_AXIS)
    greet(me)
    await_group()

    def block(ref):
        return lambda p: ref.at[p]

    def rows_block(ref):
        return lambda p: ref.at[pl.ds(pl.multiple_of(p * TOKENS, TOKENS), TOKENS), :]

    def start(i, src_at, dst_at):
        return Exchange(me, src_at, dst_at, send.at[i], recv.at[i])

    def lanes_of(x):
        return [x[:, g * GRP_W:(g + 1) * GRP_W] for g in range(GRP)]

    def rows_of(x):
        return [x[g * ROWS:(g + 1) * ROWS] for g in range(GRP)]

    stage = 0
    ex_bias = start(stage, rows_block(bias_ref), block(b_all))
    b_all[me] = bias_ref[pl.ds(pl.multiple_of(me * TOKENS, TOKENS), TOKENS), :]
    q, k, v = [cat0([heads_ref[g, t] for g in range(GRP)]) for t in range(3)]
    ks, vs = sing_stack(k), sing_stack(v)
    logits = dot_nt(ks, q) * SING_SCALE
    mask = m_ref[...]
    ex_bias.arrive()
    probs = []
    for h in range(GRP_HEADS):
        b = cat0([b_all[g, h * ROWS:(h + 1) * ROWS, :] for g in range(GRP)]).astype(F32)
        probs.append(softmax_cols(logits[h * TOKENS:(h + 1) * TOKENS] + b + mask))
    pb = [p.astype(BF16) for p in probs]
    for g, x in enumerate(rows_of(dot_tn(cat0(pb), vs))):
        o_out[g] = x
    stage += 1
    ex_o = start(stage, block(o_out), block(o_in))
    o_in[me] = o_out[me]
    gate, s = gate_ref[...], s_ref[...].astype(F32)
    ds = ds_ref[...]
    d_act = dot_nt(ds, wd_ref[...])
    n_s, r_s = norm_parts(s)
    ex_o.arrive()
    att = cat1([o_in[g] for g in range(GRP)])
    gated = (gate * att).astype(BF16)
    s_mid = (s + dot_nn(gated, wo_ref[...])).astype(BF16).astype(F32)
    nhat, r_std = norm_parts(s_mid)
    nb = nhat.astype(BF16)
    hid = dot_nn(nb, wu_ref[...])
    h1, h2 = hid[:, :4 * C_S], hid[:, 4 * C_S:]
    sg = jax.nn.sigmoid(h1)
    a1 = h1 * sg
    dhid = cat1([d_act * h2 * (sg + a1 * (1.0 - sg)), d_act * a1]).astype(BF16)
    dsm = ds.astype(F32) + norm_back(dot_nt(dhid, wu_ref[...]), nhat, r_std)
    dsmb = dsm.astype(BF16)
    d_gated = dot_nt(dsmb, wo_ref[...])
    for g, x in enumerate(lanes_of((d_gated * gate).astype(BF16))):
        do_out[g] = x
    stage += 1
    ex_do = start(stage, block(do_out), block(do_in))
    do_in[me] = do_out[me]
    act = (a1 * h2).astype(BF16)
    so_ref[...] = (s_mid + dot_nn(act, wd_ref[...])).astype(BF16)
    dgl = (d_gated * att * gate * (1.0 - gate)).astype(BF16)
    for at, x in ((P_GATED, gated), (P_DMID, dsmb), (P_X2, nb), (P_DH, dhid), (P_ACT, act), (P_DOUT, ds), (P_NS, n_s.astype(BF16))):
        pk_ref[:, at:at + x.shape[1]] = x
    ex_do.arrive()
    do = cat0([do_in[g] for g in range(GRP)])
    dp = dot_nt(vs, do)
    dsb, dk, dv = [], [], []
    for h in range(GRP_HEADS):
        d = dp[h * TOKENS:(h + 1) * TOKENS]
        dlog = probs[h] * (d - col_sum(probs[h] * d))
        for g, x in enumerate(rows_of(dlog.astype(BF16))):
            db_out[g, h * ROWS:(h + 1) * ROWS, :] = x
        dsb.append((dlog * SING_SCALE).astype(BF16))
    stage += 1
    ex_db = start(stage, block(db_out), rows_block(dbt_ref))
    rows_block(dbt_ref)(me)[...] = db_out[me]
    for h in range(GRP_HEADS):
        dk.append(dot_nn(dsb[h], q))
        dv.append(dot_nn(pb[h], do))
    for t, x in enumerate((dot_tn(cat0(dsb), ks), sing_merge(dk), sing_merge(dv))):
        for g, y in enumerate(rows_of(x.astype(BF16))):
            dq_out[g, t] = y
    stage += 1
    ex_dq = start(stage, block(dq_out), block(dq_in))
    dq_in[me] = dq_out[me]
    ex_dq.arrive()
    dp_all = cat1([dq_in[g, t] for t in range(3) for g in range(GRP)] + [dgl])
    pk_ref[:, P_DQ:] = dp_all
    dsi_ref[...] = (dsm + norm_back(dot_nt(dp_all, wq_ref[...]), n_s, r_s)).astype(BF16)
    qb = col_sum(dp_all[:, :C_S].astype(F32))
    qb_ref[...] = cat0([qb[:, t * CH:(t + 1) * CH] for t in range(3)])
    ex_db.arrive()
    for ex in (ex_bias, ex_o, ex_do, ex_db, ex_dq):
        ex.leave()


def sing_fused(*args):
    vm = pl.BlockSpec(memory_space=pltpu.VMEM)
    dma = pltpu.SemaphoreType.DMA
    piece = (GRP, ROWS, GRP_W)
    triple = (GRP, 3, ROWS, GRP_W)
    outs = (sds((ROWS, C_S), BF16), sds((ROWS, C_S), BF16), sds((ROWS, P_ALL), BF16), sds((GRP * TOKENS, TOKENS), BF16), sds((3, CH), F32))
    sems = dma((5, len(OFFSETS)))
    return pl.pallas_call(
        sing_fused_kernel, out_shape=outs, in_specs=[vm] * len(args), out_specs=(vm,) * len(outs),
        scratch_shapes=[pltpu.VMEM((GRP, TOKENS, TOKENS), BF16), pltpu.VMEM(piece, F32), pltpu.VMEM(piece, F32),
                        pltpu.VMEM(piece, BF16), pltpu.VMEM(piece, BF16), pltpu.VMEM(triple, BF16), pltpu.VMEM(triple, BF16),
                        pltpu.VMEM((GRP, TOKENS, TOKENS), BF16), sems, sems],
        compiler_params=pltpu.CompilerParams(collective_id=2, has_side_effects=True), name='sing_fused',
        cost_estimate=pl.CostEstimate(flops=2 * GIGA, bytes_accessed=NOMINAL_BYTES, transcendentals=0),
    )(*args)


QKVG, PROJ, UP, DOWN = (4360, 12, 3), (8987, 3, 1), (10139, 24, 6), (19355, 3, 3)
KEPT = (((QKVG, 0, 136),), ((QKVG, 128, 384), (PROJ, 0, 384), (UP, 0, 80)), ((UP, 72, 328),), ((UP, 320, 384), (DOWN, 0, 384)))
W_ROWS = 1632


def kept_blocks(d):
    at = 0
    for weight, lo, hi in KEPT[d]:
        for t in range(weight[-1]):
            yield weight, lo, hi, t, at
            at += hi - lo


def sing_wgrad_kernel(m_ref, o_ref):
    k = lax.axis_index(GROUP_AXIS)

    def lanes(base, tiles, idx):
        width = tiles * CH
        return m_ref[:, pl.ds(pl.multiple_of(base + idx * width, CH), width)]

    def whole(base):
        return m_ref[:, base:base + C_S]

    grads = {
        QKVG: dot_tn(whole(P_NS), lanes(P_DQ, QKVG[-1], k)),
        PROJ: dot_tn(whole(P_GATED), lanes(P_DMID, 1, jnp.minimum(k, 2))),
        UP: dot_tn(whole(P_X2), lanes(P_DH, UP[-1], k)),
        DOWN: dot_tn(lanes(P_ACT, DOWN[-1], k), whole(P_DOUT)),
    }
    for d in range(GRP):
        end = 0
        for weight, lo, hi, t, at in kept_blocks(d):
            end = at + hi - lo
            o_ref[d, at:end, :] = grads[weight][lo:hi, t * CH:(t + 1) * CH]
        if end < W_ROWS:
            o_ref[d, end:, :] = jnp.zeros((W_ROWS - end, CH), F32)


def sing_wgrad(packed_all):
    return call(sing_wgrad_kernel, [sds((4, W_ROWS, 128), F32)], flops=GIGA, name='sing_wgrad')(packed_all)


PART = 766816
OUT_ROWS = 5992
SHIFT_ROWS = 56
SMALL_AT = ((0, 2048, 4, 24), (0, 2692, 4, 32), (1, 2978, 3, 0), (1, 2981, 16, 8))
LATE_ROWS = 1536
PIECE = LATE_ROWS // 16
LATE_SIZES = (512, 128, 128, 512, 128, 128)
EARLY_SIZES = (512, 128, 512, 128, 1024, 512)
EARLY_AT = (1536, 2052, 2180, 2696, 2824, 3848)


def finish_kernel(*refs):
    late_refs, (g_ref, p_ref, small_ref, o_ref, w_ref, x_ref, buf_ref, sum_ref, copy_sem, send1, recv1, send2, recv2) = refs[:6], refs[6:]
    d, k = lax.axis_index(BATCH_AXIS), lax.axis_index(GROUP_AXIS)
    me = 4 * d + k
    row, fills = 0, []
    for i, ref in enumerate(late_refs):
        fills.append(pltpu.make_async_copy(ref, x_ref.at[pl.ds(row, LATE_SIZES[i]), :], copy_sem.at[i]))
        row += LATE_SIZES[i]
    for c in fills:
        c.start()
    barrier = pltpu.get_barrier_semaphore()

    def device(p):
        return {BATCH_AXIS: p // 4, GROUP_AXIS: lax.rem(p, 4)}

    def piece(p):
        return pl.ds(pl.multiple_of(p * PIECE, PIECE), PIECE)

    for off in range(1, N_DEV):
        pl.semaphore_signal(barrier, inc=1, device_id=device(lax.rem(me + off, N_DEV)), device_id_type=MESH_ID)
    for c in fills:
        c.wait()
    pl.semaphore_wait(barrier, 15)
    first = []
    for off in range(1, N_DEV):
        p = lax.rem(me + off, N_DEV)
        c = pltpu.make_async_remote_copy(
            src_ref=x_ref.at[piece(p), :], dst_ref=buf_ref.at[off - 1], send_sem=send1.at[off - 1], recv_sem=recv1.at[off - 1],
            device_id=device(p), device_id_type=MESH_ID)
        c.start()
        first.append(c)

    def lay_out(part):
        begin = part * PART // 128
        lanes_off = part * PART % 128
        for weight, lo, hi, t, at in kept_blocks(part):
            base, tiles, own = weight
            for k in range(GRP):
                if weight == DOWN:
                    first_row = base + own * CH * k * tiles + t - begin
                else:
                    first_row = base + own * k + t - begin
                    if own * k + t >= tiles:
                        continue
                r0 = max(lo, -(first_row // tiles))
                r1 = min(hi, (OUT_ROWS - first_row) // tiles + 1)
                src = at + r0 - lo
                w_ref[pl.ds(first_row + r0 * tiles, r1 - r0, stride=tiles), :] = g_ref[k, src:src + r1 - r0, :]
        if part:
            lane = lax.broadcasted_iota(jnp.int32, (SHIFT_ROWS, CH), 1)
            for i in range(OUT_ROWS // SHIFT_ROWS):
                rows = slice(i * SHIFT_ROWS, (i + 1) * SHIFT_ROWS)
                a = pltpu.roll(w_ref[rows, :], CH - lanes_off, 1)
                b = pltpu.roll(w_ref[rows.start + 1:rows.stop + 1, :], CH - lanes_off, 1)
                o_ref[rows, :] = jnp.where(lane < CH - lanes_off, a, b)
        else:
            o_ref[LATE_ROWS:, :] = w_ref[LATE_ROWS:OUT_ROWS, :]

    for part in range(GRP):
        @pl.when(d == part)
        def _():
            if part == 0:
                src = 0
                for n, at in zip(EARLY_SIZES, EARLY_AT):
                    w_ref[at:at + n, :] = p_ref[src:src + n, :]
                    src += n
            for own, at, n, src in SMALL_AT:
                if own == part:
                    w_ref[at:at + n, :] = small_ref[src:src + n, :]
            lay_out(part)

    for c in first:
        c.wait_recv()
    total = x_ref[piece(me), :]
    for i in range(15):
        total += buf_ref[i]
    sum_ref[...] = total

    def second(k, src):
        return pltpu.make_async_remote_copy(
            src_ref=sum_ref, dst_ref=o_ref.at[piece(src), :], send_sem=send2.at[k], recv_sem=recv2.at[src],
            device_id={BATCH_AXIS: 0, GROUP_AXIS: k}, device_id_type=MESH_ID)

    for k in range(FOUR):
        @pl.when(me != k)
        def _():
            second(k, me).start()

    @pl.when(d == 0)
    def _():
        o_ref[piece(me), :] = total

    for k in range(FOUR):
        @pl.when(me != k)
        def _():
            second(k, me).wait_send()

    @pl.when(d == 0)
    def _():
        for off in range(1, N_DEV):
            second(0, lax.rem(me + off, N_DEV)).wait_recv()

    for c in first:
        c.wait_send()


def finish(late, g_all, early, small):
    vm = pl.BlockSpec(memory_space=pltpu.VMEM)
    dma = pltpu.SemaphoreType.DMA
    return pl.pallas_call(
        finish_kernel, out_shape=sds((OUT_ROWS, 128), F32), in_specs=[vm] * 9, out_specs=vm,
        scratch_shapes=[pltpu.VMEM((6016, 128), F32), pltpu.VMEM((LATE_ROWS, 128), F32), pltpu.VMEM((15, PIECE, 128), F32),
                        pltpu.VMEM((PIECE, 128), F32), dma((6,)), dma((15,)), dma((15,)), dma((4,)), dma((16,))],
        compiler_params=pltpu.CompilerParams(collective_id=1, has_side_effects=True), name='finish',
        cost_estimate=pl.CostEstimate(flops=GIGA, bytes_accessed=NOMINAL_BYTES, transcendentals=0),
    )(*late, g_all, early, small)


def pack_kernel(*refs):
    *srcs, o_ref = refs
    at = 0
    for ref in srcs:
        n = ref.shape[0]
        if n % PACK:
            o_ref[at:at + PACK, :] = jnp.zeros((PACK, CH), F32)
        o_ref[at:at + n, :] = ref[...]
        at += padded(n)


def padded(n):
    return -(-n // PACK) * PACK


def pack_rows(*arrays):
    return call(pack_kernel, [sds((sum(padded(a.shape[0]) for a in arrays), CH), F32)], flops=GIGA, name='pack_rows')(*arrays)


def flat_cols(x):
    return x.T.reshape(x.shape)


def device_step(single_blk, pair_blk, mask_blk, d_single_blk, d_pair_blk, *weights):
    (w1_in, w1_gate, w1_out, w2_in, w2_gate, w2_out, st_qkvg, st_bias, st_proj, en_qkvg,
     en_bias, en_proj, p_up, p_down, s_qkvg, s_qbias, s_pbias, s_proj, s_up, s_down) = weights
    s_rows = single_blk[0]
    z_zero = pair_blk[0].reshape(N_POS, CH)
    mask_bias = (mask_blk[0].astype(jnp.float32) - 1.0) * MASK_PENALTY
    mask_col = mask_bias[:, None]
    right_out = mul_proj(z_zero, w1_in)
    x_out, z_one, right_out_all, left_out, turned, right_in = mul_mix(z_zero, w1_in, right_out, z_zero, w1_gate, w1_out, w2_in)
    x_in, z_two, _, _, s_gate, s_heads = mul_mix(
        turned.reshape(N_POS, CH), w2_in, right_in, z_one, w2_gate, w2_out, single=(s_rows, s_qkvg, s_qbias[None, :]))
    z_three, bias_st = att_fwd(z_two, st_bias, mask_col, st_qkvg, st_proj)
    zt_three = z_three.reshape(N_POS, CH)
    zt_four, bias_en, dzt_out = att_fwd(zt_three, en_bias, mask_col, en_qkvg, en_proj, d_pair_blk[0])
    zt_five, bias_t, turned_five = trans_fwd(zt_four, p_up, p_down, s_pbias)
    s_out, ds_in, packed, d_bias_t, g_qb = sing_fused(
        bias_t, s_heads, s_gate, s_rows, mask_col, s_proj, s_up, s_down, s_qkvg, d_single_blk[0])
    packed, d_bias_t = lax.optimization_barrier((packed, d_bias_t))
    packed_all = gather_rows(packed)
    dzt_four, g_pup, g_pdown, g_pbt = trans_bwd(
        zt_four, zt_five, dzt_out.reshape(N_POS, CH), d_bias_t, p_up, p_down, s_pbias)
    windows = sing_wgrad(packed_all)
    dzt_four, windows = lax.optimization_barrier((dzt_four, windows))
    piece = lax.psum_scatter(windows.reshape(4 * W_ROWS, 128), BATCH_AXIS, scatter_dimension=0, tiled=True)
    dz_three, end_grads, (left_out_all,) = att_backward(zt_three, dzt_four, bias_en, mask_col, en_qkvg, en_bias, en_proj, left_out)
    dz_three, piece = lax.optimization_barrier((dz_three, piece))
    pieces = gather_rows(piece)
    dz_two, start_grads, _ = att_backward(z_two, dz_three, bias_st, mask_col, st_qkvg, st_bias, st_proj)
    dz_two, pieces = lax.optimization_barrier((dz_two, pieces))
    dx_in, dgl_in, g_in_out = mul_post_bwd(dz_two, x_in, z_one, w2_gate, w2_out, False)
    five = jnp.zeros((5, 128), F32)
    early = pack_rows(start_grads[0], start_grads[2], end_grads[0], end_grads[2], g_pup, g_pdown, g_qb, g_pbt, start_grads[1], end_grads[1])
    early, dx_in = lax.optimization_barrier((early, dx_in))
    early = lax.psum(early, (BATCH_AXIS, GROUP_AXIS))
    tail = early[sum(EARLY_SIZES):]
    small = cat0([tail[:8], flat_cols(tail[8:24]), flat_cols(tail[24:28]), five[:4], flat_cols(tail[32:36]), five[:4]])
    dz_one, g_in_in, g_in_gate = mul_pre_bwd(dx_in, None, right_in, z_one, w2_in, w2_gate, dgl_in, dz_two)
    dx_out, dgl_out, g_out_out, dx_turned = mul_post_bwd(dz_one, x_out, z_zero, w1_gate, w1_out, True)
    dz_zero, g_out_in, g_out_gate, z_five = mul_pre_bwd(
        dx_out, left_out_all, right_out_all, z_zero, w1_in, w1_gate, dgl_out, dz_one,
        dx_turned.reshape(N_POS, CH), turned_five.reshape(TURNED))
    late = (g_out_in, g_out_gate, g_out_out, g_in_in, g_in_gate, g_in_out)
    grad_flat = finish(late, pieces.reshape(4, W_ROWS, 128), early, small).reshape(-1)[:PART]
    dz_zero = dz_zero.reshape(ROWS, COLS, CH)
    return s_out[None], z_five[None], ds_in[None], dz_zero[None], grad_flat


def solution(mesh):
    spec_single = P(BATCH_AXIS, GROUP_AXIS, None)
    spec_pair = P(BATCH_AXIS, GROUP_AXIS, None, None)
    spec_mask = P(BATCH_AXIS, None)

    def block_fn(single_rep, pair_rep, token_mask, d_single_out, d_pair_out, *weights):
        in_specs = (spec_single, spec_pair, spec_mask, spec_single, spec_pair) + tuple(P() for w_item in weights)
        out_specs = (spec_single, spec_pair, spec_single, spec_pair, P(BATCH_AXIS))
        mapped = jax.shard_map(device_step, mesh=mesh, in_specs=in_specs, out_specs=out_specs, check_vma=False)
        return mapped(single_rep, pair_rep, token_mask, d_single_out, d_pair_out, *weights)

    return block_fn
```

```python
import functools
import jax
import jax.numpy as jnp
from jax import lax
from jax.experimental import pallas as pl
from jax.experimental.pallas import tpu as pltpu
from jax.sharding import PartitionSpec as P

BATCH_AXIS = 'dp'
GROUP_AXIS = 'dap'
NORM_EPS = 1e-5
MASK_PENALTY = 1.0e9


def gather_rows(x_in):
    return lax.all_gather(x_in, GROUP_AXIS, axis=0, tiled=True)


F32 = jnp.float32
NOMINAL_BYTES = 4 << 20
GIGA = 1 << 30
BF16 = jnp.bfloat16
ROWS = 32
COLS = 128
CH = 128
HALF = 2 * CH
N_POS = ROWS * COLS
TRI_HEADS = 4
GRP = 4
OFFSETS = (1, 2, 3)
MESH_ID = pl.DeviceIdType.MESH
FOUR = 8
N_DEV = 16
WIDE = FOUR * COLS
TRI_DIM = 32
TRI_SCALE = TRI_DIM ** -0.5
STEP_ROWS = 8
CHUNK = STEP_ROWS * COLS


def dot_nn(a, b):
    return lax.dot_general(a, b, (((1,), (0,)), ((), ())), preferred_element_type=F32)


def dot_nt(a, b):
    return lax.dot_general(a, b, (((1,), (1,)), ((), ())), preferred_element_type=F32)


def dot_tn(a, b):
    return lax.dot_general(a, b, (((0,), (0,)), ((), ())), preferred_element_type=F32)


def cat0(xs):
    return jnp.concatenate(xs, axis=0)


def cat1(xs):
    return jnp.concatenate(xs, axis=1)


def loop(count, step, unroll=1):
    def body(i, carry):
        step(i)
        return carry

    lax.fori_loop(0, count, body, 0, unroll=unroll)


def col_mean(x):
    return jnp.mean(x, axis=0, keepdims=True)


def col_sum(x):
    return jnp.sum(x, axis=0, keepdims=True)


def row_mean(x):
    return jnp.mean(x, axis=-1, keepdims=True)


def softmax_cols(x):
    e = jnp.exp(x - jnp.max(x, axis=0, keepdims=True))
    return e * (1.0 / col_sum(e))


def col_norm(x):
    c = x - col_mean(x)
    r = lax.rsqrt(col_mean(c * c) + NORM_EPS)
    return c * r, r


def swap_all(x, split, join):
    return lax.all_to_all(x, GROUP_AXIS, split, join, tiled=True)


def norm_parts(x):
    c = x - row_mean(x)
    r = lax.rsqrt(row_mean(c * c) + NORM_EPS)
    return c * r, r


def norm_back(dn, nhat, r):
    return r * (dn - row_mean(dn) - nhat * row_mean(dn * nhat))


def chunk_ds(t, size=CHUNK):
    return pl.ds(pl.multiple_of(t * size, size), size)


def call(kernel, out_shape, scratch=(), flops=0, name=None, comm=None):
    n_out = len(out_shape)
    vm = pl.BlockSpec(memory_space=pltpu.VMEM)

    def run(*args):
        return pl.pallas_call(
            kernel, out_shape=tuple(out_shape), in_specs=[vm] * len(args), out_specs=tuple([vm] * n_out),
            scratch_shapes=list(scratch), name=name,
            compiler_params=pltpu.CompilerParams(collective_id=comm, has_side_effects=comm is not None),
            cost_estimate=pl.CostEstimate(flops=flops, bytes_accessed=NOMINAL_BYTES, transcendentals=0),
        )(*args)

    def run_one(*args):
        return run(*args)[0]

    return run if n_out > 1 else run_one


def sds(shape, dtype):
    return jax.ShapeDtypeStruct(shape, dtype)


def greet(me):
    sem = pltpu.get_barrier_semaphore()
    for off in OFFSETS:
        pl.semaphore_signal(sem, inc=1, device_id={GROUP_AXIS: lax.rem(me + off, GRP)}, device_id_type=MESH_ID)


def await_group():
    pl.semaphore_wait(pltpu.get_barrier_semaphore(), len(OFFSETS))


class Exchange:
    def __init__(self, me, src_at, dst_at, send_sem, recv_sem):
        self.copies = []
        for i, off in enumerate(OFFSETS):
            dest = lax.rem(me + off, GRP)
            self.copies.append(pltpu.make_async_remote_copy(
                src_ref=src_at(dest), dst_ref=dst_at(me), send_sem=send_sem.at[i], recv_sem=recv_sem.at[i],
                device_id={GROUP_AXIS: dest}, device_id_type=MESH_ID))
        for c in self.copies:
            c.start()

    def arrive(self):
        for c in self.copies:
            c.wait_recv()

    def leave(self):
        for c in self.copies:
            c.wait_send()


PACK = 8
CHUNKS = 4
CHUNK_ROWS = N_POS // CHUNKS


class Gather:
    def __init__(self, me, own_ref, all_ref, send, recv):
        self.all, self.send, self.recv = all_ref, send, recv
        self.partner, self.across = me + 1 - 2 * lax.rem(me, 2), lax.rem(me + 2, GRP)
        self.far = [self.copy(own_ref.at[self.rows(c), :], me, self.across, 0, c) for c in range(CHUNKS)]
        self.near = [self.copy(own_ref.at[self.rows(c), :], me, self.partner, 1, c) for c in range(CHUNKS)]
        self.passed = []
        for c in self.far + self.near:
            c.start()
        all_ref[me] = own_ref[...]

    def rows(self, c):
        return pl.ds(c * CHUNK_ROWS, CHUNK_ROWS)

    def copy(self, src, slot, dest, kind, c):
        return pltpu.make_async_remote_copy(
            src_ref=src, dst_ref=self.all.at[slot, self.rows(c), :], send_sem=self.send.at[kind, c], recv_sem=self.recv.at[kind, c],
            device_id={GROUP_AXIS: dest}, device_id_type=MESH_ID)

    def each(self, work):
        for c in range(CHUNKS + 1):
            if c < CHUNKS:
                self.far[c].wait_recv()
                self.passed.append(self.copy(self.all.at[self.across, self.rows(c), :], self.across, self.partner, 2, c))
                self.passed[c].start()
            if c:
                self.near[c - 1].wait_recv()
                self.passed[c - 1].wait_recv()
                loop(CH // CHUNKS, lambda k: work(k + (c - 1) * (CH // CHUNKS)), PACK)

    def pass_on(self):
        for c in range(CHUNKS):
            self.far[c].wait_recv()
            self.passed.append(self.copy(self.all.at[self.across, self.rows(c), :], self.across, self.partner, 2, c))
            self.passed[c].start()

    def arrive(self):
        for c in self.near + self.passed:
            c.wait_recv()

    def leave(self):
        for c in self.far + self.near + self.passed:
            c.wait_send()


def gather_sems():
    sems = pltpu.SemaphoreType.DMA((3, CHUNKS))
    return [sems, sems]


def own_rows(p, size=ROWS):
    return pl.ds(pl.multiple_of(p * size, size), size)


class Turn:
    def __init__(self, me, scr_ref, stage_ref, out_ref, send, recv):
        self.me, self.scr, self.stage, self.out, self.send, self.recv = me, scr_ref, stage_ref, out_ref, send, recv
        self.sent = []

    def half(self, n):
        lo = n * HALF_ROWS

        def cast(j):
            rows = self.scr[pl.ds(pl.multiple_of(j * ROWS + lo, HALF_ROWS), HALF_ROWS), :]
            self.stage[j // ROWS, lax.rem(j, ROWS), lo:lo + HALF_ROWS, :] = rows.astype(BF16)

        loop(COLS, cast, FOUR)
        part = (slice(None), slice(lo, lo + HALF_ROWS))
        self.sent.append(Exchange(self.me, lambda p: self.stage.at[(p, *part)], lambda m: self.out.at[(m, *part)], self.send.at[n], self.recv.at[n]))

    def finish(self):
        self.out[self.me] = self.stage[self.me]
        for ex in self.sent:
            ex.arrive()
            ex.leave()


TURNED = (GRP, ROWS, ROWS, CH)
HALF_ROWS = ROWS // 2


def turn_scratch():
    sems = pltpu.SemaphoreType.DMA((2, len(OFFSETS)))
    return [pltpu.VMEM((N_POS, CH), F32), pltpu.VMEM(TURNED, BF16), sems, sems]


def peer_sems():
    sems = pltpu.SemaphoreType.DMA((len(OFFSETS),))
    return [sems, sems]


ATT_STEP = 8
BWD_STEP = 8


def fill_bias(bias_ref, mask_ref, bm_ref):
    mask = mask_ref[...]
    for h in range(TRI_HEADS):
        cols = slice(h * COLS, (h + 1) * COLS)
        bm_ref[:, cols] = bias_ref[:, cols].astype(F32).T + mask


def head_rows(x, h):
    return x[h * TRI_DIM:(h + 1) * TRI_DIM]


def spread_heads(xt):
    zero = jnp.zeros((TRI_DIM, COLS), xt.dtype)
    return cat1([
        cat0([head_rows(xt, h) if g == h else zero for g in range(TRI_HEADS)])
        for h in range(TRI_HEADS)])


def probs_of(k, q_wide, bm_ref):
    x = dot_nn(k, q_wide) * TRI_SCALE + bm_ref[...]
    return softmax_cols(x)


def heads_nn(xt, wide):
    return cat0([dot_nn(head_rows(xt, h), wide[:, h * COLS:(h + 1) * COLS]) for h in range(TRI_HEADS)])


def att_fwd_kernel(ending, z_ref, wbt_ref, mask_ref, w_ref, wo_ref, *rest):
    *rest, wt_ref = rest
    wt_ref[...] = w_ref[...].T
    if ending:
        dp_ref, o_ref, bias_ref, dpt_ref, bm_ref, own_ref, send, recv, dp_send, dp_recv = rest
    else:
        o_ref, bias_ref, bm_ref, own_ref, send, recv, *rest = rest
    me = lax.axis_index(GROUP_AXIS)
    greet(me)
    turn = None if ending else Turn(me, rest[0], rest[1], o_ref, *rest[2:])

    def bias_step(t):
        nhat, _ = norm_parts(cat0([load_row(z_ref, t * PACK + r, ending) for r in range(PACK)]).astype(F32))
        nb = nhat.astype(BF16)
        b = [dot_nt(wbt_ref[...], nb[r * COLS:(r + 1) * COLS]) for r in range(PACK)]
        for h in range(TRI_HEADS):
            own_ref[chunk_ds(t, PACK), h * COLS:(h + 1) * COLS] = cat0([x[h:h + 1, :] for x in b])

    loop(ROWS // PACK, bias_step)
    bias_ref[own_rows(me), :] = own_ref[...].astype(BF16)
    await_group()
    ex = Exchange(me, lambda p: bias_ref.at[own_rows(me), :], lambda m: bias_ref.at[own_rows(m), :], send, recv)
    ex.arrive()
    if ending:
        ex_dp = Exchange(me, lambda p: dp_ref.at[:, own_rows(p), :], lambda m: dpt_ref.at[m], dp_send, dp_recv)
        dpt_ref[me] = dp_ref[:, own_rows(me), :]
    fill_bias(bias_ref, mask_ref, bm_ref)

    def step(t):
        z = cat0([load_row(z_ref, t * ATT_STEP + r, ending) for r in range(ATT_STEP)]).astype(F32)
        nhat, _ = norm_parts(z)
        nb = nhat.astype(BF16)
        qt_all = dot_nt(wt_ref[:CH, :], nb)
        k_all = dot_nt(nb, wt_ref[CH:HALF, :]).astype(BF16)
        vg_all = dot_nt(wt_ref[HALF:, :], nb)
        gate = jax.nn.sigmoid(vg_all[CH:])
        outs = []
        for r in range(ATT_STEP):
            cols = slice(r * COLS, (r + 1) * COLS)
            q_wide = spread_heads(qt_all[:, cols]).astype(BF16)
            probs = probs_of(k_all[cols], q_wide, bm_ref).astype(BF16)
            outs.append(heads_nn(vg_all[:CH, cols].astype(BF16), probs))
        gated = (gate * cat1(outs)).astype(BF16)
        out = z + dot_tn(gated, wo_ref[...])
        for r in range(ATT_STEP):
            rows = slice(r * COLS, (r + 1) * COLS)
            if turn is None:
                o_ref[chunk_ds(t * ATT_STEP + r, COLS), :] = out[rows].astype(BF16)
            else:
                put_strided(turn.scr, t * ATT_STEP + r, out[rows])

    halves(ROWS // ATT_STEP, step, turn)
    ex.leave()
    if ending:
        ex_dp.arrive()
        ex_dp.leave()


def halves(count, step, turn, filler=None):
    if turn is None:
        loop(count, step)
        return
    loop(count // 2, step)
    turn.half(0)
    loop(count // 2, lambda t: step(t + count // 2))
    turn.half(1)
    if filler:
        filler()
    turn.finish()


def att_fwd(z, w_b, mask_col, wt, w_o, d_pair=None):
    ending = d_pair is not None
    scr = [pltpu.VMEM((COLS, TRI_HEADS * COLS), F32), pltpu.VMEM((ROWS, TRI_HEADS * COLS), F32)] + peer_sems()
    outs = [sds((N_POS, CH) if ending else TURNED, BF16), sds((COLS, TRI_HEADS * COLS), BF16)]
    args = [z, w_b.T, mask_col, wt, w_o]
    if ending:
        outs.append(sds(TURNED, BF16))
        args.append(d_pair)
    return call(functools.partial(att_fwd_kernel, ending), outs, scr + (peer_sems() if ending else turn_scratch()) + [pltpu.VMEM((4 * CH, CH), BF16)],
                flops=3 * GIGA, name='att_fwd', comm=4 if ending else 3)(*args)


def att_bwd_kernel(ending, z_ref, dz_ref, bias_ref, mask_ref, w_ref, wo_ref, *rest):
    *rest, wt_ref = rest
    wt_ref[...] = w_ref[...].T
    z_blocked, dz_blocked = ending, not ending
    if ending:
        own_ref, all_ref, *rest = rest
        *rest, send, recv = rest
        me = lax.axis_index(GROUP_AXIS)
        greet(me)
        await_group()
        gather = Gather(me, own_ref, all_ref, send, recv)
    dzo_ref, dwr_ref, dwo_ref, db_ref, bm_ref, acc_ref, dwqg_ref, dwkv_ref = rest
    fill_bias(bias_ref, mask_ref, bm_ref)
    acc_ref[...] = jnp.zeros_like(acc_ref)
    dwqg_ref[...] = jnp.zeros_like(dwqg_ref)
    dwkv_ref[...] = jnp.zeros_like(dwkv_ref)
    dwo_ref[...] = jnp.zeros_like(dwo_ref)

    def step(t):
        nhat, r_std = norm_parts(cat0([load_row(z_ref, t * BWD_STEP + r, z_blocked) for r in range(BWD_STEP)]).astype(F32))
        nb = nhat.astype(BF16)
        pt_all = dot_nt(wt_ref[...], nb)
        kv_all = dot_nt(nb, wt_ref[CH:3 * CH, :]).astype(BF16)
        gate = jax.nn.sigmoid(pt_all[3 * CH:])
        dz = cat0([load_row(dz_ref, t * BWD_STEP + r, dz_blocked) for r in range(BWD_STEP)])
        d_gated = dot_nt(wo_ref[...], dz)
        d_att = d_gated * gate
        outs, dqs, dkvs = [], [], []
        for r in range(BWD_STEP):
            cols = slice(r * COLS, (r + 1) * COLS)
            q_wide = spread_heads(pt_all[:CH, cols]).astype(BF16)
            do_wide = spread_heads(d_att[:, cols]).astype(BF16)
            p = probs_of(kv_all[cols, :CH], q_wide, bm_ref)
            pb = p.astype(BF16)
            outs.append(heads_nn(pt_all[2 * CH:3 * CH, cols].astype(BF16), pb))
            dp = dot_nn(kv_all[cols, CH:], do_wide)
            ds = p * (dp - col_sum(dp * p))
            acc_ref[...] += ds
            dsb = (ds * TRI_SCALE).astype(BF16)
            dqs.append(heads_nn(pt_all[CH:2 * CH, cols].astype(BF16), dsb))
            dkvs.append(cat1([dot_nt(dsb, q_wide), dot_nt(pb, do_wide)]).astype(BF16))
        o = cat1(outs)
        gated = (gate * o).astype(BF16)
        dgl = d_gated * o * gate * (1.0 - gate)
        dqg = cat0([cat1(dqs), dgl]).astype(BF16)
        dkv = cat0(dkvs)
        dwo_ref[...] += dot_nn(gated, dz)
        dwqg_ref[...] += dot_nn(dqg, nb)
        dwkv_ref[...] += dot_tn(nb, dkv)
        dn = dot_nn(dkv, wt_ref[CH:3 * CH, :]) + dot_tn(dqg[:CH], wt_ref[:CH, :]) + dot_tn(dqg[CH:], wt_ref[3 * CH:, :])
        dzo_ref[chunk_ds(t, BWD_STEP * COLS), :] = (dz.astype(F32) + norm_back(dn, nhat, r_std)).astype(BF16)

    loop(ROWS // BWD_STEP, step)
    if ending:
        gather.pass_on()
    for h in range(TRI_HEADS):
        cols = slice(h * COLS, (h + 1) * COLS)
        db_ref[:, cols] = acc_ref[:, cols].T
    for m in range(2):
        dwr_ref[pl.ds(3 * m, CH, stride=4), :] = dwqg_ref[m * CH:(m + 1) * CH, :].T
        dwr_ref[pl.ds(1 + m, CH, stride=4), :] = dwkv_ref[:, m * CH:(m + 1) * CH]
    if ending:
        gather.arrive()
        gather.leave()


def att_bwd(z, dz, bias_all, mask_col, wt, w_o, left=None):
    ending = left is not None
    outs = [sds((N_POS, CH), BF16), sds((4 * CH, CH), F32), sds((CH, CH), F32), sds((COLS, TRI_HEADS * COLS), F32)]
    wide = pltpu.VMEM((COLS, TRI_HEADS * COLS), F32)
    scr = [wide, wide, pltpu.VMEM((HALF, CH), F32), pltpu.VMEM((CH, HALF), F32)]
    args = [z, dz, bias_all, mask_col, wt, w_o]
    if ending:
        outs = [sds((GRP, N_POS, CH), BF16)] + outs
        scr = scr + gather_sems()
        args.append(left)
    scr.append(pltpu.VMEM((4 * CH, CH), BF16))
    return call(functools.partial(att_bwd_kernel, ending), outs, scr, flops=8 * GIGA, name='att_bwd', comm=9 if ending else None)(*args)


def bias_bwd_kernel(ending, z_ref, dz_ref, db_ref, wbt_ref, dzo_ref, dwt_ref, parts_ref, send, recv, *rest):
    me = lax.axis_index(GROUP_AXIS)
    greet(me)
    turn = Turn(me, rest[0], rest[1], dzo_ref, *rest[2:]) if ending else None
    dwt_ref[...] = jnp.zeros_like(dwt_ref)
    wbt = wbt_ref[...]
    await_group()
    ex = Exchange(me, lambda p: db_ref.at[own_rows(p), :], lambda m: parts_ref.at[m], send, recv)
    parts_ref[me] = db_ref[own_rows(me), :]
    ex.arrive()

    def step(t):
        block = sum(parts_ref[g, chunk_ds(t, PACK), :] for g in range(GRP))
        nhat, r_std = norm_parts(cat0([load_row(z_ref, t * PACK + r, ending) for r in range(PACK)]).astype(F32))
        nb = nhat.astype(BF16)
        dwt = jnp.zeros((TRI_HEADS, CH), F32)
        dns = []
        for r in range(PACK):
            db = cat0([block[r:r + 1, h * COLS:(h + 1) * COLS] for h in range(TRI_HEADS)]).astype(BF16)
            dwt += dot_nn(db, nb[r * COLS:(r + 1) * COLS])
            dns.append(dot_tn(db, wbt))
        out = dz_ref[chunk_ds(t, PACK * COLS), :].astype(F32) + norm_back(cat0(dns), nhat, r_std)
        if turn is None:
            dzo_ref[chunk_ds(t, PACK * COLS), :] = out.astype(BF16)
        else:
            for r in range(PACK):
                put_strided(turn.scr, t * PACK + r, out[r * COLS:(r + 1) * COLS])
        dwt_ref[...] += dwt

    halves(ROWS // PACK, step, turn)
    ex.leave()


def bias_bwd(z, dz, db, w_b, ending):
    scr = [pltpu.VMEM((GRP, ROWS, TRI_HEADS * COLS), F32)] + peer_sems()
    out = sds(TURNED if ending else (N_POS, CH), BF16)
    return call(functools.partial(bias_bwd_kernel, ending), [out, sds((TRI_HEADS, CH), F32)],
                scr + turn_scratch() if ending else scr, flops=GIGA, name='bias_bwd', comm=6 if ending else 5,
                )(z, dz, db, w_b.T)


SING_HEADS = 16


def trans_fwd_kernel(z_ref, wu_ref, wd_ref, wpt_ref, o_ref, b_ref, turned_ref, scr_ref, turn_ref):
    def step(t):
        z = z_ref[chunk_ds(t), :].astype(F32)
        nhat, _ = norm_parts(z)
        hid = dot_nn(nhat.astype(BF16), wu_ref[...])
        h1, h2 = hid[:, :4 * CH], hid[:, 4 * CH:]
        act = (jax.nn.sigmoid(h1) * h1 * h2).astype(BF16)
        out = (z + dot_nn(act, wd_ref[...])).astype(BF16)
        o_ref[chunk_ds(t), :] = out
        for r in range(STEP_ROWS):
            put_strided(turn_ref, t * STEP_ROWS + r, out[r * COLS:(r + 1) * COLS].astype(F32))
        n5, _ = norm_parts(out.astype(F32))
        n5 = n5.astype(BF16)
        for r in range(STEP_ROWS):
            scr_ref[pl.ds(t * STEP_ROWS + r, SING_HEADS, stride=ROWS), :] = dot_nt(wpt_ref[...], n5[r * COLS:(r + 1) * COLS])

    loop(ROWS // STEP_ROWS, step)
    b_ref[...] = scr_ref[...].astype(BF16)
    cast_out(turn_ref, turned_ref)


def trans_fwd(z, w_up, w_down, w_pb):
    return call(trans_fwd_kernel, [sds((N_POS, CH), BF16), sds((SING_HEADS * ROWS, COLS), BF16), sds((N_POS, CH), BF16)],
                [pltpu.VMEM((SING_HEADS * ROWS, COLS), F32), pltpu.VMEM((N_POS, CH), F32)],
                flops=2 * GIGA, name='trans_fwd')(z, w_up, w_down, w_pb.T)


def trans_bwd_kernel(z_ref, z5_ref, dz_ref, db_ref, wu_ref, wd_ref, wpt_ref,
                     dzo_ref, dwr_ref, dwd_ref, dwpt_ref, dwu_ref, scr_ref, dzs_ref):

    def convert(t):
        dzs_ref[chunk_ds(t, WIDE), :] = dz_ref[chunk_ds(t, WIDE), :].astype(F32)

    loop(N_POS // WIDE, convert)

    def dz_row(j):
        return cat0([dzs_ref[pl.ds(g * ROWS * ROWS + j, ROWS, stride=ROWS), :] for g in range(GRP)])

    dwu_ref[...] = jnp.zeros_like(dwu_ref)
    dwd_ref[...] = jnp.zeros_like(dwd_ref)
    dwpt_ref[...] = jnp.zeros_like(dwpt_ref)
    scr_ref[...] = db_ref[...].astype(F32)

    def step(t):
        n5, r5 = norm_parts(z5_ref[chunk_ds(t), :].astype(F32))
        n5b = n5.astype(BF16)
        dn5 = []
        for r in range(STEP_ROWS):
            db = scr_ref[pl.ds(t * STEP_ROWS + r, SING_HEADS, stride=ROWS), :].astype(BF16)
            dwpt_ref[...] += dot_nn(db, n5b[r * COLS:(r + 1) * COLS])
            dn5.append(dot_tn(db, wpt_ref[...]))
        dz = cat0([dz_row(t * STEP_ROWS + r) for r in range(STEP_ROWS)]) + norm_back(cat0(dn5), n5, r5)
        dzb = dz.astype(BF16)
        nhat, r_std = norm_parts(z_ref[chunk_ds(t), :].astype(F32))
        nb = nhat.astype(BF16)
        hid = dot_nn(nb, wu_ref[...])
        h1, h2 = hid[:, :4 * CH], hid[:, 4 * CH:]
        sg = jax.nn.sigmoid(h1)
        a1 = h1 * sg
        d_act = dot_nt(dzb, wd_ref[...])
        dwd_ref[...] += dot_tn((a1 * h2).astype(BF16), dzb)
        dhid = cat1([d_act * h2 * (sg + a1 * (1.0 - sg)), d_act * a1]).astype(BF16)
        dwu_ref[...] += dot_tn(nb, dhid)
        dn = dot_nt(dhid, wu_ref[...])
        dzo_ref[chunk_ds(t), :] = (dz + norm_back(dn, nhat, r_std)).astype(BF16)

    loop(ROWS // STEP_ROWS, step)
    store_rows(dwr_ref, dwu_ref[...], PACK)


def trans_bwd(z, z5, dz, db, w_up, w_down, w_pb):
    outs = [sds((N_POS, CH), BF16), sds((8 * CH, CH), F32), sds((4 * CH, CH), F32), sds((SING_HEADS, CH), F32)]
    scr = [pltpu.VMEM((CH, 8 * CH), F32), pltpu.VMEM((SING_HEADS * ROWS, COLS), F32), pltpu.VMEM((N_POS, CH), F32)]
    return call(trans_bwd_kernel, outs, scr, flops=6 * GIGA, name='trans_bwd')(z, z5, dz, db, w_up, w_down, w_pb.T)


def load_row(ref, i, blocked):
    if not blocked:
        return ref[chunk_ds(i, COLS), :]
    return cat0([ref[pl.ds(pl.multiple_of(s * ROWS * ROWS + i * ROWS, ROWS), ROWS), :] for s in range(GRP)])


def load_rows(ref, t, blocked):
    if not blocked:
        return ref[chunk_ds(t), :]
    return cat0([load_row(ref, t * STEP_ROWS + r, True) for r in range(STEP_ROWS)])


def put_strided(scr_ref, i, value):
    scr_ref[pl.ds(i, COLS, stride=ROWS), :] = value


def get_strided(scr_ref, i):
    return scr_ref[pl.ds(i, COLS, stride=ROWS), :]


def get_four(scr_ref, t):
    return cat1([get_strided(scr_ref, t * FOUR + r) for r in range(FOUR)])


def cast_out(scr_ref, o_ref):
    def step(t):
        o_ref[chunk_ds(t, 256), :] = scr_ref[chunk_ds(t, 256), :].astype(BF16)

    loop(N_POS // 256, step)


def group_rows(ref, c):
    return cat0([ref[s, chunk_ds(c, ROWS), :] for s in range(GRP)])


def project(z_ref, wt_ref, scr_ref, out_ref, blocked):
    def step(t):
        z = cat0([load_row(z_ref, t * FOUR + r, blocked) for r in range(FOUR)]).astype(F32)
        nhat, _ = norm_parts(z)
        pt = dot_nt(wt_ref[...], nhat.astype(BF16))
        val = jax.nn.sigmoid(pt[CH:]) * pt[:CH]
        for r in range(FOUR):
            put_strided(scr_ref, t * FOUR + r, val[:, r * COLS:(r + 1) * COLS])

    loop(ROWS // FOUR, step)
    cast_out(scr_ref, out_ref)


def proj_kernel(z_ref, w_ref, o_ref, scr_ref, wt_ref):
    wt_ref[...] = w_ref[:, HALF:].T
    project(z_ref, wt_ref, scr_ref, o_ref, False)


def mul_proj(z, w):
    return call(proj_kernel, [sds((N_POS, CH), BF16)], [pltpu.VMEM((N_POS, CH), F32), pltpu.VMEM((HALF, CH), BF16)],
                flops=GIGA, name='mul_proj')(z, w)


def sing_heads(me, s_ref, w_ref, qb_ref, gate_ref, out_ref, in_ref, send, recv):
    nhat, _ = norm_parts(s_ref[...].astype(F32))
    p_all = dot_nn(nhat.astype(BF16), w_ref[...])
    gate_ref[...] = jax.nn.sigmoid(p_all[:, 3 * C_S:])
    qkv = cat1([p_all[:, :C_S] + qb_ref[...].astype(F32), p_all[:, C_S:3 * C_S]]).astype(BF16)
    for t in range(3):
        for g in range(GRP):
            at = t * C_S + g * GRP_W
            out_ref[g, t] = qkv[:, at:at + GRP_W]
    in_ref[me] = out_ref[me]
    return Exchange(me, lambda p: out_ref.at[p], lambda m: in_ref.at[m], send, recv)


def make_mix(outgoing):
    def kernel(*refs):
        turn = None
        me = lax.axis_index(GROUP_AXIS)
        greet(me)
        if outgoing:
            (zl_ref, wl_ref, own_ref, z_ref, wg_ref, wo_ref, wn_ref, x_ref, o_ref, right_ref, left_ref, turned_ref, next_ref,
             scr_ref, stage_ref, send, recv, g_send, g_recv, wt_ref) = refs
            turn = Turn(me, scr_ref, stage_ref, turned_ref, send, recv)
        else:
            (zl_ref, wl_ref, own_ref, z_ref, wg_ref, wo_ref, s_ref, wq_ref, qb_ref, x_ref, o_ref, right_ref, left_ref, gate_ref, heads_ref,
             heads_out, send, recv, g_send, g_recv, wt_ref) = refs
        await_group()
        gather = Gather(me, own_ref, right_ref, g_send, g_recv)
        ex = None if outgoing else sing_heads(me, s_ref, wq_ref, qb_ref, gate_ref, heads_out, heads_ref, send, recv)
        wt_ref[...] = wl_ref[:, :HALF].T
        project(zl_ref, wt_ref, x_ref, left_ref, not outgoing)

        def mix(c):
            a = left_ref[chunk_ds(c, ROWS), :]
            b = group_rows(right_ref, c)
            x_ref[chunk_ds(c, ROWS), :] = dot_nt(a, b) if outgoing else dot_nn(a, b)

        gather.each(mix)

        def step(t):
            x = get_four(x_ref, t)
            xb = col_norm(x)[0].astype(BF16)
            z = z_ref[chunk_ds(t, WIDE), :].astype(F32)
            nhat, _ = norm_parts(z)
            gate = jax.nn.sigmoid(dot_nn(nhat.astype(BF16), wg_ref[...]))
            out = z + gate * dot_tn(xb, wo_ref[...])
            if outgoing:
                for r in range(FOUR):
                    put_strided(turn.scr, t * FOUR + r, out[r * COLS:(r + 1) * COLS])
            o_ref[chunk_ds(t, WIDE), :] = out.astype(BF16)

        def following():
            wt_ref[...] = wn_ref[:, HALF:].T
            project(o_ref, wt_ref, scr_ref, next_ref, False)

        halves(ROWS // FOUR, step, turn, following)
        gather.leave()
        if ex is not None:
            ex.arrive()
            ex.leave()

    return kernel


def mul_mix(z_left, wt_left, right, z, w_gate, w_out, wt_next=None, single=None):
    outgoing = single is None
    flat = sds((N_POS, CH), BF16)
    outs = [sds((N_POS, COLS), F32), flat, sds((GRP, N_POS, CH), BF16), flat]
    scr = gather_sems() + [pltpu.VMEM((HALF, CH), BF16)]
    if outgoing:
        outs += [sds(TURNED, BF16), flat]
        scr = turn_scratch() + scr
    else:
        heads = (GRP, 3, ROWS, GRP_W)
        outs += [sds((ROWS, C_S), F32), sds(heads, BF16)]
        scr = [pltpu.VMEM(heads, BF16)] + peer_sems() + scr
    return call(make_mix(outgoing), outs, scr, flops=3 * GIGA, name='mul_mix', comm=7 if outgoing else 10)(z_left, wt_left, right, z, w_gate, w_out, *(single or (wt_next,)))


def make_post_bwd(outgoing):
    def kernel(dz_ref, x_ref, z_ref, wg_ref, wo_ref, dx_ref, dgl_ref, dwo_ref, *rest):
        scr_ref, rest = rest[-1], rest[:-1]
        turn = None
        if outgoing:
            me = lax.axis_index(GROUP_AXIS)
            greet(me)
            turned_ref, turn_scr, stage_ref, send, recv = rest
            turn = Turn(me, turn_scr, stage_ref, turned_ref, send, recv)
        dwo_ref[...] = jnp.zeros_like(dwo_ref)

        def step(t):
            x = get_four(x_ref, t)
            xhat, r = col_norm(x)
            xb = xhat.astype(BF16)
            nhat, _ = norm_parts(z_ref[chunk_ds(t, WIDE), :].astype(F32))
            gate = jax.nn.sigmoid(dot_nn(nhat.astype(BF16), wg_ref[...]))
            du = dz_ref[chunk_ds(t, WIDE), :].astype(F32)
            dy = (gate * du).astype(BF16)
            dgl_ref[chunk_ds(t, WIDE), :] = (dot_tn(xb, wo_ref[...]) * du * gate * (1.0 - gate)).astype(BF16)
            dwo_ref[...] += dot_nn(xb, dy)
            dn = dot_nt(wo_ref[...], dy)
            dx = r * (dn - col_mean(dn) - xhat * col_mean(dn * xhat))
            for r in range(FOUR):
                part = dx[:, r * COLS:(r + 1) * COLS]
                put_strided(scr_ref, t * FOUR + r, part)
                if outgoing:
                    put_strided(turn.scr, t * FOUR + r, part.T)

        if outgoing:
            await_group()
        halves(ROWS // FOUR, step, turn)
        cast_out(scr_ref, dx_ref)

    return kernel


def mul_post_bwd(dz, x, z, w_gate, w_out, outgoing):
    outs = [sds((N_POS, COLS), BF16), sds((N_POS, CH), BF16), sds((CH, CH), F32)]
    scr = [pltpu.VMEM((N_POS, CH), F32)]
    if outgoing:
        outs.append(sds(TURNED, BF16))
        scr = turn_scratch() + scr
    return call(make_post_bwd(outgoing), outs, scr, flops=3 * GIGA, name='mul_post_bwd', comm=8 if outgoing else None)(dz, x, z, w_gate, w_out)


def make_pre_bwd(outgoing):
    def kernel(*refs):
        *refs, wt_ref = refs
        if outgoing:
            (dx_ref, dxr_ref, left_ref, right_ref, z_ref, w_ref, wg_ref, dgl_ref, dz_ref, turned_ref, dzo_ref, dwr_ref, dwg_ref, zrow_ref,
             da_ref, db_ref, dwt_ref, scr_ref, send, recv) = refs
            me = lax.axis_index(GROUP_AXIS)
            greet(me)
            await_group()
            ex = Exchange(me, lambda p: turned_ref.at[p], lambda m: zrow_ref.at[:, own_rows(m), :], send, recv)
            zrow_ref[:, own_rows(me), :] = turned_ref[me]
            wt_ref[...] = w_ref[...].T

            def turn(j):
                put_strided(scr_ref, j, load_row(dxr_ref, j, True).astype(F32).T)

            loop(ROWS, turn, 2)

            def mix(c):
                da_ref[chunk_ds(c, ROWS), :] = dot_nn(dx_ref[chunk_ds(c, ROWS), :], group_rows(right_ref, c))
                db_ref[chunk_ds(c, ROWS), :] = dot_nn(scr_ref[chunk_ds(c, ROWS), :].astype(BF16), group_rows(left_ref, c))
        else:
            (own_ref, right_ref, z_ref, w_ref, wg_ref, dgl_ref, dz_ref, dzo_ref, dwr_ref, dwg_ref, da_ref, db_ref, dwt_ref,
             dx_ref, left_ref, pt_ref, send, recv) = refs
            me = lax.axis_index(GROUP_AXIS)
            greet(me)
            await_group()
            gather = Gather(me, own_ref, dx_ref, send, recv)
            wt_ref[...] = w_ref[...].T

            def prepare(t):
                nb = norm_parts(z_ref[chunk_ds(t, WIDE), :].astype(F32))[0].astype(BF16)
                pt = dot_nt(wt_ref[...], nb)
                pt_ref[t] = pt
                val = jax.nn.sigmoid(pt[CH:HALF]) * pt[:CH]
                for r in range(FOUR):
                    put_strided(da_ref, t * FOUR + r, val[:, r * COLS:(r + 1) * COLS])

            loop(ROWS // FOUR, prepare)
            cast_out(da_ref, left_ref)

            def mix(c):
                dx = group_rows(dx_ref, c)
                da_ref[chunk_ds(c, ROWS), :] = dot_nt(right_ref[chunk_ds(c, ROWS), :], dx)
                db_ref[chunk_ds(c, ROWS), :] = dot_nn(left_ref[chunk_ds(c, ROWS), :], dx)

        if outgoing:
            loop(CH, mix, PACK)
        else:
            gather.each(mix)
        dwt_ref[...] = jnp.zeros_like(dwt_ref)
        dwg_ref[...] = jnp.zeros_like(dwg_ref)

        def step(t):
            nhat, r_std = norm_parts(z_ref[chunk_ds(t, WIDE), :].astype(F32))
            nb = nhat.astype(BF16)
            pt = dot_nt(wt_ref[...], nb) if outgoing else pt_ref[t]
            parts = []
            for m, d_ref in enumerate((da_ref, db_ref)):
                d = get_four(d_ref, t)
                val = pt[2 * m * CH:(2 * m + 1) * CH]
                sg = jax.nn.sigmoid(pt[(2 * m + 1) * CH:(2 * m + 2) * CH])
                dv = d * sg
                parts += [dv, dv * val * (1.0 - sg)]
            dpt = cat0(parts).astype(BF16)
            dgl = dgl_ref[chunk_ds(t, WIDE), :]
            dwt_ref[...] += dot_nn(dpt, nb)
            dwg_ref[...] += dot_tn(nb, dgl)
            dn = dot_tn(dpt, wt_ref[...]) + dot_nt(dgl, wg_ref[...])
            dzo_ref[chunk_ds(t, WIDE), :] = (dz_ref[chunk_ds(t, WIDE), :].astype(F32) + norm_back(dn, nhat, r_std)).astype(BF16)

        loop(ROWS // FOUR, step)
        for t in range(GRP):
            dwr_ref[pl.ds(t, CH, stride=GRP), :] = dwt_ref[t * CH:(t + 1) * CH, :].T
        if outgoing:
            ex.arrive()
            ex.leave()
        else:
            gather.leave()

    return kernel


def mul_pre_bwd(dx, left, right, z, wt, w_gate, dgl, dz, dx_turned=None, z_turned=None):
    outgoing = dx_turned is not None
    args = [dx] + ([dx_turned, left] if outgoing else []) + [right, z, wt, w_gate, dgl, dz] + ([z_turned] if outgoing else [])
    outs = [sds((N_POS, CH), BF16), sds((4 * CH, CH), F32), sds((CH, CH), F32)]
    block = pltpu.VMEM((N_POS, CH), F32)
    scr = [block, block, pltpu.VMEM((4 * CH, CH), F32)]
    if outgoing:
        outs.append(sds((ROWS, COLS, CH), BF16))
        scr += [block] + peer_sems()
    else:
        scr += [pltpu.VMEM((GRP, N_POS, CH), BF16), pltpu.VMEM((N_POS, CH), BF16), pltpu.VMEM((ROWS // FOUR, 4 * CH, WIDE), F32)] + gather_sems()
    return call(make_pre_bwd(outgoing), outs, scr + [pltpu.VMEM((4 * CH, CH), BF16)],
                flops=6 * GIGA, name='mul_pre_bwd', comm=12 if outgoing else 11)(*args)


def att_backward(z, dz, bias_all, mask_col, w_qkvg, w_tb, w_o, left=None):
    *left_all, dz_part, g_qkvg, g_out, db = att_bwd(z, dz, bias_all, mask_col, w_qkvg, w_o, left)
    dz_new, g_bt = bias_bwd(z, dz_part, db, w_tb, left is not None)
    return dz_new.reshape(N_POS, CH), [g_qkvg, g_bt, g_out], left_all


C_S = 384
SING_DIM = 24
SING_SCALE = SING_DIM ** -0.5
GRP_HEADS = SING_HEADS // GRP
GRP_W = GRP_HEADS * SING_DIM
TOKENS = 128


def store_rows(out_ref, value, tiles):
    n = value.shape[0]
    if tiles == 1:
        out_ref[...] = value
        return
    for t in range(tiles):
        out_ref[pl.ds(t, n, stride=tiles), :] = value[:, t * 128:(t + 1) * 128]


def sing_stack(x):
    lane = lax.broadcasted_iota(jnp.int32, (TOKENS, GRP_W), 1) // SING_DIM
    x = x.astype(F32)
    return cat0([jnp.where(lane == h, x, 0.0) for h in range(GRP_HEADS)]).astype(BF16)


def sing_merge(parts):
    lane = lax.broadcasted_iota(jnp.int32, (TOKENS, GRP_W), 1) // SING_DIM
    out = jnp.where(lane == 0, parts[0], 0.0)
    for h in range(1, GRP_HEADS):
        out = jnp.where(lane == h, parts[h], out)
    return out


P_GATED, P_DMID, P_X2, P_DH, P_ACT, P_DOUT = 0, 384, 768, 1152, 4224, 5760
P_NS, P_DQ = 6144, 6528


P_ALL = 8064


def sing_fused_kernel(bias_ref, heads_ref, gate_ref, s_ref, m_ref, wo_ref, wu_ref, wd_ref, wq_ref, ds_ref,
                      so_ref, dsi_ref, pk_ref, dbt_ref, qb_ref,
                      b_all, o_out, o_in, do_out, do_in, dq_out, dq_in, db_out, send, recv):
    me = lax.axis_index(GROUP_AXIS)
    greet(me)
    await_group()

    def block(ref):
        return lambda p: ref.at[p]

    def rows_block(ref):
        return lambda p: ref.at[pl.ds(pl.multiple_of(p * TOKENS, TOKENS), TOKENS), :]

    def start(i, src_at, dst_at):
        return Exchange(me, src_at, dst_at, send.at[i], recv.at[i])

    def lanes_of(x):
        return [x[:, g * GRP_W:(g + 1) * GRP_W] for g in range(GRP)]

    def rows_of(x):
        return [x[g * ROWS:(g + 1) * ROWS] for g in range(GRP)]

    stage = 0
    ex_bias = start(stage, rows_block(bias_ref), block(b_all))
    b_all[me] = bias_ref[pl.ds(pl.multiple_of(me * TOKENS, TOKENS), TOKENS), :]
    q, k, v = [cat0([heads_ref[g, t] for g in range(GRP)]) for t in range(3)]
    ks, vs = sing_stack(k), sing_stack(v)
    logits = dot_nt(ks, q) * SING_SCALE
    mask = m_ref[...]
    ex_bias.arrive()
    probs = []
    for h in range(GRP_HEADS):
        b = cat0([b_all[g, h * ROWS:(h + 1) * ROWS, :] for g in range(GRP)]).astype(F32)
        probs.append(softmax_cols(logits[h * TOKENS:(h + 1) * TOKENS] + b + mask))
    pb = [p.astype(BF16) for p in probs]
    for g, x in enumerate(rows_of(dot_tn(cat0(pb), vs))):
        o_out[g] = x
    stage += 1
    ex_o = start(stage, block(o_out), block(o_in))
    o_in[me] = o_out[me]
    gate, s = gate_ref[...], s_ref[...].astype(F32)
    ds = ds_ref[...]
    d_act = dot_nt(ds, wd_ref[...])
    n_s, r_s = norm_parts(s)
    ex_o.arrive()
    att = cat1([o_in[g] for g in range(GRP)])
    gated = (gate * att).astype(BF16)
    s_mid = (s + dot_nn(gated, wo_ref[...])).astype(BF16).astype(F32)
    nhat, r_std = norm_parts(s_mid)
    nb = nhat.astype(BF16)
    hid = dot_nn(nb, wu_ref[...])
    h1, h2 = hid[:, :4 * C_S], hid[:, 4 * C_S:]
    sg = jax.nn.sigmoid(h1)
    a1 = h1 * sg
    dhid = cat1([d_act * h2 * (sg + a1 * (1.0 - sg)), d_act * a1]).astype(BF16)
    dsm = ds.astype(F32) + norm_back(dot_nt(dhid, wu_ref[...]), nhat, r_std)
    dsmb = dsm.astype(BF16)
    d_gated = dot_nt(dsmb, wo_ref[...])
    for g, x in enumerate(lanes_of((d_gated * gate).astype(BF16))):
        do_out[g] = x
    stage += 1
    ex_do = start(stage, block(do_out), block(do_in))
    do_in[me] = do_out[me]
    act = (a1 * h2).astype(BF16)
    so_ref[...] = (s_mid + dot_nn(act, wd_ref[...])).astype(BF16)
    dgl = (d_gated * att * gate * (1.0 - gate)).astype(BF16)
    for at, x in ((P_GATED, gated), (P_DMID, dsmb), (P_X2, nb), (P_DH, dhid), (P_ACT, act), (P_DOUT, ds), (P_NS, n_s.astype(BF16))):
        pk_ref[:, at:at + x.shape[1]] = x
    ex_do.arrive()
    do = cat0([do_in[g] for g in range(GRP)])
    dp = dot_nt(vs, do)
    dsb, dk, dv = [], [], []
    for h in range(GRP_HEADS):
        d = dp[h * TOKENS:(h + 1) * TOKENS]
        dlog = probs[h] * (d - col_sum(probs[h] * d))
        for g, x in enumerate(rows_of(dlog.astype(BF16))):
            db_out[g, h * ROWS:(h + 1) * ROWS, :] = x
        dsb.append((dlog * SING_SCALE).astype(BF16))
    stage += 1
    ex_db = start(stage, block(db_out), rows_block(dbt_ref))
    rows_block(dbt_ref)(me)[...] = db_out[me]
    for h in range(GRP_HEADS):
        dk.append(dot_nn(dsb[h], q))
        dv.append(dot_nn(pb[h], do))
    for t, x in enumerate((dot_tn(cat0(dsb), ks), sing_merge(dk), sing_merge(dv))):
        for g, y in enumerate(rows_of(x.astype(BF16))):
            dq_out[g, t] = y
    stage += 1
    ex_dq = start(stage, block(dq_out), block(dq_in))
    dq_in[me] = dq_out[me]
    ex_dq.arrive()
    dp_all = cat1([dq_in[g, t] for t in range(3) for g in range(GRP)] + [dgl])
    pk_ref[:, P_DQ:] = dp_all
    dsi_ref[...] = (dsm + norm_back(dot_nt(dp_all, wq_ref[...]), n_s, r_s)).astype(BF16)
    qb = col_sum(dp_all[:, :C_S].astype(F32))
    qb_ref[...] = cat0([qb[:, t * CH:(t + 1) * CH] for t in range(3)])
    ex_db.arrive()
    for ex in (ex_bias, ex_o, ex_do, ex_db, ex_dq):
        ex.leave()


def sing_fused(*args):
    vm = pl.BlockSpec(memory_space=pltpu.VMEM)
    dma = pltpu.SemaphoreType.DMA
    piece = (GRP, ROWS, GRP_W)
    triple = (GRP, 3, ROWS, GRP_W)
    outs = (sds((ROWS, C_S), BF16), sds((ROWS, C_S), BF16), sds((ROWS, P_ALL), BF16), sds((GRP * TOKENS, TOKENS), BF16), sds((3, CH), F32))
    sems = dma((5, len(OFFSETS)))
    return pl.pallas_call(
        sing_fused_kernel, out_shape=outs, in_specs=[vm] * len(args), out_specs=(vm,) * len(outs),
        scratch_shapes=[pltpu.VMEM((GRP, TOKENS, TOKENS), BF16), pltpu.VMEM(piece, F32), pltpu.VMEM(piece, F32),
                        pltpu.VMEM(piece, BF16), pltpu.VMEM(piece, BF16), pltpu.VMEM(triple, BF16), pltpu.VMEM(triple, BF16),
                        pltpu.VMEM((GRP, TOKENS, TOKENS), BF16), sems, sems],
        compiler_params=pltpu.CompilerParams(collective_id=2, has_side_effects=True), name='sing_fused',
        cost_estimate=pl.CostEstimate(flops=2 * GIGA, bytes_accessed=NOMINAL_BYTES, transcendentals=0),
    )(*args)


QKVG, PROJ, UP, DOWN = (4360, 12, 3), (8987, 3, 1), (10139, 24, 6), (19355, 3, 3)
KEPT = (((QKVG, 0, 136),), ((QKVG, 128, 384), (PROJ, 0, 384), (UP, 0, 80)), ((UP, 72, 328),), ((UP, 320, 384), (DOWN, 0, 384)))
W_ROWS = 1632


def kept_blocks(d):
    at = 0
    for weight, lo, hi in KEPT[d]:
        for t in range(weight[-1]):
            yield weight, lo, hi, t, at
            at += hi - lo


def sing_wgrad_kernel(m_ref, o_ref):
    k = lax.axis_index(GROUP_AXIS)

    def lanes(base, tiles, idx):
        width = tiles * CH
        return m_ref[:, pl.ds(pl.multiple_of(base + idx * width, CH), width)]

    def whole(base):
        return m_ref[:, base:base + C_S]

    grads = {
        QKVG: dot_tn(whole(P_NS), lanes(P_DQ, QKVG[-1], k)),
        PROJ: dot_tn(whole(P_GATED), lanes(P_DMID, 1, jnp.minimum(k, 2))),
        UP: dot_tn(whole(P_X2), lanes(P_DH, UP[-1], k)),
        DOWN: dot_tn(lanes(P_ACT, DOWN[-1], k), whole(P_DOUT)),
    }
    for d in range(GRP):
        end = 0
        for weight, lo, hi, t, at in kept_blocks(d):
            end = at + hi - lo
            o_ref[d, at:end, :] = grads[weight][lo:hi, t * CH:(t + 1) * CH]
        if end < W_ROWS:
            o_ref[d, end:, :] = jnp.zeros((W_ROWS - end, CH), F32)


def sing_wgrad(packed_all):
    return call(sing_wgrad_kernel, [sds((4, W_ROWS, 128), F32)], flops=GIGA, name='sing_wgrad')(packed_all)


PART = 766816
OUT_ROWS = 5992
SHIFT_ROWS = 56
SMALL_AT = ((0, 2048, 4, 24), (0, 2692, 4, 32), (1, 2978, 3, 0), (1, 2981, 16, 8))
LATE_ROWS = 1536
PIECE = LATE_ROWS // 16
LATE_SIZES = (512, 128, 128, 512, 128, 128)
EARLY_SIZES = (512, 128, 512, 128, 1024, 512)
EARLY_AT = (1536, 2052, 2180, 2696, 2824, 3848)


def finish_kernel(*refs):
    late_refs, (g_ref, p_ref, small_ref, o_ref, w_ref, x_ref, buf_ref, sum_ref, copy_sem, send1, recv1, send2, recv2) = refs[:6], refs[6:]
    d, k = lax.axis_index(BATCH_AXIS), lax.axis_index(GROUP_AXIS)
    me = 4 * d + k
    row, fills = 0, []
    for i, ref in enumerate(late_refs):
        fills.append(pltpu.make_async_copy(ref, x_ref.at[pl.ds(row, LATE_SIZES[i]), :], copy_sem.at[i]))
        row += LATE_SIZES[i]
    for c in fills:
        c.start()
    barrier = pltpu.get_barrier_semaphore()

    def device(p):
        return {BATCH_AXIS: p // 4, GROUP_AXIS: lax.rem(p, 4)}

    def piece(p):
        return pl.ds(pl.multiple_of(p * PIECE, PIECE), PIECE)

    for off in range(1, N_DEV):
        pl.semaphore_signal(barrier, inc=1, device_id=device(lax.rem(me + off, N_DEV)), device_id_type=MESH_ID)
    for c in fills:
        c.wait()
    pl.semaphore_wait(barrier, 15)
    first = []
    for off in range(1, N_DEV):
        p = lax.rem(me + off, N_DEV)
        c = pltpu.make_async_remote_copy(
            src_ref=x_ref.at[piece(p), :], dst_ref=buf_ref.at[off - 1], send_sem=send1.at[off - 1], recv_sem=recv1.at[off - 1],
            device_id=device(p), device_id_type=MESH_ID)
        c.start()
        first.append(c)

    def lay_out(part):
        begin = part * PART // 128
        lanes_off = part * PART % 128
        for weight, lo, hi, t, at in kept_blocks(part):
            base, tiles, own = weight
            for k in range(GRP):
                if weight == DOWN:
                    first_row = base + own * CH * k * tiles + t - begin
                else:
                    first_row = base + own * k + t - begin
                    if own * k + t >= tiles:
                        continue
                r0 = max(lo, -(first_row // tiles))
                r1 = min(hi, (OUT_ROWS - first_row) // tiles + 1)
                src = at + r0 - lo
                w_ref[pl.ds(first_row + r0 * tiles, r1 - r0, stride=tiles), :] = g_ref[k, src:src + r1 - r0, :]
        if part:
            lane = lax.broadcasted_iota(jnp.int32, (SHIFT_ROWS, CH), 1)

            def shift(i):
                w = pltpu.roll(w_ref[pl.ds(pl.multiple_of(i * SHIFT_ROWS, PACK), SHIFT_ROWS + PACK), :], CH - lanes_off, 1)
                o_ref[chunk_ds(i, SHIFT_ROWS), :] = jnp.where(lane < CH - lanes_off, w[:SHIFT_ROWS], w[1:SHIFT_ROWS + 1])

            loop(OUT_ROWS // SHIFT_ROWS, shift)
        else:
            o_ref[LATE_ROWS:, :] = w_ref[LATE_ROWS:OUT_ROWS, :]

    for part in range(GRP):
        @pl.when(d == part)
        def _():
            if part == 0:
                src = 0
                for n, at in zip(EARLY_SIZES, EARLY_AT):
                    w_ref[at:at + n, :] = p_ref[src:src + n, :]
                    src += n
            for own, at, n, src in SMALL_AT:
                if own == part:
                    w_ref[at:at + n, :] = small_ref[src:src + n, :]
            lay_out(part)

    for c in first:
        c.wait_recv()
    total = x_ref[piece(me), :]
    for i in range(15):
        total += buf_ref[i]
    sum_ref[...] = total

    def second(k, src):
        return pltpu.make_async_remote_copy(
            src_ref=sum_ref, dst_ref=o_ref.at[piece(src), :], send_sem=send2.at[k], recv_sem=recv2.at[src],
            device_id={BATCH_AXIS: 0, GROUP_AXIS: k}, device_id_type=MESH_ID)

    for k in range(GRP):
        @pl.when(me != k)
        def _():
            second(k, me).start()

    @pl.when(d == 0)
    def _():
        o_ref[piece(me), :] = total

    for k in range(GRP):
        @pl.when(me != k)
        def _():
            second(k, me).wait_send()

    @pl.when(d == 0)
    def _():
        for off in range(1, N_DEV):
            second(0, lax.rem(me + off, N_DEV)).wait_recv()

    for c in first:
        c.wait_send()


def finish(late, g_all, early, small):
    vm = pl.BlockSpec(memory_space=pltpu.VMEM)
    dma = pltpu.SemaphoreType.DMA
    return pl.pallas_call(
        finish_kernel, out_shape=sds((OUT_ROWS, 128), F32), in_specs=[vm] * 9, out_specs=vm,
        scratch_shapes=[pltpu.VMEM((6016, 128), F32), pltpu.VMEM((LATE_ROWS, 128), F32), pltpu.VMEM((15, PIECE, 128), F32),
                        pltpu.VMEM((PIECE, 128), F32), dma((6,)), dma((15,)), dma((15,)), dma((4,)), dma((16,))],
        compiler_params=pltpu.CompilerParams(collective_id=1, has_side_effects=True), name='finish',
        cost_estimate=pl.CostEstimate(flops=GIGA, bytes_accessed=NOMINAL_BYTES, transcendentals=0),
    )(*late, g_all, early, small)


def pack_kernel(*refs):
    *srcs, o_ref = refs
    at = 0
    for ref in srcs:
        n = ref.shape[0]
        if n % PACK:
            o_ref[at:at + PACK, :] = jnp.zeros((PACK, CH), F32)
        o_ref[at:at + n, :] = ref[...]
        at += padded(n)


def padded(n):
    return -(-n // PACK) * PACK


def pack_rows(*arrays):
    return call(pack_kernel, [sds((sum(padded(a.shape[0]) for a in arrays), CH), F32)], flops=GIGA, name='pack_rows')(*arrays)


def flat_cols(x):
    return x.T.reshape(x.shape)


def device_step(single_blk, pair_blk, mask_blk, d_single_blk, d_pair_blk, *weights):
    (w1_in, w1_gate, w1_out, w2_in, w2_gate, w2_out, st_qkvg, st_bias, st_proj, en_qkvg,
     en_bias, en_proj, p_up, p_down, s_qkvg, s_qbias, s_pbias, s_proj, s_up, s_down) = weights
    s_rows = single_blk[0]
    z_zero = pair_blk[0].reshape(N_POS, CH)
    mask_bias = (mask_blk[0].astype(jnp.float32) - 1.0) * MASK_PENALTY
    mask_col = mask_bias[:, None]
    right_out = mul_proj(z_zero, w1_in)
    x_out, z_one, right_out_all, left_out, turned, right_in = mul_mix(z_zero, w1_in, right_out, z_zero, w1_gate, w1_out, w2_in)
    x_in, z_two, _, _, s_gate, s_heads = mul_mix(
        turned.reshape(N_POS, CH), w2_in, right_in, z_one, w2_gate, w2_out, single=(s_rows, s_qkvg, s_qbias[None, :]))
    z_three, bias_st = att_fwd(z_two, st_bias, mask_col, st_qkvg, st_proj)
    zt_three = z_three.reshape(N_POS, CH)
    zt_four, bias_en, dzt_out = att_fwd(zt_three, en_bias, mask_col, en_qkvg, en_proj, d_pair_blk[0])
    zt_five, bias_t, turned_five = trans_fwd(zt_four, p_up, p_down, s_pbias)
    s_out, ds_in, packed, d_bias_t, g_qb = sing_fused(
        bias_t, s_heads, s_gate, s_rows, mask_col, s_proj, s_up, s_down, s_qkvg, d_single_blk[0])
    packed, d_bias_t = lax.optimization_barrier((packed, d_bias_t))
    packed_all = gather_rows(packed)
    dzt_four, g_pup, g_pdown, g_pbt = trans_bwd(
        zt_four, zt_five, dzt_out.reshape(N_POS, CH), d_bias_t, p_up, p_down, s_pbias)
    windows = sing_wgrad(packed_all)
    dzt_four, windows = lax.optimization_barrier((dzt_four, windows))
    piece = lax.psum_scatter(windows.reshape(4 * W_ROWS, 128), BATCH_AXIS, scatter_dimension=0, tiled=True)
    dz_three, end_grads, (left_out_all,) = att_backward(zt_three, dzt_four, bias_en, mask_col, en_qkvg, en_bias, en_proj, left_out)
    dz_three, piece = lax.optimization_barrier((dz_three, piece))
    pieces = gather_rows(piece)
    dz_two, start_grads, _ = att_backward(z_two, dz_three, bias_st, mask_col, st_qkvg, st_bias, st_proj)
    dz_two, pieces = lax.optimization_barrier((dz_two, pieces))
    dx_in, dgl_in, g_in_out = mul_post_bwd(dz_two, x_in, z_one, w2_gate, w2_out, False)
    five = jnp.zeros((5, 128), F32)
    early = pack_rows(start_grads[0], start_grads[2], end_grads[0], end_grads[2], g_pup, g_pdown, g_qb, g_pbt, start_grads[1], end_grads[1])
    early, dx_in = lax.optimization_barrier((early, dx_in))
    early = lax.psum(early, (BATCH_AXIS, GROUP_AXIS))
    tail = early[sum(EARLY_SIZES):]
    small = cat0([tail[:8], flat_cols(tail[8:24]), flat_cols(tail[24:28]), five[:4], flat_cols(tail[32:36]), five[:4]])
    dz_one, g_in_in, g_in_gate = mul_pre_bwd(dx_in, None, right_in, z_one, w2_in, w2_gate, dgl_in, dz_two)
    dx_out, dgl_out, g_out_out, dx_turned = mul_post_bwd(dz_one, x_out, z_zero, w1_gate, w1_out, True)
    dz_zero, g_out_in, g_out_gate, z_five = mul_pre_bwd(
        dx_out, left_out_all, right_out_all, z_zero, w1_in, w1_gate, dgl_out, dz_one,
        dx_turned.reshape(N_POS, CH), turned_five.reshape(TURNED))
    late = (g_out_in, g_out_gate, g_out_out, g_in_in, g_in_gate, g_in_out)
    grad_flat = finish(late, pieces.reshape(4, W_ROWS, 128), early, small).reshape(-1)[:PART]
    dz_zero = dz_zero.reshape(ROWS, COLS, CH)
    return s_out[None], z_five[None], ds_in[None], dz_zero[None], grad_flat


def solution(mesh):
    spec_single = P(BATCH_AXIS, GROUP_AXIS, None)
    spec_pair = P(BATCH_AXIS, GROUP_AXIS, None, None)
    spec_mask = P(BATCH_AXIS, None)

    def block_fn(single_rep, pair_rep, token_mask, d_single_out, d_pair_out, *weights):
        in_specs = (spec_single, spec_pair, spec_mask, spec_single, spec_pair) + tuple(P() for w_item in weights)
        out_specs = (spec_single, spec_pair, spec_single, spec_pair, P(BATCH_AXIS))
        mapped = jax.shard_map(device_step, mesh=mesh, in_specs=in_specs, out_specs=out_specs, check_vma=False)
        return mapped(single_rep, pair_rep, token_mask, d_single_out, d_pair_out, *weights)

    return block_fn
```

```python
import functools
import jax
import jax.numpy as jnp
from jax import lax
from jax.experimental import pallas as pl
from jax.experimental.pallas import tpu as pltpu
from jax.sharding import PartitionSpec as P

BATCH_AXIS = 'dp'
GROUP_AXIS = 'dap'
NORM_EPS = 1e-5
MASK_PENALTY = 1.0e9


def gather_rows(x_in):
    return lax.all_gather(x_in, GROUP_AXIS, axis=0, tiled=True)


F32 = jnp.float32
NOMINAL_BYTES = 4 << 20
GIGA = 1 << 30
BF16 = jnp.bfloat16
ROWS = 32
COLS = 128
CH = 128
HALF = 2 * CH
N_POS = ROWS * COLS
TRI_HEADS = 4
GRP = 4
OFFSETS = (1, 2, 3)
MESH_ID = pl.DeviceIdType.MESH
FOUR = 8
N_DEV = 16
WIDE = FOUR * COLS
TRI_DIM = 32
TRI_SCALE = TRI_DIM ** -0.5
STEP_ROWS = 8
CHUNK = STEP_ROWS * COLS


def dot_nn(a, b):
    return lax.dot_general(a, b, (((1,), (0,)), ((), ())), preferred_element_type=F32)


def dot_nt(a, b):
    return lax.dot_general(a, b, (((1,), (1,)), ((), ())), preferred_element_type=F32)


def dot_tn(a, b):
    return lax.dot_general(a, b, (((0,), (0,)), ((), ())), preferred_element_type=F32)


def cat0(xs):
    return jnp.concatenate(xs, axis=0)


def cat1(xs):
    return jnp.concatenate(xs, axis=1)


def loop(count, step, unroll=1):
    def body(i, carry):
        step(i)
        return carry

    lax.fori_loop(0, count, body, 0, unroll=unroll)


def col_mean(x):
    return jnp.mean(x, axis=0, keepdims=True)


def col_sum(x):
    return jnp.sum(x, axis=0, keepdims=True)


def row_mean(x):
    return jnp.mean(x, axis=-1, keepdims=True)


def softmax_cols(x):
    e = jnp.exp(x - jnp.max(x, axis=0, keepdims=True))
    return e * (1.0 / col_sum(e))


def col_norm(x):
    c = x - col_mean(x)
    r = lax.rsqrt(col_mean(c * c) + NORM_EPS)
    return c * r, r


def swap_all(x, split, join):
    return lax.all_to_all(x, GROUP_AXIS, split, join, tiled=True)


def norm_parts(x):
    c = x - row_mean(x)
    r = lax.rsqrt(row_mean(c * c) + NORM_EPS)
    return c * r, r


def norm_back(dn, nhat, r):
    return r * (dn - row_mean(dn) - nhat * row_mean(dn * nhat))


def chunk_ds(t, size=CHUNK):
    return pl.ds(pl.multiple_of(t * size, size), size)


def call(kernel, out_shape, scratch=(), flops=0, name=None, comm=None):
    n_out = len(out_shape)
    vm = pl.BlockSpec(memory_space=pltpu.VMEM)

    def run(*args):
        return pl.pallas_call(
            kernel, out_shape=tuple(out_shape), in_specs=[vm] * len(args), out_specs=tuple([vm] * n_out),
            scratch_shapes=list(scratch), name=name,
            compiler_params=pltpu.CompilerParams(collective_id=comm, has_side_effects=comm is not None),
            cost_estimate=pl.CostEstimate(flops=flops, bytes_accessed=NOMINAL_BYTES, transcendentals=0),
        )(*args)

    def run_one(*args):
        return run(*args)[0]

    return run if n_out > 1 else run_one


def sds(shape, dtype):
    return jax.ShapeDtypeStruct(shape, dtype)


def greet(me):
    sem = pltpu.get_barrier_semaphore()
    for off in OFFSETS:
        pl.semaphore_signal(sem, inc=1, device_id={GROUP_AXIS: lax.rem(me + off, GRP)}, device_id_type=MESH_ID)


def await_group():
    pl.semaphore_wait(pltpu.get_barrier_semaphore(), len(OFFSETS))


class Exchange:
    def __init__(self, me, src_at, dst_at, send_sem, recv_sem):
        self.copies = []
        for i, off in enumerate(OFFSETS):
            dest = lax.rem(me + off, GRP)
            self.copies.append(pltpu.make_async_remote_copy(
                src_ref=src_at(dest), dst_ref=dst_at(me), send_sem=send_sem.at[i], recv_sem=recv_sem.at[i],
                device_id={GROUP_AXIS: dest}, device_id_type=MESH_ID))
        for c in self.copies:
            c.start()

    def arrive(self):
        for c in self.copies:
            c.wait_recv()

    def leave(self):
        for c in self.copies:
            c.wait_send()


PACK = 8
CHUNKS = 8
CHUNK_ROWS = N_POS // CHUNKS


class Gather:
    def __init__(self, me, own_ref, all_ref, send, recv):
        self.all, self.send, self.recv = all_ref, send, recv
        self.partner, self.across = me + 1 - 2 * lax.rem(me, 2), lax.rem(me + 2, GRP)
        self.far = [self.copy(own_ref.at[self.rows(c), :], me, self.across, 0, c) for c in range(CHUNKS)]
        self.near = [self.copy(own_ref.at[self.rows(c), :], me, self.partner, 1, c) for c in range(CHUNKS)]
        self.passed = []
        for c in self.far + self.near:
            c.start()
        all_ref[me] = own_ref[...]

    def rows(self, c):
        return pl.ds(c * CHUNK_ROWS, CHUNK_ROWS)

    def copy(self, src, slot, dest, kind, c):
        return pltpu.make_async_remote_copy(
            src_ref=src, dst_ref=self.all.at[slot, self.rows(c), :], send_sem=self.send.at[kind, c], recv_sem=self.recv.at[kind, c],
            device_id={GROUP_AXIS: dest}, device_id_type=MESH_ID)

    def each(self, work):
        for c in range(CHUNKS + 1):
            if c < CHUNKS:
                self.far[c].wait_recv()
                self.passed.append(self.copy(self.all.at[self.across, self.rows(c), :], self.across, self.partner, 2, c))
                self.passed[c].start()
            if c:
                self.near[c - 1].wait_recv()
                self.passed[c - 1].wait_recv()
                loop(CH // CHUNKS, lambda k: work(k + (c - 1) * (CH // CHUNKS)), PACK)

    def pass_on(self):
        for c in range(CHUNKS):
            self.far[c].wait_recv()
            self.passed.append(self.copy(self.all.at[self.across, self.rows(c), :], self.across, self.partner, 2, c))
            self.passed[c].start()

    def arrive(self):
        for c in self.near + self.passed:
            c.wait_recv()

    def leave(self):
        for c in self.far + self.near + self.passed:
            c.wait_send()


def gather_sems():
    sems = pltpu.SemaphoreType.DMA((3, CHUNKS))
    return [sems, sems]


def own_rows(p, size=ROWS):
    return pl.ds(pl.multiple_of(p * size, size), size)


class Turn:
    def __init__(self, me, scr_ref, stage_ref, out_ref, send, recv):
        self.me, self.scr, self.stage, self.out, self.send, self.recv = me, scr_ref, stage_ref, out_ref, send, recv
        self.sent = []

    def half(self, n):
        lo = n * HALF_ROWS

        def cast(j):
            rows = self.scr[pl.ds(pl.multiple_of(j * ROWS + lo, HALF_ROWS), HALF_ROWS), :]
            self.stage[j // ROWS, lax.rem(j, ROWS), lo:lo + HALF_ROWS, :] = rows.astype(BF16)

        loop(COLS, cast, FOUR)
        part = (slice(None), slice(lo, lo + HALF_ROWS))
        self.sent.append(Exchange(self.me, lambda p: self.stage.at[(p, *part)], lambda m: self.out.at[(m, *part)], self.send.at[n], self.recv.at[n]))

    def finish(self):
        self.out[self.me] = self.stage[self.me]
        for ex in self.sent:
            ex.arrive()
            ex.leave()


TURNED = (GRP, ROWS, ROWS, CH)
HALF_ROWS = ROWS // 2


def turn_scratch():
    sems = pltpu.SemaphoreType.DMA((2, len(OFFSETS)))
    return [pltpu.VMEM((N_POS, CH), F32), pltpu.VMEM(TURNED, BF16), sems, sems]


def peer_sems():
    sems = pltpu.SemaphoreType.DMA((len(OFFSETS),))
    return [sems, sems]


ATT_STEP = 8
BWD_STEP = 8


def fill_bias(bias_ref, mask_ref, bm_ref):
    mask = mask_ref[...]
    for h in range(TRI_HEADS):
        cols = slice(h * COLS, (h + 1) * COLS)
        bm_ref[:, cols] = bias_ref[:, cols].astype(F32).T + mask


def head_rows(x, h):
    return x[h * TRI_DIM:(h + 1) * TRI_DIM]


def spread_heads(xt):
    zero = jnp.zeros((TRI_DIM, COLS), xt.dtype)
    return cat1([
        cat0([head_rows(xt, h) if g == h else zero for g in range(TRI_HEADS)])
        for h in range(TRI_HEADS)])


def probs_of(k, q_wide, bm_ref):
    x = dot_nn(k, q_wide) * TRI_SCALE + bm_ref[...]
    return softmax_cols(x)


def heads_nn(xt, wide):
    return cat0([dot_nn(head_rows(xt, h), wide[:, h * COLS:(h + 1) * COLS]) for h in range(TRI_HEADS)])


def att_fwd_kernel(ending, z_ref, wbt_ref, mask_ref, w_ref, wo_ref, *rest):
    *rest, wt_ref = rest
    wt_ref[...] = w_ref[...].T
    if ending:
        dp_ref, o_ref, bias_ref, dpt_ref, bm_ref, own_ref, send, recv, dp_send, dp_recv = rest
    else:
        o_ref, bias_ref, bm_ref, own_ref, send, recv, *rest = rest
    me = lax.axis_index(GROUP_AXIS)
    greet(me)
    turn = None if ending else Turn(me, rest[0], rest[1], o_ref, *rest[2:])

    def bias_step(t):
        nhat, _ = norm_parts(cat0([load_row(z_ref, t * PACK + r, ending) for r in range(PACK)]).astype(F32))
        nb = nhat.astype(BF16)
        b = [dot_nt(wbt_ref[...], nb[r * COLS:(r + 1) * COLS]) for r in range(PACK)]
        for h in range(TRI_HEADS):
            own_ref[chunk_ds(t, PACK), h * COLS:(h + 1) * COLS] = cat0([x[h:h + 1, :] for x in b])

    loop(ROWS // PACK, bias_step)
    bias_ref[own_rows(me), :] = own_ref[...].astype(BF16)
    await_group()
    ex = Exchange(me, lambda p: bias_ref.at[own_rows(me), :], lambda m: bias_ref.at[own_rows(m), :], send, recv)
    ex.arrive()
    if ending:
        ex_dp = Exchange(me, lambda p: dp_ref.at[:, own_rows(p), :], lambda m: dpt_ref.at[m], dp_send, dp_recv)
        dpt_ref[me] = dp_ref[:, own_rows(me), :]
    fill_bias(bias_ref, mask_ref, bm_ref)

    def step(t):
        z = cat0([load_row(z_ref, t * ATT_STEP + r, ending) for r in range(ATT_STEP)]).astype(F32)
        nhat, _ = norm_parts(z)
        nb = nhat.astype(BF16)
        qt_all = dot_nt(wt_ref[:CH, :], nb)
        k_all = dot_nt(nb, wt_ref[CH:HALF, :]).astype(BF16)
        vg_all = dot_nt(wt_ref[HALF:, :], nb)
        gate = jax.nn.sigmoid(vg_all[CH:])
        outs = []
        for r in range(ATT_STEP):
            cols = slice(r * COLS, (r + 1) * COLS)
            q_wide = spread_heads(qt_all[:, cols]).astype(BF16)
            probs = probs_of(k_all[cols], q_wide, bm_ref).astype(BF16)
            outs.append(heads_nn(vg_all[:CH, cols].astype(BF16), probs))
        gated = (gate * cat1(outs)).astype(BF16)
        out = z + dot_tn(gated, wo_ref[...])
        for r in range(ATT_STEP):
            rows = slice(r * COLS, (r + 1) * COLS)
            if turn is None:
                o_ref[chunk_ds(t * ATT_STEP + r, COLS), :] = out[rows].astype(BF16)
            else:
                put_strided(turn.scr, t * ATT_STEP + r, out[rows])

    halves(ROWS // ATT_STEP, step, turn)
    ex.leave()
    if ending:
        ex_dp.arrive()
        ex_dp.leave()


def halves(count, step, turn, filler=None):
    if turn is None:
        loop(count, step)
        return
    loop(count // 2, step)
    turn.half(0)
    loop(count // 2, lambda t: step(t + count // 2))
    turn.half(1)
    if filler:
        filler()
    turn.finish()


def att_fwd(z, w_b, mask_col, wt, w_o, d_pair=None):
    ending = d_pair is not None
    scr = [pltpu.VMEM((COLS, TRI_HEADS * COLS), F32), pltpu.VMEM((ROWS, TRI_HEADS * COLS), F32)] + peer_sems()
    outs = [sds((N_POS, CH) if ending else TURNED, BF16), sds((COLS, TRI_HEADS * COLS), BF16)]
    args = [z, w_b.T, mask_col, wt, w_o]
    if ending:
        outs.append(sds(TURNED, BF16))
        args.append(d_pair)
    return call(functools.partial(att_fwd_kernel, ending), outs, scr + (peer_sems() if ending else turn_scratch()) + [pltpu.VMEM((4 * CH, CH), BF16)],
                flops=3 * GIGA, name='att_fwd', comm=4 if ending else 3)(*args)


def att_bwd_kernel(ending, z_ref, dz_ref, bias_ref, mask_ref, w_ref, wo_ref, *rest):
    *rest, wt_ref = rest
    wt_ref[...] = w_ref[...].T
    z_blocked, dz_blocked = ending, not ending
    if ending:
        own_ref, all_ref, *rest = rest
        *rest, send, recv = rest
        me = lax.axis_index(GROUP_AXIS)
        greet(me)
        await_group()
        gather = Gather(me, own_ref, all_ref, send, recv)
    dzo_ref, dwr_ref, dwo_ref, db_ref, bm_ref, acc_ref, dwqg_ref, dwkv_ref = rest
    fill_bias(bias_ref, mask_ref, bm_ref)
    acc_ref[...] = jnp.zeros_like(acc_ref)
    dwqg_ref[...] = jnp.zeros_like(dwqg_ref)
    dwkv_ref[...] = jnp.zeros_like(dwkv_ref)
    dwo_ref[...] = jnp.zeros_like(dwo_ref)

    def step(t):
        nhat, r_std = norm_parts(cat0([load_row(z_ref, t * BWD_STEP + r, z_blocked) for r in range(BWD_STEP)]).astype(F32))
        nb = nhat.astype(BF16)
        pt_all = dot_nt(wt_ref[...], nb)
        kv_all = dot_nt(nb, wt_ref[CH:3 * CH, :]).astype(BF16)
        gate = jax.nn.sigmoid(pt_all[3 * CH:])
        dz = cat0([load_row(dz_ref, t * BWD_STEP + r, dz_blocked) for r in range(BWD_STEP)])
        d_gated = dot_nt(wo_ref[...], dz)
        d_att = d_gated * gate
        outs, dqs, dkvs = [], [], []
        for r in range(BWD_STEP):
            cols = slice(r * COLS, (r + 1) * COLS)
            q_wide = spread_heads(pt_all[:CH, cols]).astype(BF16)
            do_wide = spread_heads(d_att[:, cols]).astype(BF16)
            p = probs_of(kv_all[cols, :CH], q_wide, bm_ref)
            pb = p.astype(BF16)
            outs.append(heads_nn(pt_all[2 * CH:3 * CH, cols].astype(BF16), pb))
            dp = dot_nn(kv_all[cols, CH:], do_wide)
            ds = p * (dp - col_sum(dp * p))
            acc_ref[...] += ds
            dsb = (ds * TRI_SCALE).astype(BF16)
            dqs.append(heads_nn(pt_all[CH:2 * CH, cols].astype(BF16), dsb))
            dkvs.append(cat1([dot_nt(dsb, q_wide), dot_nt(pb, do_wide)]).astype(BF16))
        o = cat1(outs)
        gated = (gate * o).astype(BF16)
        dgl = d_gated * o * gate * (1.0 - gate)
        dqg = cat0([cat1(dqs), dgl]).astype(BF16)
        dkv = cat0(dkvs)
        dwo_ref[...] += dot_nn(gated, dz)
        dwqg_ref[...] += dot_nn(dqg, nb)
        dwkv_ref[...] += dot_tn(nb, dkv)
        dn = dot_nn(dkv, wt_ref[CH:3 * CH, :]) + dot_tn(dqg[:CH], wt_ref[:CH, :]) + dot_tn(dqg[CH:], wt_ref[3 * CH:, :])
        dzo_ref[chunk_ds(t, BWD_STEP * COLS), :] = (dz.astype(F32) + norm_back(dn, nhat, r_std)).astype(BF16)

    loop(ROWS // BWD_STEP, step)
    if ending:
        gather.pass_on()
    for h in range(TRI_HEADS):
        cols = slice(h * COLS, (h + 1) * COLS)
        db_ref[:, cols] = acc_ref[:, cols].T
    for m in range(2):
        dwr_ref[pl.ds(3 * m, CH, stride=4), :] = dwqg_ref[m * CH:(m + 1) * CH, :].T
        dwr_ref[pl.ds(1 + m, CH, stride=4), :] = dwkv_ref[:, m * CH:(m + 1) * CH]
    if ending:
        gather.arrive()
        gather.leave()


def att_bwd(z, dz, bias_all, mask_col, wt, w_o, left=None):
    ending = left is not None
    outs = [sds((N_POS, CH), BF16), sds((4 * CH, CH), F32), sds((CH, CH), F32), sds((COLS, TRI_HEADS * COLS), F32)]
    wide = pltpu.VMEM((COLS, TRI_HEADS * COLS), F32)
    scr = [wide, wide, pltpu.VMEM((HALF, CH), F32), pltpu.VMEM((CH, HALF), F32)]
    args = [z, dz, bias_all, mask_col, wt, w_o]
    if ending:
        outs = [sds((GRP, N_POS, CH), BF16)] + outs
        scr = scr + gather_sems()
        args.append(left)
    scr.append(pltpu.VMEM((4 * CH, CH), BF16))
    return call(functools.partial(att_bwd_kernel, ending), outs, scr, flops=8 * GIGA, name='att_bwd', comm=9 if ending else None)(*args)


def bias_bwd_kernel(ending, z_ref, dz_ref, db_ref, wbt_ref, dzo_ref, dwt_ref, parts_ref, send, recv, *rest):
    me = lax.axis_index(GROUP_AXIS)
    greet(me)
    turn = Turn(me, rest[0], rest[1], dzo_ref, *rest[2:]) if ending else None
    dwt_ref[...] = jnp.zeros_like(dwt_ref)
    wbt = wbt_ref[...]
    await_group()
    ex = Exchange(me, lambda p: db_ref.at[own_rows(p), :], lambda m: parts_ref.at[m], send, recv)
    parts_ref[me] = db_ref[own_rows(me), :]
    ex.arrive()

    def step(t):
        block = sum(parts_ref[g, chunk_ds(t, PACK), :] for g in range(GRP))
        nhat, r_std = norm_parts(cat0([load_row(z_ref, t * PACK + r, ending) for r in range(PACK)]).astype(F32))
        nb = nhat.astype(BF16)
        dwt = jnp.zeros((TRI_HEADS, CH), F32)
        dns = []
        for r in range(PACK):
            db = cat0([block[r:r + 1, h * COLS:(h + 1) * COLS] for h in range(TRI_HEADS)]).astype(BF16)
            dwt += dot_nn(db, nb[r * COLS:(r + 1) * COLS])
            dns.append(dot_tn(db, wbt))
        out = dz_ref[chunk_ds(t, PACK * COLS), :].astype(F32) + norm_back(cat0(dns), nhat, r_std)
        if turn is None:
            dzo_ref[chunk_ds(t, PACK * COLS), :] = out.astype(BF16)
        else:
            for r in range(PACK):
                put_strided(turn.scr, t * PACK + r, out[r * COLS:(r + 1) * COLS])
        dwt_ref[...] += dwt

    halves(ROWS // PACK, step, turn)
    ex.leave()


def bias_bwd(z, dz, db, w_b, ending):
    scr = [pltpu.VMEM((GRP, ROWS, TRI_HEADS * COLS), F32)] + peer_sems()
    out = sds(TURNED if ending else (N_POS, CH), BF16)
    return call(functools.partial(bias_bwd_kernel, ending), [out, sds((TRI_HEADS, CH), F32)],
                scr + turn_scratch() if ending else scr, flops=GIGA, name='bias_bwd', comm=6 if ending else 5,
                )(z, dz, db, w_b.T)


SING_HEADS = 16


def trans_fwd_kernel(z_ref, wu_ref, wd_ref, wpt_ref, o_ref, b_ref, turned_ref, scr_ref, turn_ref):
    def step(t):
        z = z_ref[chunk_ds(t), :].astype(F32)
        nhat, _ = norm_parts(z)
        hid = dot_nn(nhat.astype(BF16), wu_ref[...])
        h1, h2 = hid[:, :4 * CH], hid[:, 4 * CH:]
        act = (jax.nn.sigmoid(h1) * h1 * h2).astype(BF16)
        out = (z + dot_nn(act, wd_ref[...])).astype(BF16)
        o_ref[chunk_ds(t), :] = out
        for r in range(STEP_ROWS):
            put_strided(turn_ref, t * STEP_ROWS + r, out[r * COLS:(r + 1) * COLS].astype(F32))
        n5, _ = norm_parts(out.astype(F32))
        n5 = n5.astype(BF16)
        for r in range(STEP_ROWS):
            scr_ref[pl.ds(t * STEP_ROWS + r, SING_HEADS, stride=ROWS), :] = dot_nt(wpt_ref[...], n5[r * COLS:(r + 1) * COLS])

    loop(ROWS // STEP_ROWS, step)
    b_ref[...] = scr_ref[...].astype(BF16)
    cast_out(turn_ref, turned_ref)


def trans_fwd(z, w_up, w_down, w_pb):
    return call(trans_fwd_kernel, [sds((N_POS, CH), BF16), sds((SING_HEADS * ROWS, COLS), BF16), sds((N_POS, CH), BF16)],
                [pltpu.VMEM((SING_HEADS * ROWS, COLS), F32), pltpu.VMEM((N_POS, CH), F32)],
                flops=2 * GIGA, name='trans_fwd')(z, w_up, w_down, w_pb.T)


def trans_bwd_kernel(z_ref, z5_ref, dz_ref, db_ref, wu_ref, wd_ref, wpt_ref,
                     dzo_ref, dwr_ref, dwd_ref, dwpt_ref, dwu_ref, scr_ref, dzs_ref):

    def convert(t):
        dzs_ref[chunk_ds(t, WIDE), :] = dz_ref[chunk_ds(t, WIDE), :].astype(F32)

    loop(N_POS // WIDE, convert)

    def dz_row(j):
        return cat0([dzs_ref[pl.ds(g * ROWS * ROWS + j, ROWS, stride=ROWS), :] for g in range(GRP)])

    dwu_ref[...] = jnp.zeros_like(dwu_ref)
    dwd_ref[...] = jnp.zeros_like(dwd_ref)
    dwpt_ref[...] = jnp.zeros_like(dwpt_ref)
    scr_ref[...] = db_ref[...].astype(F32)

    def step(t):
        n5, r5 = norm_parts(z5_ref[chunk_ds(t), :].astype(F32))
        n5b = n5.astype(BF16)
        dn5 = []
        for r in range(STEP_ROWS):
            db = scr_ref[pl.ds(t * STEP_ROWS + r, SING_HEADS, stride=ROWS), :].astype(BF16)
            dwpt_ref[...] += dot_nn(db, n5b[r * COLS:(r + 1) * COLS])
            dn5.append(dot_tn(db, wpt_ref[...]))
        dz = cat0([dz_row(t * STEP_ROWS + r) for r in range(STEP_ROWS)]) + norm_back(cat0(dn5), n5, r5)
        dzb = dz.astype(BF16)
        nhat, r_std = norm_parts(z_ref[chunk_ds(t), :].astype(F32))
        nb = nhat.astype(BF16)
        hid = dot_nn(nb, wu_ref[...])
        h1, h2 = hid[:, :4 * CH], hid[:, 4 * CH:]
        sg = jax.nn.sigmoid(h1)
        a1 = h1 * sg
        d_act = dot_nt(dzb, wd_ref[...])
        dwd_ref[...] += dot_tn((a1 * h2).astype(BF16), dzb)
        dhid = cat1([d_act * h2 * (sg + a1 * (1.0 - sg)), d_act * a1]).astype(BF16)
        dwu_ref[...] += dot_tn(nb, dhid)
        dn = dot_nt(dhid, wu_ref[...])
        dzo_ref[chunk_ds(t), :] = (dz + norm_back(dn, nhat, r_std)).astype(BF16)

    loop(ROWS // STEP_ROWS, step)
    store_rows(dwr_ref, dwu_ref[...], PACK)


def trans_bwd(z, z5, dz, db, w_up, w_down, w_pb):
    outs = [sds((N_POS, CH), BF16), sds((8 * CH, CH), F32), sds((4 * CH, CH), F32), sds((SING_HEADS, CH), F32)]
    scr = [pltpu.VMEM((CH, 8 * CH), F32), pltpu.VMEM((SING_HEADS * ROWS, COLS), F32), pltpu.VMEM((N_POS, CH), F32)]
    return call(trans_bwd_kernel, outs, scr, flops=6 * GIGA, name='trans_bwd')(z, z5, dz, db, w_up, w_down, w_pb.T)


def load_row(ref, i, blocked):
    if not blocked:
        return ref[chunk_ds(i, COLS), :]
    return cat0([ref[pl.ds(pl.multiple_of(s * ROWS * ROWS + i * ROWS, ROWS), ROWS), :] for s in range(GRP)])


def load_rows(ref, t, blocked):
    if not blocked:
        return ref[chunk_ds(t), :]
    return cat0([load_row(ref, t * STEP_ROWS + r, True) for r in range(STEP_ROWS)])


def put_strided(scr_ref, i, value):
    scr_ref[pl.ds(i, COLS, stride=ROWS), :] = value


def get_strided(scr_ref, i):
    return scr_ref[pl.ds(i, COLS, stride=ROWS), :]


def get_four(scr_ref, t):
    return cat1([get_strided(scr_ref, t * FOUR + r) for r in range(FOUR)])


def cast_out(scr_ref, o_ref):
    def step(t):
        o_ref[chunk_ds(t, 256), :] = scr_ref[chunk_ds(t, 256), :].astype(BF16)

    loop(N_POS // 256, step)


def group_rows(ref, c):
    return cat0([ref[s, chunk_ds(c, ROWS), :] for s in range(GRP)])


def project(z_ref, wt_ref, scr_ref, out_ref, blocked):
    def step(t):
        z = cat0([load_row(z_ref, t * FOUR + r, blocked) for r in range(FOUR)]).astype(F32)
        nhat, _ = norm_parts(z)
        pt = dot_nt(wt_ref[...], nhat.astype(BF16))
        val = jax.nn.sigmoid(pt[CH:]) * pt[:CH]
        for r in range(FOUR):
            put_strided(scr_ref, t * FOUR + r, val[:, r * COLS:(r + 1) * COLS])

    loop(ROWS // FOUR, step)
    cast_out(scr_ref, out_ref)


def proj_kernel(z_ref, w_ref, o_ref, scr_ref, wt_ref):
    wt_ref[...] = w_ref[:, HALF:].T
    project(z_ref, wt_ref, scr_ref, o_ref, False)


def mul_proj(z, w):
    return call(proj_kernel, [sds((N_POS, CH), BF16)], [pltpu.VMEM((N_POS, CH), F32), pltpu.VMEM((HALF, CH), BF16)],
                flops=GIGA, name='mul_proj')(z, w)


def sing_heads(me, s_ref, w_ref, qb_ref, gate_ref, out_ref, in_ref, send, recv):
    nhat, _ = norm_parts(s_ref[...].astype(F32))
    p_all = dot_nn(nhat.astype(BF16), w_ref[...])
    gate_ref[...] = jax.nn.sigmoid(p_all[:, 3 * C_S:])
    qkv = cat1([p_all[:, :C_S] + qb_ref[...].astype(F32), p_all[:, C_S:3 * C_S]]).astype(BF16)
    for t in range(3):
        for g in range(GRP):
            at = t * C_S + g * GRP_W
            out_ref[g, t] = qkv[:, at:at + GRP_W]
    in_ref[me] = out_ref[me]
    return Exchange(me, lambda p: out_ref.at[p], lambda m: in_ref.at[m], send, recv)


def make_mix(outgoing):
    def kernel(*refs):
        turn = None
        me = lax.axis_index(GROUP_AXIS)
        greet(me)
        if outgoing:
            (zl_ref, wl_ref, own_ref, z_ref, wg_ref, wo_ref, wn_ref, x_ref, o_ref, right_ref, left_ref, turned_ref, next_ref,
             scr_ref, stage_ref, send, recv, g_send, g_recv, wt_ref) = refs
            turn = Turn(me, scr_ref, stage_ref, turned_ref, send, recv)
        else:
            (zl_ref, wl_ref, own_ref, z_ref, wg_ref, wo_ref, s_ref, wq_ref, qb_ref, x_ref, o_ref, right_ref, left_ref, gate_ref, heads_ref,
             heads_out, send, recv, g_send, g_recv, wt_ref) = refs
        await_group()
        gather = Gather(me, own_ref, right_ref, g_send, g_recv)
        ex = None if outgoing else sing_heads(me, s_ref, wq_ref, qb_ref, gate_ref, heads_out, heads_ref, send, recv)
        wt_ref[...] = wl_ref[:, :HALF].T
        project(zl_ref, wt_ref, x_ref, left_ref, not outgoing)

        def mix(c):
            a = left_ref[chunk_ds(c, ROWS), :]
            b = group_rows(right_ref, c)
            x_ref[chunk_ds(c, ROWS), :] = dot_nt(a, b) if outgoing else dot_nn(a, b)

        gather.each(mix)

        def step(t):
            x = get_four(x_ref, t)
            xb = col_norm(x)[0].astype(BF16)
            z = z_ref[chunk_ds(t, WIDE), :].astype(F32)
            nhat, _ = norm_parts(z)
            gate = jax.nn.sigmoid(dot_nn(nhat.astype(BF16), wg_ref[...]))
            out = z + gate * dot_tn(xb, wo_ref[...])
            if outgoing:
                for r in range(FOUR):
                    put_strided(turn.scr, t * FOUR + r, out[r * COLS:(r + 1) * COLS])
            o_ref[chunk_ds(t, WIDE), :] = out.astype(BF16)

        def following():
            wt_ref[...] = wn_ref[:, HALF:].T
            project(o_ref, wt_ref, scr_ref, next_ref, False)

        halves(ROWS // FOUR, step, turn, following)
        gather.leave()
        if ex is not None:
            ex.arrive()
            ex.leave()

    return kernel


def mul_mix(z_left, wt_left, right, z, w_gate, w_out, wt_next=None, single=None):
    outgoing = single is None
    flat = sds((N_POS, CH), BF16)
    outs = [sds((N_POS, COLS), F32), flat, sds((GRP, N_POS, CH), BF16), flat]
    scr = gather_sems() + [pltpu.VMEM((HALF, CH), BF16)]
    if outgoing:
        outs += [sds(TURNED, BF16), flat]
        scr = turn_scratch() + scr
    else:
        heads = (GRP, 3, ROWS, GRP_W)
        outs += [sds((ROWS, C_S), F32), sds(heads, BF16)]
        scr = [pltpu.VMEM(heads, BF16)] + peer_sems() + scr
    return call(make_mix(outgoing), outs, scr, flops=3 * GIGA, name='mul_mix', comm=7 if outgoing else 10)(z_left, wt_left, right, z, w_gate, w_out, *(single or (wt_next,)))


def make_post_bwd(outgoing):
    def kernel(dz_ref, x_ref, z_ref, wg_ref, wo_ref, dx_ref, dgl_ref, dwo_ref, *rest):
        scr_ref, rest = rest[-1], rest[:-1]
        turn = None
        if outgoing:
            me = lax.axis_index(GROUP_AXIS)
            greet(me)
            turned_ref, turn_scr, stage_ref, send, recv = rest
            turn = Turn(me, turn_scr, stage_ref, turned_ref, send, recv)
        dwo_ref[...] = jnp.zeros_like(dwo_ref)

        def step(t):
            x = get_four(x_ref, t)
            xhat, r = col_norm(x)
            xb = xhat.astype(BF16)
            nhat, _ = norm_parts(z_ref[chunk_ds(t, WIDE), :].astype(F32))
            gate = jax.nn.sigmoid(dot_nn(nhat.astype(BF16), wg_ref[...]))
            du = dz_ref[chunk_ds(t, WIDE), :].astype(F32)
            dy = (gate * du).astype(BF16)
            dgl_ref[chunk_ds(t, WIDE), :] = (dot_tn(xb, wo_ref[...]) * du * gate * (1.0 - gate)).astype(BF16)
            dwo_ref[...] += dot_nn(xb, dy)
            dn = dot_nt(wo_ref[...], dy)
            dx = r * (dn - col_mean(dn) - xhat * col_mean(dn * xhat))
            for r in range(FOUR):
                part = dx[:, r * COLS:(r + 1) * COLS]
                put_strided(scr_ref, t * FOUR + r, part)
                if outgoing:
                    put_strided(turn.scr, t * FOUR + r, part.T)

        if outgoing:
            await_group()
        def store_dx():
            cast_out(scr_ref, dx_ref)

        halves(ROWS // FOUR, step, turn, store_dx)
        if not outgoing:
            store_dx()

    return kernel


def mul_post_bwd(dz, x, z, w_gate, w_out, outgoing):
    outs = [sds((N_POS, COLS), BF16), sds((N_POS, CH), BF16), sds((CH, CH), F32)]
    scr = [pltpu.VMEM((N_POS, CH), F32)]
    if outgoing:
        outs.append(sds(TURNED, BF16))
        scr = turn_scratch() + scr
    return call(make_post_bwd(outgoing), outs, scr, flops=3 * GIGA, name='mul_post_bwd', comm=8 if outgoing else None)(dz, x, z, w_gate, w_out)


def make_pre_bwd(outgoing):
    def kernel(*refs):
        *refs, wt_ref = refs
        if outgoing:
            (dx_ref, dxr_ref, left_ref, right_ref, z_ref, w_ref, wg_ref, dgl_ref, dz_ref, turned_ref, dzo_ref, dwr_ref, dwg_ref, zrow_ref,
             da_ref, db_ref, dwt_ref, scr_ref, send, recv) = refs
            me = lax.axis_index(GROUP_AXIS)
            greet(me)
            await_group()
            ex = Exchange(me, lambda p: turned_ref.at[p], lambda m: zrow_ref.at[:, own_rows(m), :], send, recv)
            zrow_ref[:, own_rows(me), :] = turned_ref[me]
            wt_ref[...] = w_ref[...].T

            def turn(j):
                put_strided(scr_ref, j, load_row(dxr_ref, j, True).astype(F32).T)

            loop(ROWS, turn, 2)

            def mix(c):
                da_ref[chunk_ds(c, ROWS), :] = dot_nn(dx_ref[chunk_ds(c, ROWS), :], group_rows(right_ref, c))
                db_ref[chunk_ds(c, ROWS), :] = dot_nn(scr_ref[chunk_ds(c, ROWS), :].astype(BF16), group_rows(left_ref, c))
        else:
            (own_ref, right_ref, z_ref, w_ref, wg_ref, dgl_ref, dz_ref, dzo_ref, dwr_ref, dwg_ref, da_ref, db_ref, dwt_ref,
             dx_ref, left_ref, pt_ref, send, recv) = refs
            me = lax.axis_index(GROUP_AXIS)
            greet(me)
            await_group()
            gather = Gather(me, own_ref, dx_ref, send, recv)
            wt_ref[...] = w_ref[...].T

            def prepare(t):
                nb = norm_parts(z_ref[chunk_ds(t, WIDE), :].astype(F32))[0].astype(BF16)
                pt = dot_nt(wt_ref[...], nb)
                pt_ref[t] = pt
                val = jax.nn.sigmoid(pt[CH:HALF]) * pt[:CH]
                for r in range(FOUR):
                    put_strided(da_ref, t * FOUR + r, val[:, r * COLS:(r + 1) * COLS])

            loop(ROWS // FOUR, prepare)
            cast_out(da_ref, left_ref)

            def mix(c):
                dx = group_rows(dx_ref, c)
                da_ref[chunk_ds(c, ROWS), :] = dot_nt(right_ref[chunk_ds(c, ROWS), :], dx)
                db_ref[chunk_ds(c, ROWS), :] = dot_nn(left_ref[chunk_ds(c, ROWS), :], dx)

        if outgoing:
            loop(CH, mix, PACK)
        else:
            gather.each(mix)
        dwt_ref[...] = jnp.zeros_like(dwt_ref)
        dwg_ref[...] = jnp.zeros_like(dwg_ref)

        def step(t):
            nhat, r_std = norm_parts(z_ref[chunk_ds(t, WIDE), :].astype(F32))
            nb = nhat.astype(BF16)
            pt = dot_nt(wt_ref[...], nb) if outgoing else pt_ref[t]
            parts = []
            for m, d_ref in enumerate((da_ref, db_ref)):
                d = get_four(d_ref, t)
                val = pt[2 * m * CH:(2 * m + 1) * CH]
                sg = jax.nn.sigmoid(pt[(2 * m + 1) * CH:(2 * m + 2) * CH])
                dv = d * sg
                parts += [dv, dv * val * (1.0 - sg)]
            dpt = cat0(parts).astype(BF16)
            dgl = dgl_ref[chunk_ds(t, WIDE), :]
            dwt_ref[...] += dot_nn(dpt, nb)
            dwg_ref[...] += dot_tn(nb, dgl)
            dn = dot_tn(dpt, wt_ref[...]) + dot_nt(dgl, wg_ref[...])
            dzo_ref[chunk_ds(t, WIDE), :] = (dz_ref[chunk_ds(t, WIDE), :].astype(F32) + norm_back(dn, nhat, r_std)).astype(BF16)

        loop(ROWS // FOUR, step)
        for t in range(GRP):
            dwr_ref[pl.ds(t, CH, stride=GRP), :] = dwt_ref[t * CH:(t + 1) * CH, :].T
        if outgoing:
            ex.arrive()
            ex.leave()
        else:
            gather.leave()

    return kernel


def mul_pre_bwd(dx, left, right, z, wt, w_gate, dgl, dz, dx_turned=None, z_turned=None):
    outgoing = dx_turned is not None
    args = [dx] + ([dx_turned, left] if outgoing else []) + [right, z, wt, w_gate, dgl, dz] + ([z_turned] if outgoing else [])
    outs = [sds((N_POS, CH), BF16), sds((4 * CH, CH), F32), sds((CH, CH), F32)]
    block = pltpu.VMEM((N_POS, CH), F32)
    scr = [block, block, pltpu.VMEM((4 * CH, CH), F32)]
    if outgoing:
        outs.append(sds((ROWS, COLS, CH), BF16))
        scr += [block] + peer_sems()
    else:
        scr += [pltpu.VMEM((GRP, N_POS, CH), BF16), pltpu.VMEM((N_POS, CH), BF16), pltpu.VMEM((ROWS // FOUR, 4 * CH, WIDE), F32)] + gather_sems()
    return call(make_pre_bwd(outgoing), outs, scr + [pltpu.VMEM((4 * CH, CH), BF16)],
                flops=6 * GIGA, name='mul_pre_bwd', comm=12 if outgoing else 11)(*args)


def att_backward(z, dz, bias_all, mask_col, w_qkvg, w_tb, w_o, left=None):
    *left_all, dz_part, g_qkvg, g_out, db = att_bwd(z, dz, bias_all, mask_col, w_qkvg, w_o, left)
    dz_new, g_bt = bias_bwd(z, dz_part, db, w_tb, left is not None)
    return dz_new.reshape(N_POS, CH), [g_qkvg, g_bt, g_out], left_all


C_S = 384
SING_DIM = 24
SING_SCALE = SING_DIM ** -0.5
GRP_HEADS = SING_HEADS // GRP
GRP_W = GRP_HEADS * SING_DIM
TOKENS = 128


def store_rows(out_ref, value, tiles):
    n = value.shape[0]
    if tiles == 1:
        out_ref[...] = value
        return
    for t in range(tiles):
        out_ref[pl.ds(t, n, stride=tiles), :] = value[:, t * 128:(t + 1) * 128]


def sing_stack(x):
    lane = lax.broadcasted_iota(jnp.int32, (TOKENS, GRP_W), 1) // SING_DIM
    x = x.astype(F32)
    return cat0([jnp.where(lane == h, x, 0.0) for h in range(GRP_HEADS)]).astype(BF16)


def sing_merge(parts):
    lane = lax.broadcasted_iota(jnp.int32, (TOKENS, GRP_W), 1) // SING_DIM
    out = jnp.where(lane == 0, parts[0], 0.0)
    for h in range(1, GRP_HEADS):
        out = jnp.where(lane == h, parts[h], out)
    return out


P_GATED, P_DMID, P_X2, P_DH, P_ACT, P_DOUT = 0, 384, 768, 1152, 4224, 5760
P_NS, P_DQ = 6144, 6528


P_ALL = 8064


def sing_fused_kernel(bias_ref, heads_ref, gate_ref, s_ref, m_ref, wo_ref, wu_ref, wd_ref, wq_ref, ds_ref,
                      so_ref, dsi_ref, pk_ref, dbt_ref, qb_ref,
                      b_all, o_out, o_in, do_out, do_in, dq_out, dq_in, db_out, send, recv):
    me = lax.axis_index(GROUP_AXIS)
    greet(me)
    await_group()

    def block(ref):
        return lambda p: ref.at[p]

    def rows_block(ref):
        return lambda p: ref.at[pl.ds(pl.multiple_of(p * TOKENS, TOKENS), TOKENS), :]

    def start(i, src_at, dst_at):
        return Exchange(me, src_at, dst_at, send.at[i], recv.at[i])

    def lanes_of(x):
        return [x[:, g * GRP_W:(g + 1) * GRP_W] for g in range(GRP)]

    def rows_of(x):
        return [x[g * ROWS:(g + 1) * ROWS] for g in range(GRP)]

    stage = 0
    ex_bias = start(stage, rows_block(bias_ref), block(b_all))
    b_all[me] = bias_ref[pl.ds(pl.multiple_of(me * TOKENS, TOKENS), TOKENS), :]
    q, k, v = [cat0([heads_ref[g, t] for g in range(GRP)]) for t in range(3)]
    ks, vs = sing_stack(k), sing_stack(v)
    logits = dot_nt(ks, q) * SING_SCALE
    mask = m_ref[...]
    ex_bias.arrive()
    probs = []
    for h in range(GRP_HEADS):
        b = cat0([b_all[g, h * ROWS:(h + 1) * ROWS, :] for g in range(GRP)]).astype(F32)
        probs.append(softmax_cols(logits[h * TOKENS:(h + 1) * TOKENS] + b + mask))
    pb = [p.astype(BF16) for p in probs]
    for g, x in enumerate(rows_of(dot_tn(cat0(pb), vs))):
        o_out[g] = x
    stage += 1
    ex_o = start(stage, block(o_out), block(o_in))
    o_in[me] = o_out[me]
    gate, s = gate_ref[...], s_ref[...].astype(F32)
    ds = ds_ref[...]
    d_act = dot_nt(ds, wd_ref[...])
    n_s, r_s = norm_parts(s)
    ex_o.arrive()
    att = cat1([o_in[g] for g in range(GRP)])
    gated = (gate * att).astype(BF16)
    s_mid = (s + dot_nn(gated, wo_ref[...])).astype(BF16).astype(F32)
    nhat, r_std = norm_parts(s_mid)
    nb = nhat.astype(BF16)
    hid = dot_nn(nb, wu_ref[...])
    h1, h2 = hid[:, :4 * C_S], hid[:, 4 * C_S:]
    sg = jax.nn.sigmoid(h1)
    a1 = h1 * sg
    dhid = cat1([d_act * h2 * (sg + a1 * (1.0 - sg)), d_act * a1]).astype(BF16)
    dsm = ds.astype(F32) + norm_back(dot_nt(dhid, wu_ref[...]), nhat, r_std)
    dsmb = dsm.astype(BF16)
    d_gated = dot_nt(dsmb, wo_ref[...])
    for g, x in enumerate(lanes_of((d_gated * gate).astype(BF16))):
        do_out[g] = x
    stage += 1
    ex_do = start(stage, block(do_out), block(do_in))
    do_in[me] = do_out[me]
    act = (a1 * h2).astype(BF16)
    so_ref[...] = (s_mid + dot_nn(act, wd_ref[...])).astype(BF16)
    dgl = (d_gated * att * gate * (1.0 - gate)).astype(BF16)
    for at, x in ((P_GATED, gated), (P_DMID, dsmb), (P_X2, nb), (P_DH, dhid), (P_ACT, act), (P_DOUT, ds), (P_NS, n_s.astype(BF16))):
        pk_ref[:, at:at + x.shape[1]] = x
    ex_do.arrive()
    do = cat0([do_in[g] for g in range(GRP)])
    dp = dot_nt(vs, do)
    dsb, dk, dv = [], [], []
    for h in range(GRP_HEADS):
        d = dp[h * TOKENS:(h + 1) * TOKENS]
        dlog = probs[h] * (d - col_sum(probs[h] * d))
        for g, x in enumerate(rows_of(dlog.astype(BF16))):
            db_out[g, h * ROWS:(h + 1) * ROWS, :] = x
        dsb.append((dlog * SING_SCALE).astype(BF16))
    stage += 1
    ex_db = start(stage, block(db_out), rows_block(dbt_ref))
    rows_block(dbt_ref)(me)[...] = db_out[me]
    for h in range(GRP_HEADS):
        dk.append(dot_nn(dsb[h], q))
        dv.append(dot_nn(pb[h], do))
    for t, x in enumerate((dot_tn(cat0(dsb), ks), sing_merge(dk), sing_merge(dv))):
        for g, y in enumerate(rows_of(x.astype(BF16))):
            dq_out[g, t] = y
    stage += 1
    ex_dq = start(stage, block(dq_out), block(dq_in))
    dq_in[me] = dq_out[me]
    ex_dq.arrive()
    dp_all = cat1([dq_in[g, t] for t in range(3) for g in range(GRP)] + [dgl])
    pk_ref[:, P_DQ:] = dp_all
    dsi_ref[...] = (dsm + norm_back(dot_nt(dp_all, wq_ref[...]), n_s, r_s)).astype(BF16)
    qb = col_sum(dp_all[:, :C_S].astype(F32))
    qb_ref[...] = cat0([qb[:, t * CH:(t + 1) * CH] for t in range(3)])
    ex_db.arrive()
    for ex in (ex_bias, ex_o, ex_do, ex_db, ex_dq):
        ex.leave()


def sing_fused(*args):
    vm = pl.BlockSpec(memory_space=pltpu.VMEM)
    dma = pltpu.SemaphoreType.DMA
    piece = (GRP, ROWS, GRP_W)
    triple = (GRP, 3, ROWS, GRP_W)
    outs = (sds((ROWS, C_S), BF16), sds((ROWS, C_S), BF16), sds((ROWS, P_ALL), BF16), sds((GRP * TOKENS, TOKENS), BF16), sds((3, CH), F32))
    sems = dma((5, len(OFFSETS)))
    return pl.pallas_call(
        sing_fused_kernel, out_shape=outs, in_specs=[vm] * len(args), out_specs=(vm,) * len(outs),
        scratch_shapes=[pltpu.VMEM((GRP, TOKENS, TOKENS), BF16), pltpu.VMEM(piece, F32), pltpu.VMEM(piece, F32),
                        pltpu.VMEM(piece, BF16), pltpu.VMEM(piece, BF16), pltpu.VMEM(triple, BF16), pltpu.VMEM(triple, BF16),
                        pltpu.VMEM((GRP, TOKENS, TOKENS), BF16), sems, sems],
        compiler_params=pltpu.CompilerParams(collective_id=2, has_side_effects=True), name='sing_fused',
        cost_estimate=pl.CostEstimate(flops=2 * GIGA, bytes_accessed=NOMINAL_BYTES, transcendentals=0),
    )(*args)


QKVG, PROJ, UP, DOWN = (4360, 12, 3), (8987, 3, 1), (10139, 24, 6), (19355, 3, 3)
KEPT = (((QKVG, 0, 136),), ((QKVG, 128, 384), (PROJ, 0, 384), (UP, 0, 80)), ((UP, 72, 328),), ((UP, 320, 384), (DOWN, 0, 384)))
W_ROWS = 1632


def kept_blocks(d):
    at = 0
    for weight, lo, hi in KEPT[d]:
        for t in range(weight[-1]):
            yield weight, lo, hi, t, at
            at += hi - lo


def sing_wgrad_kernel(m_ref, o_ref):
    k = lax.axis_index(GROUP_AXIS)

    def lanes(base, tiles, idx):
        width = tiles * CH
        return m_ref[:, pl.ds(pl.multiple_of(base + idx * width, CH), width)]

    def whole(base):
        return m_ref[:, base:base + C_S]

    grads = {
        QKVG: dot_tn(whole(P_NS), lanes(P_DQ, QKVG[-1], k)),
        PROJ: dot_tn(whole(P_GATED), lanes(P_DMID, 1, jnp.minimum(k, 2))),
        UP: dot_tn(whole(P_X2), lanes(P_DH, UP[-1], k)),
        DOWN: dot_tn(lanes(P_ACT, DOWN[-1], k), whole(P_DOUT)),
    }
    for d in range(GRP):
        end = 0
        for weight, lo, hi, t, at in kept_blocks(d):
            end = at + hi - lo
            o_ref[d, at:end, :] = grads[weight][lo:hi, t * CH:(t + 1) * CH]
        if end < W_ROWS:
            o_ref[d, end:, :] = jnp.zeros((W_ROWS - end, CH), F32)


def sing_wgrad(packed_all):
    return call(sing_wgrad_kernel, [sds((4, W_ROWS, 128), F32)], flops=GIGA, name='sing_wgrad')(packed_all)


PART = 766816
OUT_ROWS = 5992
SHIFT_ROWS = 56
SMALL_AT = ((0, 2048, 4, 24), (0, 2692, 4, 32), (1, 2978, 3, 0), (1, 2981, 16, 8))
LATE_ROWS = 1536
PIECE = LATE_ROWS // 16
LATE_SIZES = (512, 128, 128, 512, 128, 128)
EARLY_SIZES = (512, 128, 512, 128, 1024, 512)
EARLY_AT = (1536, 2052, 2180, 2696, 2824, 3848)


def finish_kernel(*refs):
    late_refs, (g_ref, p_ref, small_ref, o_ref, w_ref, x_ref, buf_ref, sum_ref, copy_sem, send1, recv1, send2, recv2) = refs[:6], refs[6:]
    d, k = lax.axis_index(BATCH_AXIS), lax.axis_index(GROUP_AXIS)
    me = 4 * d + k
    row, fills = 0, []
    for i, ref in enumerate(late_refs):
        fills.append(pltpu.make_async_copy(ref, x_ref.at[pl.ds(row, LATE_SIZES[i]), :], copy_sem.at[i]))
        row += LATE_SIZES[i]
    for c in fills:
        c.start()
    barrier = pltpu.get_barrier_semaphore()

    def device(p):
        return {BATCH_AXIS: p // 4, GROUP_AXIS: lax.rem(p, 4)}

    def piece(p):
        return pl.ds(pl.multiple_of(p * PIECE, PIECE), PIECE)

    for off in range(1, N_DEV):
        pl.semaphore_signal(barrier, inc=1, device_id=device(lax.rem(me + off, N_DEV)), device_id_type=MESH_ID)
    for c in fills:
        c.wait()
    pl.semaphore_wait(barrier, 15)
    first = []
    for off in range(1, N_DEV):
        p = lax.rem(me + off, N_DEV)
        c = pltpu.make_async_remote_copy(
            src_ref=x_ref.at[piece(p), :], dst_ref=buf_ref.at[off - 1], send_sem=send1.at[off - 1], recv_sem=recv1.at[off - 1],
            device_id=device(p), device_id_type=MESH_ID)
        c.start()
        first.append(c)

    def lay_out(part):
        begin = part * PART // 128
        lanes_off = part * PART % 128
        for weight, lo, hi, t, at in kept_blocks(part):
            base, tiles, own = weight
            for k in range(GRP):
                if weight == DOWN:
                    first_row = base + own * CH * k * tiles + t - begin
                else:
                    first_row = base + own * k + t - begin
                    if own * k + t >= tiles:
                        continue
                r0 = max(lo, -(first_row // tiles))
                r1 = min(hi, (OUT_ROWS - first_row) // tiles + 1)
                src = at + r0 - lo
                w_ref[pl.ds(first_row + r0 * tiles, r1 - r0, stride=tiles), :] = g_ref[k, src:src + r1 - r0, :]
        if part:
            lane = lax.broadcasted_iota(jnp.int32, (SHIFT_ROWS, CH), 1)

            def shift(i):
                w = pltpu.roll(w_ref[pl.ds(pl.multiple_of(i * SHIFT_ROWS, PACK), SHIFT_ROWS + PACK), :], CH - lanes_off, 1)
                o_ref[chunk_ds(i, SHIFT_ROWS), :] = jnp.where(lane < CH - lanes_off, w[:SHIFT_ROWS], w[1:SHIFT_ROWS + 1])

            loop(OUT_ROWS // SHIFT_ROWS, shift)
        else:
            o_ref[LATE_ROWS:, :] = w_ref[LATE_ROWS:OUT_ROWS, :]

    for part in range(GRP):
        @pl.when(d == part)
        def _():
            if part == 0:
                src = 0
                for n, at in zip(EARLY_SIZES, EARLY_AT):
                    w_ref[at:at + n, :] = p_ref[src:src + n, :]
                    src += n
            for own, at, n, src in SMALL_AT:
                if own == part:
                    w_ref[at:at + n, :] = small_ref[src:src + n, :]
            lay_out(part)

    for c in first:
        c.wait_recv()
    total = x_ref[piece(me), :]
    for i in range(15):
        total += buf_ref[i]
    sum_ref[...] = total

    def second(k, src):
        return pltpu.make_async_remote_copy(
            src_ref=sum_ref, dst_ref=o_ref.at[piece(src), :], send_sem=send2.at[k], recv_sem=recv2.at[src],
            device_id={BATCH_AXIS: 0, GROUP_AXIS: k}, device_id_type=MESH_ID)

    for k in range(GRP):
        @pl.when(me != k)
        def _():
            second(k, me).start()

    @pl.when(d == 0)
    def _():
        o_ref[piece(me), :] = total

    for k in range(GRP):
        @pl.when(me != k)
        def _():
            second(k, me).wait_send()

    @pl.when(d == 0)
    def _():
        for off in range(1, N_DEV):
            second(0, lax.rem(me + off, N_DEV)).wait_recv()

    for c in first:
        c.wait_send()


def finish(late, g_all, early, small):
    vm = pl.BlockSpec(memory_space=pltpu.VMEM)
    dma = pltpu.SemaphoreType.DMA
    return pl.pallas_call(
        finish_kernel, out_shape=sds((OUT_ROWS, 128), F32), in_specs=[vm] * 9, out_specs=vm,
        scratch_shapes=[pltpu.VMEM((6016, 128), F32), pltpu.VMEM((LATE_ROWS, 128), F32), pltpu.VMEM((15, PIECE, 128), F32),
                        pltpu.VMEM((PIECE, 128), F32), dma((6,)), dma((15,)), dma((15,)), dma((4,)), dma((16,))],
        compiler_params=pltpu.CompilerParams(collective_id=1, has_side_effects=True), name='finish',
        cost_estimate=pl.CostEstimate(flops=GIGA, bytes_accessed=NOMINAL_BYTES, transcendentals=0),
    )(*late, g_all, early, small)


def pack_kernel(*refs):
    *srcs, o_ref = refs
    at = 0
    for ref in srcs:
        n = ref.shape[0]
        if n % PACK:
            o_ref[at:at + PACK, :] = jnp.zeros((PACK, CH), F32)
        o_ref[at:at + n, :] = ref[...]
        at += padded(n)


def padded(n):
    return -(-n // PACK) * PACK


def pack_rows(*arrays):
    return call(pack_kernel, [sds((sum(padded(a.shape[0]) for a in arrays), CH), F32)], flops=GIGA, name='pack_rows')(*arrays)


def flat_cols(x):
    return x.T.reshape(x.shape)


def device_step(single_blk, pair_blk, mask_blk, d_single_blk, d_pair_blk, *weights):
    (w1_in, w1_gate, w1_out, w2_in, w2_gate, w2_out, st_qkvg, st_bias, st_proj, en_qkvg,
     en_bias, en_proj, p_up, p_down, s_qkvg, s_qbias, s_pbias, s_proj, s_up, s_down) = weights
    s_rows = single_blk[0]
    z_zero = pair_blk[0].reshape(N_POS, CH)
    mask_bias = (mask_blk[0].astype(jnp.float32) - 1.0) * MASK_PENALTY
    mask_col = mask_bias[:, None]
    right_out = mul_proj(z_zero, w1_in)
    x_out, z_one, right_out_all, left_out, turned, right_in = mul_mix(z_zero, w1_in, right_out, z_zero, w1_gate, w1_out, w2_in)
    x_in, z_two, _, _, s_gate, s_heads = mul_mix(
        turned.reshape(N_POS, CH), w2_in, right_in, z_one, w2_gate, w2_out, single=(s_rows, s_qkvg, s_qbias[None, :]))
    z_three, bias_st = att_fwd(z_two, st_bias, mask_col, st_qkvg, st_proj)
    zt_three = z_three.reshape(N_POS, CH)
    zt_four, bias_en, dzt_out = att_fwd(zt_three, en_bias, mask_col, en_qkvg, en_proj, d_pair_blk[0])
    zt_five, bias_t, turned_five = trans_fwd(zt_four, p_up, p_down, s_pbias)
    s_out, ds_in, packed, d_bias_t, g_qb = sing_fused(
        bias_t, s_heads, s_gate, s_rows, mask_col, s_proj, s_up, s_down, s_qkvg, d_single_blk[0])
    packed, d_bias_t = lax.optimization_barrier((packed, d_bias_t))
    packed_all = gather_rows(packed)
    dzt_four, g_pup, g_pdown, g_pbt = trans_bwd(
        zt_four, zt_five, dzt_out.reshape(N_POS, CH), d_bias_t, p_up, p_down, s_pbias)
    windows = sing_wgrad(packed_all)
    dzt_four, windows = lax.optimization_barrier((dzt_four, windows))
    piece = lax.psum_scatter(windows.reshape(4 * W_ROWS, 128), BATCH_AXIS, scatter_dimension=0, tiled=True)
    dz_three, end_grads, (left_out_all,) = att_backward(zt_three, dzt_four, bias_en, mask_col, en_qkvg, en_bias, en_proj, left_out)
    dz_three, piece = lax.optimization_barrier((dz_three, piece))
    pieces = gather_rows(piece)
    dz_two, start_grads, _ = att_backward(z_two, dz_three, bias_st, mask_col, st_qkvg, st_bias, st_proj)
    dz_two, pieces = lax.optimization_barrier((dz_two, pieces))
    dx_in, dgl_in, g_in_out = mul_post_bwd(dz_two, x_in, z_one, w2_gate, w2_out, False)
    early = pack_rows(start_grads[0], start_grads[2], end_grads[0], end_grads[2], g_pup, g_pdown, g_qb, g_pbt, start_grads[1], end_grads[1])
    early, dx_in = lax.optimization_barrier((early, dx_in))
    early = lax.psum(early, (BATCH_AXIS, GROUP_AXIS))
    tail = early[sum(EARLY_SIZES):]
    small = cat0([tail[:8], flat_cols(tail[8:24]), flat_cols(tail[24:28]), tail[28:32], flat_cols(tail[32:36]), tail[36:]])
    dz_one, g_in_in, g_in_gate = mul_pre_bwd(dx_in, None, right_in, z_one, w2_in, w2_gate, dgl_in, dz_two)
    dx_out, dgl_out, g_out_out, dx_turned = mul_post_bwd(dz_one, x_out, z_zero, w1_gate, w1_out, True)
    dz_zero, g_out_in, g_out_gate, z_five = mul_pre_bwd(
        dx_out, left_out_all, right_out_all, z_zero, w1_in, w1_gate, dgl_out, dz_one,
        dx_turned.reshape(N_POS, CH), turned_five.reshape(TURNED))
    late = (g_out_in, g_out_gate, g_out_out, g_in_in, g_in_gate, g_in_out)
    grad_flat = finish(late, pieces.reshape(4, W_ROWS, 128), early, small).reshape(-1)[:PART]
    dz_zero = dz_zero.reshape(ROWS, COLS, CH)
    return s_out[None], z_five[None], ds_in[None], dz_zero[None], grad_flat


def solution(mesh):
    spec_single = P(BATCH_AXIS, GROUP_AXIS, None)
    spec_pair = P(BATCH_AXIS, GROUP_AXIS, None, None)
    spec_mask = P(BATCH_AXIS, None)

    def block_fn(single_rep, pair_rep, token_mask, d_single_out, d_pair_out, *weights):
        in_specs = (spec_single, spec_pair, spec_mask, spec_single, spec_pair) + tuple(P() for w_item in weights)
        out_specs = (spec_single, spec_pair, spec_single, spec_pair, P(BATCH_AXIS))
        mapped = jax.shard_map(device_step, mesh=mesh, in_specs=in_specs, out_specs=out_specs, check_vma=False)
        return mapped(single_rep, pair_rep, token_mask, d_single_out, d_pair_out, *weights)

    return block_fn
```
